16 devices in a mesh: dp: 2 (over z), ep: 8 (over y, x, core).
Axes of the slice: x: 2, y: 2, z: 2, core: 2. Of those that a mesh axis runs over, the one named last changes fastest.
Arguments:
- x_tokens: bfloat16 [2048, 2048], P(('dp', 'ep')), parts along dimension 0
- dy_tokens: bfloat16 [2048, 2048], P(('dp', 'ep')), parts along dimension 0
- expert_ids: int32 [2048, 10], P(('dp', 'ep')), parts along dimension 0
- gate_vals: float32 [2048, 10], P(('dp', 'ep')), parts along dimension 0
- slot_pos: int32 [2048, 10], P(('dp', 'ep')), parts along dimension 0
- w_gate: bfloat16 [32, 2048, 512], P('ep')
- w_up: bfloat16 [32, 2048, 512], P('ep')
- w_down: bfloat16 [32, 512, 2048], P('ep')
- shared_gate: bfloat16 [2048, 512], replicated
- shared_up: bfloat16 [2048, 512], replicated
- shared_down: bfloat16 [512, 2048], replicated
Outputs:
- output 1: bfloat16 [2048, 2048], P(('dp', 'ep')), parts along dimension 0
- output 2: float32 [64, 2048, 512], P(('dp', 'ep')), parts along dimension 0
- output 3: float32 [64, 2048, 512], P(('dp', 'ep')), parts along dimension 0
- output 4: float32 [64, 512, 2048], P(('dp', 'ep')), parts along dimension 0
- output 5: float32 [16, 2048, 512], P(('dp', 'ep')), parts along dimension 0
- output 6: float32 [16, 2048, 512], P(('dp', 'ep')), parts along dimension 0
- output 7: float32 [16, 512, 2048], P(('dp', 'ep')), parts along dimension 0
There are 2 independent parts. The reference program is written for one: setup_inputs(seed, part) draws one part's arguments, and reference() takes and returns one part's arrays. A program takes and returns all parts, laid end to end along the dimension named above; an argument that names none is the same for every part.
All inputs are finite; a program needn't handle non-finite values.
Results may differ from the reference program's by a relative error of at most 0.0104866.
Values are sent between devices in bfloat16 or wider.
A program may use at most 1 GiB of HBM per device.

```python
import jax
import jax.numpy as jnp
from jax import lax

MODEL_DIM = 2048
EXPERT_FF = 512
SHARED_FF = 512
TOP_K = 10
TOK_DEV = 128
GROUP_SIZE = 8
NUM_EXPERTS = 32
CAPACITY = 60


def draw_routing(route_key):
    bias_key, hot_key, noise_key = jax.random.split(route_key, 3)
    expert_range = jnp.arange(NUM_EXPERTS, dtype=jnp.int32)
    expert_bias = jax.random.randint(bias_key, (NUM_EXPERTS,), 0, 256)
    hot_expert = jax.random.randint(hot_key, (GROUP_SIZE,), 0, NUM_EXPERTS)
    noise = jax.random.randint(noise_key, (GROUP_SIZE, TOK_DEV, NUM_EXPERTS), 0, 1024)
    forced = (jnp.arange(TOK_DEV)[None, :, None] < CAPACITY) & (expert_range[None, None, :] == hot_expert[:, None, None])
    score = (noise + expert_bias[None, None, :] + 4096 * forced.astype(jnp.int32)) * NUM_EXPERTS + expert_range
    choices = lax.top_k(score, TOP_K)[1]

    def source_slots(source_choices):
        flat_choices = source_choices.reshape(-1)
        onehot = (flat_choices[:, None] == expert_range[None, :]).astype(jnp.int32)
        earlier = jnp.cumsum(onehot, axis=0) - onehot
        slot_rank = jnp.sum(earlier * onehot, axis=1)
        return jnp.where(slot_rank < CAPACITY, slot_rank, -1).reshape(TOK_DEV, TOP_K)

    positions = lax.map(source_slots, choices)
    return choices.reshape(-1, TOP_K).astype(jnp.int32), positions.reshape(-1, TOP_K).astype(jnp.int32)


def setup_inputs(seed: int = 0, part: int = 0) -> dict:
    part_key = jax.random.fold_in(jax.random.key(seed), part)
    key_x, key_dy, key_gate, key_route = jax.random.split(part_key, 4)
    weight_keys = jax.random.split(jax.random.key(seed + 1), 6)
    tokens = GROUP_SIZE * TOK_DEV
    x_tokens = jax.random.normal(key_x, (tokens, MODEL_DIM), jnp.float32).astype(jnp.bfloat16)
    dy_tokens = jax.random.normal(key_dy, (tokens, MODEL_DIM), jnp.float32).astype(jnp.bfloat16)
    gate_vals = jax.random.uniform(key_gate, (tokens, TOP_K), jnp.float32, 0.25, 1.0)
    expert_ids, slot_pos = draw_routing(key_route)
    in_scale = MODEL_DIM ** -0.5
    ff_scale = EXPERT_FF ** -0.5
    shared_scale = SHARED_FF ** -0.5
    w_gate = (jax.random.normal(weight_keys[0], (NUM_EXPERTS, MODEL_DIM, EXPERT_FF), jnp.float32) * in_scale).astype(jnp.bfloat16)
    w_up = (jax.random.normal(weight_keys[1], (NUM_EXPERTS, MODEL_DIM, EXPERT_FF), jnp.float32) * in_scale).astype(jnp.bfloat16)
    w_down = (jax.random.normal(weight_keys[2], (NUM_EXPERTS, EXPERT_FF, MODEL_DIM), jnp.float32) * ff_scale).astype(jnp.bfloat16)
    shared_gate = (jax.random.normal(weight_keys[3], (MODEL_DIM, SHARED_FF), jnp.float32) * in_scale).astype(jnp.bfloat16)
    shared_up = (jax.random.normal(weight_keys[4], (MODEL_DIM, SHARED_FF), jnp.float32) * in_scale).astype(jnp.bfloat16)
    shared_down = (jax.random.normal(weight_keys[5], (SHARED_FF, MODEL_DIM), jnp.float32) * shared_scale).astype(jnp.bfloat16)
    return {'x_tokens': x_tokens, 'dy_tokens': dy_tokens, 'expert_ids': expert_ids, 'gate_vals': gate_vals, 'slot_pos': slot_pos, 'w_gate': w_gate, 'w_up': w_up, 'w_down': w_down, 'shared_gate': shared_gate, 'shared_up': shared_up, 'shared_down': shared_down}


def expert_grads(x_rows, dz_rows, gate_w, up_w, down_w):
    act_gate = jnp.dot(x_rows, gate_w, preferred_element_type=jnp.float32).astype(jnp.bfloat16)
    act_up = jnp.dot(x_rows, up_w, preferred_element_type=jnp.float32).astype(jnp.bfloat16)
    gate_f32 = act_gate.astype(jnp.float32)
    up_f32 = act_up.astype(jnp.float32)
    sigma = jax.nn.sigmoid(gate_f32)
    silu_gate = gate_f32 * sigma
    hidden = (silu_gate * up_f32).astype(jnp.bfloat16)
    grad_hidden = jnp.dot(dz_rows, down_w.T, preferred_element_type=jnp.float32)
    grad_gate = (grad_hidden * up_f32 * sigma * (1.0 + gate_f32 * (1.0 - sigma))).astype(jnp.bfloat16)
    grad_up = (grad_hidden * silu_gate).astype(jnp.bfloat16)
    grad_down_w = jnp.dot(hidden.T, dz_rows, preferred_element_type=jnp.float32)
    grad_gate_w = jnp.dot(x_rows.T, grad_gate, preferred_element_type=jnp.float32)
    grad_up_w = jnp.dot(x_rows.T, grad_up, preferred_element_type=jnp.float32)
    grad_rows = jnp.dot(grad_gate, gate_w.T, preferred_element_type=jnp.float32) + jnp.dot(grad_up, up_w.T, preferred_element_type=jnp.float32)
    return grad_rows, grad_gate_w, grad_up_w, grad_down_w


def reference(x_tokens, dy_tokens, expert_ids, gate_vals, slot_pos, w_gate, w_up, w_down, shared_gate, shared_up, shared_down):
    tokens = GROUP_SIZE * TOK_DEV
    slot_rows = GROUP_SIZE * CAPACITY
    total_rows = NUM_EXPERTS * slot_rows
    source = jnp.arange(tokens, dtype=jnp.int32)[:, None] // TOK_DEV
    target = jnp.where(slot_pos >= 0, expert_ids * slot_rows + source * CAPACITY + slot_pos, total_rows).reshape(-1)
    token_index = jnp.broadcast_to(jnp.arange(tokens, dtype=jnp.int32)[:, None], (tokens, TOP_K)).reshape(-1)
    row_token = jnp.full((total_rows + 1,), tokens, jnp.int32).at[target].set(token_index)[:total_rows].reshape(NUM_EXPERTS, slot_rows)
    row_gate = jnp.zeros((total_rows + 1,), jnp.float32).at[target].set(gate_vals.reshape(-1))[:total_rows].reshape(NUM_EXPERTS, slot_rows)

    def expert_step(routed_sum, expert_in):
        token_rows, gate_rows, gate_w, up_w, down_w = expert_in
        x_rows = jnp.take(x_tokens, token_rows, axis=0, mode='fill', fill_value=0)
        dy_rows = jnp.take(dy_tokens, token_rows, axis=0, mode='fill', fill_value=0)
        dz_rows = (dy_rows.astype(jnp.float32) * gate_rows[:, None]).astype(jnp.bfloat16)
        grad_rows, grad_gate_w, grad_up_w, grad_down_w = expert_grads(x_rows, dz_rows, gate_w, up_w, down_w)
        returned = grad_rows.astype(jnp.bfloat16).astype(jnp.float32)
        routed_sum = routed_sum.at[token_rows].add(returned, mode='drop')
        return routed_sum, (grad_gate_w, grad_up_w, grad_down_w)

    routed_sum, expert_w_grads = lax.scan(expert_step, jnp.zeros((tokens, MODEL_DIM), jnp.float32), (row_token, row_gate, w_gate, w_up, w_down))
    grad_w_gate, grad_w_up, grad_w_down = expert_w_grads

    def shared_step(source_in):
        x_rows, dy_rows = source_in
        return expert_grads(x_rows, dy_rows, shared_gate, shared_up, shared_down)

    shared_dx, grad_shared_gate, grad_shared_up, grad_shared_down = lax.map(shared_step, (x_tokens.reshape(GROUP_SIZE, TOK_DEV, MODEL_DIM), dy_tokens.reshape(GROUP_SIZE, TOK_DEV, MODEL_DIM)))
    grad_x = (routed_sum + shared_dx.reshape(tokens, MODEL_DIM)).astype(jnp.bfloat16)
    return (grad_x, grad_w_gate, grad_w_up, grad_w_down, grad_shared_gate, grad_shared_up, grad_shared_down)
```

```python
import jax
import jax.numpy as jnp
from jax import lax
from jax.experimental import pallas as pl
from jax.experimental.pallas import tpu as pltpu
from jax.sharding import PartitionSpec as P

MESH = pl.DeviceIdType.MESH
SLOT = 64
BF16 = jnp.bfloat16
F32 = jnp.float32


def swiglu_parts(act_gate, act_up, grad_hidden):
    gate_f32 = act_gate.astype(F32)
    up_f32 = act_up.astype(F32)
    sigma = jax.nn.sigmoid(gate_f32)
    silu_gate = gate_f32 * sigma
    hidden = (silu_gate * up_f32).astype(BF16)
    grad_gate = (grad_hidden * up_f32 * sigma * (1.0 + gate_f32 * (1.0 - sigma))).astype(BF16)
    grad_up = (grad_hidden * silu_gate).astype(BF16)
    return hidden, grad_gate, grad_up


def shared_backward(x_tokens, dy_tokens, shared_gate, shared_up, shared_down):
    act_gate = jnp.dot(x_tokens, shared_gate, preferred_element_type=F32).astype(BF16)
    act_up = jnp.dot(x_tokens, shared_up, preferred_element_type=F32).astype(BF16)
    grad_hidden = jnp.einsum('td,fd->tf', dy_tokens, shared_down, preferred_element_type=F32)
    hidden, grad_gate, grad_up = swiglu_parts(act_gate, act_up, grad_hidden)
    grad_gate_w = jnp.einsum('td,tf->df', x_tokens, grad_gate, preferred_element_type=F32)
    grad_up_w = jnp.einsum('td,tf->df', x_tokens, grad_up, preferred_element_type=F32)
    grad_down_w = jnp.einsum('tf,td->fd', hidden, dy_tokens, preferred_element_type=F32)
    grad_input = jnp.einsum('tf,df->td', grad_gate, shared_gate, preferred_element_type=F32) + jnp.einsum('tf,df->td', grad_up, shared_up, preferred_element_type=F32)
    return grad_input, grad_gate_w, grad_up_w, grad_down_w


def dot_nn(a, b):
    return lax.dot_general(a, b, (((1,), (0,)), ((), ())), preferred_element_type=F32)


def dot_nt(a, b):
    return lax.dot_general(a, b, (((1,), (1,)), ((), ())), preferred_element_type=F32)


def dot_tn(a, b):
    return lax.dot_general(a, b, (((0,), (0,)), ((), ())), preferred_element_type=F32)


def places():
    me = lax.axis_index('ep')
    core = lax.rem(me, 2)
    flip_x = 2 - 4 * lax.rem(me // 2, 2)
    flip_y = 4 - 8 * (me // 4)
    first = me + flip_x * (1 - core) + flip_y * core
    second = me + flip_y * (1 - core) + flip_x * core
    diag = me + flip_x + flip_y
    partner = me + 1 - 2 * core
    return me, core, first, second, diag, partner


def remote(src, dst, send_sem, recv_sem, device):
    return pltpu.make_async_remote_copy(src_ref=src, dst_ref=dst, send_sem=send_sem, recv_sem=recv_sem, device_id={'ep': device}, device_id_type=MESH)


def gather_kernel(x_ref, dy_ref, code_ref, gate_ref, xg_ref, dyg_ref, codeg_ref, gateg_ref, xbuf, dybuf, send_sem, recv_sem, meta_send, meta_recv, out_sem):
    me, core, first, second, diag, partner = places()
    barrier = pltpu.get_barrier_semaphore()
    for step in range(1, 8):
        pl.semaphore_signal(barrier, inc=1, device_id={'ep': lax.rem(me + step, 8)}, device_id_type=MESH)
    pl.semaphore_wait(barrier, 7)

    meta = []
    for step in range(1, 8):
        peer = lax.rem(me + step, 8)
        for which, (src, dst) in enumerate(((code_ref, codeg_ref), (gate_ref, gateg_ref))):
            copy = remote(src, dst.at[me], meta_send.at[which, step - 1], meta_recv.at[which, step - 1], peer)
            copy.start()
            meta.append(copy)
    codeg_ref[me] = code_ref[...]
    gateg_ref[me] = gate_ref[...]

    def own(array, src, buf):
        to_first = remote(src, buf.at[me], send_sem.at[array, 0], recv_sem.at[array, 0], first)
        to_second = remote(src, buf.at[me], send_sem.at[array, 1], recv_sem.at[array, 1], second)
        to_partner = remote(src, buf.at[me], send_sem.at[array, 2], recv_sem.at[array, 2], partner)
        to_first.start()
        to_second.start()
        to_partner.start()
        return [to_first, to_second, to_partner]

    def forward(array, buf, block, slot, device):
        copy = remote(buf.at[block], buf.at[block], send_sem.at[array, slot], recv_sem.at[array, slot], device)
        copy.start()
        return copy

    arrays = ((x_ref, xbuf, xg_ref), (dy_ref, dybuf, dyg_ref))
    sent = []
    outs = []
    sent.append(own(0, x_ref, xbuf))
    for array, (src, buf, out) in enumerate(arrays):
        copies = sent[array]
        copies[0].wait_recv()
        copies.append(forward(array, buf, first, 3, second))
        copies.append(forward(array, buf, first, 4, partner))
        if array == 0:
            sent.append(own(1, dy_ref, dybuf))
        copies[1].wait_recv()
        copies.append(forward(array, buf, second, 5, partner))
        copies[3].wait_recv()
        copies.append(forward(array, buf, diag, 6, partner))
        for index in (2, 4, 5, 6):
            copies[index].wait_recv()
        mine = pltpu.make_async_copy(src, out.at[me], out_sem.at[array, 0])
        mine.start()
        outs.append(mine)
        for step in range(1, 8):
            block = lax.rem(me + step, 8)
            copy = pltpu.make_async_copy(buf.at[block], out.at[block], out_sem.at[array, step])
            copy.start()
            outs.append(copy)
    for copies in sent:
        for copy in copies:
            copy.wait_send()
    for copy in meta:
        copy.wait()
    for copy in outs:
        copy.wait()


def gather_tokens(x_tokens, dy_tokens, code, gate):
    tokens, width = x_tokens.shape
    vmem = pl.BlockSpec(memory_space=pltpu.VMEM)
    hbm = pl.BlockSpec(memory_space=pl.ANY)
    return pl.pallas_call(
        gather_kernel,
        out_shape=(
            jax.ShapeDtypeStruct((8, tokens, width), BF16),
            jax.ShapeDtypeStruct((8, tokens, width), BF16),
            jax.ShapeDtypeStruct((8,) + code.shape, jnp.int32),
            jax.ShapeDtypeStruct((8,) + gate.shape, F32),
        ),
        in_specs=[vmem] * 4,
        out_specs=(hbm, hbm, vmem, vmem),
        scratch_shapes=[
            pltpu.VMEM((8, tokens, width), BF16),
            pltpu.VMEM((8, tokens, width), BF16),
            pltpu.SemaphoreType.DMA((2, 7)),
            pltpu.SemaphoreType.DMA((2, 7)),
            pltpu.SemaphoreType.DMA((2, 7)),
            pltpu.SemaphoreType.DMA((2, 7)),
            pltpu.SemaphoreType.DMA((2, 8)),
        ],
        compiler_params=pltpu.CompilerParams(collective_id=0, has_side_effects=True),
        name='gather_tokens',
    )(x_tokens, dy_tokens, code, gate)


TILES = 4


def expert_kernel(xg_ref, dyg_ref, code_ref, gate_ref, w1_ref, w3_ref, w2_ref, dw1_ref, dw3_ref, dw2_ref, part_ref, x_rows, z_rows, hidden_t, grad_gate, grad_up, onehot_t, acc, out_sem):
    expert = pl.program_id(0)
    tile = pl.program_id(1)
    local = lax.axis_index('ep') * 4 + expert

    @pl.when(tile == 0)
    def _():
        def pick(source, carry):
            slot = lax.broadcasted_iota(jnp.int32, (SLOT, 128), 0) + local * SLOT
            onehot = jnp.zeros((SLOT, 128), F32)
            gates = jnp.zeros((SLOT, 128), F32)
            for choice in range(10):
                hit = slot == code_ref[source, choice:choice + 1, :]
                onehot = jnp.where(hit, 1.0, onehot)
                gates = jnp.where(hit, gate_ref[source, choice:choice + 1, :], gates)
            gate_row = jnp.sum(gates, axis=1, keepdims=True)
            select = onehot.astype(BF16)
            onehot_t[source] = onehot.T.astype(BF16)
            rows = pl.ds(pl.multiple_of(source * SLOT, SLOT), SLOT)
            x_rows[rows, :] = dot_nn(select, xg_ref[source]).astype(BF16)
            z_rows[rows, :] = (dot_nn(select, dyg_ref[source]) * gate_row).astype(BF16)
            return carry

        lax.fori_loop(0, 8, pick, 0)
        act_gate = dot_nn(x_rows[...], w1_ref[0]).astype(BF16)
        act_up = dot_nn(x_rows[...], w3_ref[0]).astype(BF16)
        grad_hidden = dot_nt(z_rows[...], w2_ref[0])
        hidden, d_gate, d_up = swiglu_parts(act_gate, act_up, grad_hidden)
        hidden_t[...] = hidden.T
        grad_gate[...] = d_gate
        grad_up[...] = d_up

    cols = pl.ds(pl.multiple_of(tile * 512, 512), 512)
    rows_out = (dot_nt(grad_gate[...], w1_ref[0, cols, :]) + dot_nt(grad_up[...], w3_ref[0, cols, :])).astype(BF16)
    for source in range(8):
        term = dot_nn(onehot_t[source], rows_out[source * SLOT:(source + 1) * SLOT, :])

        @pl.when(expert == 0)
        def _():
            acc[tile, source] = term

        @pl.when(expert > 0)
        def _():
            acc[tile, source] += term

    x_cols_t = x_rows[:, cols].T
    dw1_ref[0] = dot_nn(x_cols_t, grad_gate[...])
    dw3_ref[0] = dot_nn(x_cols_t, grad_up[...])
    dw2_ref[0] = dot_nn(hidden_t[...], z_rows[:, cols])

    @pl.when(expert == 3)
    def _():
        pltpu.make_async_copy(acc.at[tile], part_ref.at[tile], out_sem.at[tile]).start()

    @pl.when(jnp.logical_and(expert == 3, tile == TILES - 1))
    def _():
        for index in range(TILES):
            pltpu.make_async_copy(acc.at[index], part_ref.at[index], out_sem.at[index]).wait()


def expert_backward(xg, dyg, code, gate, w_gate, w_up, w_down):
    experts, width, inner = w_gate.shape
    tokens = xg.shape[1]
    vmem = pl.BlockSpec(memory_space=pltpu.VMEM)
    whole = lambda e, t: (e, 0, 0)
    return pl.pallas_call(
        expert_kernel,
        grid=(experts, TILES),
        out_shape=(
            jax.ShapeDtypeStruct((experts, width, inner), F32),
            jax.ShapeDtypeStruct((experts, width, inner), F32),
            jax.ShapeDtypeStruct((experts, inner, width), F32),
            jax.ShapeDtypeStruct((TILES, 8, tokens, width // TILES), F32),
        ),
        in_specs=[
            pl.BlockSpec((8, tokens, width), lambda e, t: (0, 0, 0), pipeline_mode=pl.Buffered(1)),
            pl.BlockSpec((8, tokens, width), lambda e, t: (0, 0, 0), pipeline_mode=pl.Buffered(1)),
            vmem,
            vmem,
            pl.BlockSpec((1, width, inner), whole),
            pl.BlockSpec((1, width, inner), whole),
            pl.BlockSpec((1, inner, width), whole),
        ],
        out_specs=(
            pl.BlockSpec((1, width // TILES, inner), lambda e, t: (e, t, 0)),
            pl.BlockSpec((1, width // TILES, inner), lambda e, t: (e, t, 0)),
            pl.BlockSpec((1, inner, width // TILES), lambda e, t: (e, 0, t)),
            pl.BlockSpec(memory_space=pl.ANY),
        ),
        scratch_shapes=[
            pltpu.VMEM((8 * SLOT, width), BF16),
            pltpu.VMEM((8 * SLOT, width), BF16),
            pltpu.VMEM((inner, 8 * SLOT), BF16),
            pltpu.VMEM((8 * SLOT, inner), BF16),
            pltpu.VMEM((8 * SLOT, inner), BF16),
            pltpu.VMEM((8, tokens, SLOT), BF16),
            pltpu.VMEM((TILES, 8, tokens, width // TILES), F32),
            pltpu.SemaphoreType.DMA((TILES,)),
        ],
        compiler_params=pltpu.CompilerParams(dimension_semantics=('arbitrary', 'arbitrary'), vmem_limit_bytes=66000000),
        cost_estimate=pl.CostEstimate(flops=40_000_000_000, bytes_accessed=90_000_000, transcendentals=1_000_000),
        name='expert_backward',
    )(xg, dyg, code, gate, w_gate, w_up, w_down)


def scatter_kernel(part_ref, shared_ref, out_ref, mine, pair, got_first, got_second, got_last, load_sem, pair_send, pair_recv, first_send, first_recv, second_send, second_recv, last_send, last_recv):
    me, core, first, second, diag, partner = places()
    chip, first_chip, second_chip, diag_chip = me // 2, first // 2, second // 2, diag // 2
    barrier = pltpu.get_barrier_semaphore()
    for device in (partner, first, second):
        pl.semaphore_signal(barrier, inc=1, device_id={'ep': device}, device_id_type=MESH)
    pl.semaphore_wait(barrier, 3)

    other = 1 - core
    loads, pairs = {}, {}
    for index, (give, take) in enumerate(((diag_chip, diag_chip), (second_chip, first_chip), (first_chip, second_chip), (chip, chip))):
        for half in range(2):
            copy = remote(part_ref.at[other * 2 + half, give], pair.at[half, give], pair_send.at[index, half], pair_recv.at[index, half], partner)
            copy.start()
            pairs[index, half] = copy
            copy = pltpu.make_async_copy(part_ref.at[core * 2 + half, take], mine.at[half, take], load_sem.at[index, half])
            copy.start()
            loads[index, half] = copy

    def both(index, half, block):
        loads[index, half].wait()
        pairs[index, half].wait_recv()
        return mine[half, block] + pair[half, block]

    firsts, seconds = {}, {}
    for index, block in ((0, diag_chip), (1, first_chip)):
        for half in range(2):
            mine[half, block] = both(index, half, block)
            copy = remote(mine.at[half, block], got_first.at[index, half], first_send.at[index, half], first_recv.at[index, half], first)
            copy.start()
            firsts[index, half] = copy
    for half in range(2):
        value = both(2, half, second_chip)
        firsts[0, half].wait_recv()
        mine[half, second_chip] = value + got_first[0, half]
        copy = remote(mine.at[half, second_chip], got_second.at[half], second_send.at[half], second_recv.at[half], second)
        copy.start()
        seconds[half] = copy
    lasts = {}
    for half in range(2):
        value = both(3, half, chip)
        firsts[1, half].wait_recv()
        mine[half, chip] = value + got_first[1, half]
    for half in range(2):
        seconds[half].wait_recv()
        mine[half, chip] += got_second[half]
        copy = remote(mine.at[half, chip, other], got_last.at[half], last_send.at[half], last_recv.at[half], partner)
        copy.start()
        lasts[half] = copy
    for half in range(2):
        cols = pl.ds(pl.multiple_of(core * 1024 + half * 512, 512), 512)
        out_ref[:, cols] = (mine[half, chip, core] + shared_ref[:, cols]).astype(BF16)
    for half in range(2):
        lasts[half].wait_recv()
        cols = pl.ds(pl.multiple_of(other * 1024 + half * 512, 512), 512)
        out_ref[:, cols] = (got_last[half] + shared_ref[:, cols]).astype(BF16)
    for group in (pairs, firsts, seconds, lasts):
        for copy in group.values():
            copy.wait_send()


def scatter_sum(part, shared_dx):
    tokens, width = shared_dx.shape
    vmem = pl.BlockSpec(memory_space=pltpu.VMEM)
    piece = (2, tokens, width // TILES)
    part = part.reshape((TILES, 4) + piece)
    dma = pltpu.SemaphoreType.DMA
    return pl.pallas_call(
        scatter_kernel,
        out_shape=jax.ShapeDtypeStruct((tokens, width), BF16),
        in_specs=[pl.BlockSpec(memory_space=pl.ANY), vmem],
        out_specs=vmem,
        scratch_shapes=[
            pltpu.VMEM((2, 4) + piece, F32),
            pltpu.VMEM((2, 4) + piece, F32),
            pltpu.VMEM((2, 2) + piece, F32),
            pltpu.VMEM((2,) + piece, F32),
            pltpu.VMEM((2, tokens, width // TILES), F32),
            dma((4, 2)),
            dma((4, 2)),
            dma((4, 2)),
            dma((2, 2)),
            dma((2, 2)),
            dma((2,)),
            dma((2,)),
            dma((2,)),
            dma((2,)),
        ],
        compiler_params=pltpu.CompilerParams(collective_id=1, has_side_effects=True),
        name='scatter_sum',
    )(part, shared_dx)


def solution(mesh):
    token_spec = P(('dp', 'ep'), None)
    expert_spec = P('ep', None, None)
    whole_spec = P(None, None)
    grad_spec = P(('dp', 'ep'), None, None)

    def local_backward(x_tokens, dy_tokens, expert_ids, gate_vals, slot_pos, w_gate, w_up, w_down, shared_gate, shared_up, shared_down):
        code = jnp.where(slot_pos >= 0, expert_ids * SLOT + slot_pos, -1)
        code = jnp.pad(code.T, ((0, 6), (0, 0)), constant_values=-1)
        gate = jnp.pad(gate_vals.T, ((0, 6), (0, 0)))
        xg, dyg, codes, gates = gather_tokens(x_tokens, dy_tokens, code, gate)
        grad_w_gate, grad_w_up, grad_w_down, part = expert_backward(xg, dyg, codes, gates, w_gate, w_up, w_down)
        shared_dx, grad_shared_gate, grad_shared_up, grad_shared_down = shared_backward(x_tokens, dy_tokens, shared_gate, shared_up, shared_down)
        grad_x = scatter_sum(part, shared_dx)
        return grad_x, grad_w_gate, grad_w_up, grad_w_down, grad_shared_gate[None], grad_shared_up[None], grad_shared_down[None]

    return jax.shard_map(local_backward, mesh=mesh, in_specs=(token_spec, token_spec, token_spec, token_spec, token_spec, expert_spec, expert_spec, expert_spec, whole_spec, whole_spec, whole_spec), out_specs=(token_spec, grad_spec, grad_spec, grad_spec, grad_spec, grad_spec, grad_spec), check_vma=False)
```

```python
import jax
import jax.numpy as jnp
from jax import lax
from jax.experimental import pallas as pl
from jax.experimental.pallas import tpu as pltpu
from jax.sharding import PartitionSpec as P

MESH = pl.DeviceIdType.MESH
SLOT = 64
BF16 = jnp.bfloat16
F32 = jnp.float32


def swiglu_parts(act_gate, act_up, grad_hidden):
    gate_f32 = act_gate.astype(F32)
    up_f32 = act_up.astype(F32)
    sigma = jax.nn.sigmoid(gate_f32)
    silu_gate = gate_f32 * sigma
    hidden = (silu_gate * up_f32).astype(BF16)
    grad_gate = (grad_hidden * up_f32 * sigma * (1.0 + gate_f32 * (1.0 - sigma))).astype(BF16)
    grad_up = (grad_hidden * silu_gate).astype(BF16)
    return hidden, grad_gate, grad_up


def dot_nn(a, b):
    return lax.dot_general(a, b, (((1,), (0,)), ((), ())), preferred_element_type=F32)


def dot_nt(a, b):
    return lax.dot_general(a, b, (((1,), (1,)), ((), ())), preferred_element_type=F32)


def dot_tn(a, b):
    return lax.dot_general(a, b, (((0,), (0,)), ((), ())), preferred_element_type=F32)


def places():
    me = lax.axis_index('ep')
    core = lax.rem(me, 2)
    flip_x = 2 - 4 * lax.rem(me // 2, 2)
    flip_y = 4 - 8 * (me // 4)
    first = me + flip_x * (1 - core) + flip_y * core
    second = me + flip_y * (1 - core) + flip_x * core
    diag = me + flip_x + flip_y
    partner = me + 1 - 2 * core
    return me, core, first, second, diag, partner


def remote(src, dst, send_sem, recv_sem, device):
    return pltpu.make_async_remote_copy(src_ref=src, dst_ref=dst, send_sem=send_sem, recv_sem=recv_sem, device_id={'ep': device}, device_id_type=MESH)


def pair_of(role, step):
    me, core, first, second, diag, partner = places()
    other = 1 - core
    if role == 0:
        return me * (1 - step) + partner * step
    if role == 1:
        return first * (1 - step) + ((second // 2) * 2 + other) * step
    if role == 2:
        return second * (1 - step) + ((first // 2) * 2 + other) * step
    return diag * (1 - step) + ((diag // 2) * 2 + other) * step


def one_hot(code, base, rows):
    slot = lax.broadcasted_iota(jnp.int32, (rows, 128), 0) + base
    hits = jnp.zeros((rows, 128), F32)
    for choice in range(10):
        hits = jnp.where(slot == code[choice:choice + 1, :], 1.0, hits)
    return hits


def gather_kernel(x_ref, dy_ref, code_ref, gate_ref, w1_ref, w3_ref, xr_ref, zr_ref, a_ref, b_ref, codeg_ref, xbuf, dybuf, x_rows, z_rows, w1_buf, w3_buf, a_buf, b_buf, gateg, send_sem, recv_sem, meta_send, meta_recv, load_sem, out_sem, act_sem):
    me, core, first, second, diag, partner = places()
    loads = []
    for expert in range(4):
        for which, (src, dst) in enumerate(((w1_ref, w1_buf), (w3_ref, w3_buf))):
            copy = pltpu.make_async_copy(src.at[expert], dst.at[expert], load_sem.at[which, expert])
            copy.start()
            loads.append(copy)
    barrier = pltpu.get_barrier_semaphore()
    for step in range(1, 8):
        pl.semaphore_signal(barrier, inc=1, device_id={'ep': lax.rem(me + step, 8)}, device_id_type=MESH)
    pl.semaphore_wait(barrier, 7)

    half = 64
    srcs = (x_ref, dy_ref)
    bufs = (xbuf, dybuf)
    copies = {}

    def send(array, part, kind, block, device, own=False):
        rows = pl.ds(part * half, half)
        src = srcs[array].at[rows] if own else bufs[array].at[block, rows]
        copy = remote(src, bufs[array].at[block, rows], send_sem.at[array, part, kind], recv_sem.at[array, part, kind], device)
        copy.start()
        copies[array, part, kind] = copy

    def got(array, part, kind):
        copies[array, part, kind].wait_recv()

    for part in range(2):
        send(0, part, 0, me, first, own=True)
    meta = []
    for step in range(1, 8):
        peer = lax.rem(me + step, 8)
        for which, (src, dst) in enumerate(((code_ref, codeg_ref), (gate_ref, gateg))):
            copy = remote(src, dst.at[me], meta_send.at[which, step - 1], meta_recv.at[which, step - 1], peer)
            copy.start()
            meta.append(copy)
    for array in range(2):
        for part in range(2):
            send(array, part, 2, me, partner, own=True)
    codeg_ref[me] = code_ref[...]
    gateg[me] = gate_ref[...]
    xbuf[me] = x_ref[...]
    dybuf[me] = dy_ref[...]

    outs = []

    def pick(array, role):
        def one(step, carry):
            source = pair_of(role, step)
            hits = one_hot(codeg_ref[source], me * 256, 256)
            select = hits.astype(BF16)
            if array == 1:
                slot = lax.broadcasted_iota(jnp.int32, (256, 128), 0) + me * 256
                gates = jnp.zeros((256, 128), F32)
                for choice in range(10):
                    gates = jnp.where(slot == codeg_ref[source, choice:choice + 1, :], gateg[source, choice:choice + 1, :], gates)
                scale = jnp.sum(gates, axis=1, keepdims=True)
            rows = (x_rows, z_rows)[array]
            for tile in range(4):
                cols = slice(tile * 512, tile * 512 + 512)
                value = dot_nn(select, bufs[array][source, :, cols])
                if array == 1:
                    value = value * scale
                rows[source, :, :, cols] = value.astype(BF16).reshape(4, SLOT, 512)
            return carry

        lax.fori_loop(0, 2, one, 0)
        for step in range(2):
            source = pair_of(role, step)
            copy = pltpu.make_async_copy((x_rows, z_rows)[array].at[source], (xr_ref, zr_ref)[array].at[source], out_sem.at[array, role, step])
            copy.start()
            outs.append(copy)

    def relay_first(array):
        for part in range(2):
            got(array, part, 0)
            send(array, part, 1, me, second, own=True)
            send(array, part, 3, first, second)
            send(array, part, 4, first, partner)

    def relay_rest(array, part):
        got(array, part, 1)
        send(array, part, 5, second, partner)
        got(array, part, 3)
        send(array, part, 6, diag, partner)

    def activations(expert):
        rows = x_rows[:, expert].reshape(8 * SLOT, 2048)
        for which, (w_buf, act, out) in enumerate(((w1_buf, a_buf, a_ref), (w3_buf, b_buf, b_ref))):
            loads[expert * 2 + which].wait()
            act[:, expert] = dot_nn(rows, w_buf[expert]).astype(BF16).reshape(8, SLOT, 512)
            copy = pltpu.make_async_copy(act.at[:, expert], out.at[:, expert], act_sem.at[which, expert])
            copy.start()
            outs.append(copy)

    relay_first(0)
    for copy in meta:
        copy.wait_recv()
    got(0, 0, 2)
    got(0, 1, 2)
    pick(0, 0)
    got(0, 0, 4)
    got(0, 1, 4)
    pick(0, 1)
    for part in range(2):
        relay_rest(0, part)
        send(1, part, 0, me, first, own=True)
    got(1, 0, 2)
    got(1, 1, 2)
    pick(1, 0)
    for part in range(2):
        got(0, part, 5)
        got(0, part, 6)
    pick(0, 2)
    pick(0, 3)
    activations(0)
    relay_first(1)
    activations(1)
    got(1, 0, 4)
    got(1, 1, 4)
    pick(1, 1)
    activations(2)
    relay_rest(1, 0)
    activations(3)
    relay_rest(1, 1)
    for part in range(2):
        got(1, part, 5)
    pick(1, 2)
    for part in range(2):
        got(1, part, 6)
    pick(1, 3)
    for copy in copies.values():
        copy.wait_send()
    for copy in meta:
        copy.wait_send()
    for copy in outs:
        copy.wait()


def gather_rows(x_tokens, dy_tokens, code, gate, w_gate, w_up):
    tokens, width = x_tokens.shape
    experts, _, inner = w_gate.shape
    vmem = pl.BlockSpec(memory_space=pltpu.VMEM)
    hbm = pl.BlockSpec(memory_space=pl.ANY)
    rows = jax.ShapeDtypeStruct((8, experts, SLOT, width), BF16)
    acts = jax.ShapeDtypeStruct((8, experts, SLOT, inner), BF16)
    dma = pltpu.SemaphoreType.DMA
    return pl.pallas_call(
        gather_kernel,
        out_shape=(rows, rows, acts, acts, jax.ShapeDtypeStruct((8,) + code.shape, jnp.int32)),
        in_specs=[vmem] * 4 + [hbm] * 2,
        out_specs=(hbm, hbm, hbm, hbm, vmem),
        scratch_shapes=[
            pltpu.VMEM((8, tokens, width), BF16),
            pltpu.VMEM((8, tokens, width), BF16),
            pltpu.VMEM(rows.shape, BF16),
            pltpu.VMEM(rows.shape, BF16),
            pltpu.VMEM(w_gate.shape, BF16),
            pltpu.VMEM(w_up.shape, BF16),
            pltpu.VMEM(acts.shape, BF16),
            pltpu.VMEM(acts.shape, BF16),
            pltpu.VMEM((8,) + gate.shape, F32),
            dma((2, 2, 7)),
            dma((2, 2, 7)),
            dma((2, 7)),
            dma((2, 7)),
            dma((2, 4)),
            dma((2, 4, 2)),
            dma((2, 4)),
        ],
        compiler_params=pltpu.CompilerParams(collective_id=0, has_side_effects=True, vmem_limit_bytes=64000000),
        name='gather_rows',
    )(x_tokens, dy_tokens, code, gate, w_gate, w_up)


def middle_kernel(z_ref, a_ref, b_ref, code_ref, w1_ref, w3_ref, w2_ref, h_ref, da_ref, db_ref, give_ref, keep_ref, r_mine, r_send, r_got, picks, sums, send_sem, recv_sem, out_sem):
    me, core, first, second, diag, partner = places()
    other = 1 - core
    expert = pl.program_id(0)

    def swap(index):
        return remote(r_send.at[index], r_got.at[index], send_sem.at[index], recv_sem.at[index], partner)

    @pl.when(expert == 0)
    def _():
        barrier = pltpu.get_barrier_semaphore()
        pl.semaphore_signal(barrier, inc=1, device_id={'ep': partner}, device_id_type=MESH)

        def one(source, carry):
            picks[source, :, 0:256] = one_hot(code_ref[source], me * 256, 256).T.astype(BF16)
            picks[source, :, 256:512] = one_hot(code_ref[source], partner * 256, 256).T.astype(BF16)
            return carry

        lax.fori_loop(0, 8, one, 0)
        pl.semaphore_wait(barrier, 1)

    grad_hidden = dot_nt(z_ref[:, 0].reshape(512, 2048), w2_ref[0])
    hidden, d_gate, d_up = swiglu_parts(a_ref[:, 0].reshape(512, 512), b_ref[:, 0].reshape(512, 512), grad_hidden)
    h_ref[:, 0] = hidden.reshape(8, SLOT, 512)
    da_ref[:, 0] = d_gate.reshape(8, SLOT, 512)
    db_ref[:, 0] = d_up.reshape(8, SLOT, 512)

    def rows_back(dst, side):
        for tile in range(2):
            at = pl.ds(pl.multiple_of(side * 1024 + tile * 512, 512), 512)
            value = dot_nt(da_ref[:, 0].reshape(512, 512), w1_ref[0, at, :]) + dot_nt(db_ref[:, 0].reshape(512, 512), w3_ref[0, at, :])
            dst[expert, :, :, tile * 512:(tile + 1) * 512] = value.astype(BF16).reshape(8, SLOT, 512)

    rows_back(r_send, other)
    swap(expert).start()
    rows_back(r_mine, core)

    @pl.when(expert == 3)
    def _():
        for index in range(4):
            swap(index).wait_recv()
        outs = []
        for index, chip in enumerate((diag // 2, first // 2, second // 2, me // 2)):
            for which in range(2):
                source = chip * 2 + which
                pick = picks[source]
                sums[index, which] = dot_nn(pick[:, 0:256], r_mine[:, source].reshape(256, 1024)) + dot_nn(pick[:, 256:512], r_got[:, source].reshape(256, 1024))
            copy = pltpu.make_async_copy(sums.at[index], (give_ref, give_ref, keep_ref, keep_ref)[index].at[index % 2], out_sem.at[index])
            copy.start()
            outs.append(copy)
        for index in range(4):
            swap(index).wait_send()
        for copy in outs:
            copy.wait()


def middle(z_rows, act_gate, act_up, codes, w_gate, w_up, w_down):
    experts, width, inner = w_gate.shape
    tokens = codes.shape[2]
    by_expert = lambda e: (0, e, 0, 0)
    acts = pl.BlockSpec((8, 1, SLOT, inner), by_expert)
    act_shape = jax.ShapeDtypeStruct((8, experts, SLOT, inner), BF16)
    part = jax.ShapeDtypeStruct((2, 2, tokens, width // 2), F32)
    half = (experts, 8, SLOT, width // 2)
    dma = pltpu.SemaphoreType.DMA
    return pl.pallas_call(
        middle_kernel,
        grid=(experts,),
        out_shape=(act_shape, act_shape, act_shape, part, part),
        in_specs=[
            pl.BlockSpec((8, 1, SLOT, width), by_expert),
            acts,
            acts,
            pl.BlockSpec(memory_space=pltpu.VMEM),
            pl.BlockSpec((1, width, inner), lambda e: (e, 0, 0)),
            pl.BlockSpec((1, width, inner), lambda e: (e, 0, 0)),
            pl.BlockSpec((1, inner, width), lambda e: (e, 0, 0)),
        ],
        out_specs=(acts, acts, acts, pl.BlockSpec(memory_space=pl.ANY), pl.BlockSpec(memory_space=pl.ANY)),
        scratch_shapes=[
            pltpu.VMEM(half, BF16),
            pltpu.VMEM(half, BF16),
            pltpu.VMEM(half, BF16),
            pltpu.VMEM((8, tokens, 512), BF16),
            pltpu.VMEM((4, 2, tokens, width // 2), F32),
            dma((4,)),
            dma((4,)),
            dma((4,)),
        ],
        compiler_params=pltpu.CompilerParams(collective_id=1, has_side_effects=True, dimension_semantics=('arbitrary',), vmem_limit_bytes=64000000),
        name='middle',
    )(z_rows, act_gate, act_up, codes, w_gate, w_up, w_down)


TILES = 4


def weight_kernel(x_ref, z_ref, h_ref, da_ref, db_ref, dw1_ref, dw3_ref, dw2_ref, hidden_t):
    tile = pl.program_id(1)
    rows = 8 * SLOT

    @pl.when(tile == 0)
    def _():
        hidden_t[...] = h_ref[:, 0].reshape(rows, 512).T

    cols = pl.ds(pl.multiple_of(tile * 512, 512), 512)
    x_cols_t = x_ref[:, 0, :, cols].reshape(rows, 512).T
    dw1_ref[0] = dot_nn(x_cols_t, da_ref[:, 0].reshape(rows, 512))
    dw3_ref[0] = dot_nn(x_cols_t, db_ref[:, 0].reshape(rows, 512))
    dw2_ref[0] = dot_nn(hidden_t[...], z_ref[:, 0, :, cols].reshape(rows, 512))


def weight_grads(x_rows, z_rows, hidden, d_gate, d_up):
    _, experts, _, width = x_rows.shape
    inner = hidden.shape[3]
    by_expert = lambda e, t: (0, e, 0, 0)
    row_spec = pl.BlockSpec((8, 1, SLOT, width), by_expert)
    act_spec = pl.BlockSpec((8, 1, SLOT, inner), by_expert)
    return pl.pallas_call(
        weight_kernel,
        grid=(experts, TILES),
        out_shape=(
            jax.ShapeDtypeStruct((experts, width, inner), F32),
            jax.ShapeDtypeStruct((experts, width, inner), F32),
            jax.ShapeDtypeStruct((experts, inner, width), F32),
        ),
        in_specs=[row_spec, row_spec, act_spec, act_spec, act_spec],
        out_specs=(
            pl.BlockSpec((1, width // TILES, inner), lambda e, t: (e, t, 0)),
            pl.BlockSpec((1, width // TILES, inner), lambda e, t: (e, t, 0)),
            pl.BlockSpec((1, inner, width // TILES), lambda e, t: (e, 0, t)),
        ),
        scratch_shapes=[pltpu.VMEM((inner, 8 * SLOT), BF16)],
        compiler_params=pltpu.CompilerParams(dimension_semantics=('arbitrary', 'arbitrary'), vmem_limit_bytes=50000000),
        cost_estimate=pl.CostEstimate(flops=12_900_000_000, bytes_accessed=70_000_000, transcendentals=0),
        name='weight_grads',
    )(x_rows, z_rows, hidden, d_gate, d_up)


def shared_kernel(x_ref, dy_ref, w1_ref, w3_ref, w2_ref, dx_ref, dw1_ref, dw3_ref, dw2_ref, hidden_t, grad_gate, grad_up):
    tile = pl.program_id(0)

    @pl.when(tile == 0)
    def _():
        act_gate = dot_nn(x_ref[...], w1_ref[...]).astype(BF16)
        act_up = dot_nn(x_ref[...], w3_ref[...]).astype(BF16)
        hidden, d_gate, d_up = swiglu_parts(act_gate, act_up, dot_nt(dy_ref[...], w2_ref[...]))
        hidden_t[...] = hidden.T
        grad_gate[...] = d_gate
        grad_up[...] = d_up

    cols = pl.ds(pl.multiple_of(tile * 512, 512), 512)
    dx_ref[...] = dot_nt(grad_gate[...], w1_ref[cols, :]) + dot_nt(grad_up[...], w3_ref[cols, :])
    x_cols_t = x_ref[:, cols].T
    dw1_ref[0] = dot_nn(x_cols_t, grad_gate[...])
    dw3_ref[0] = dot_nn(x_cols_t, grad_up[...])
    dw2_ref[0] = dot_nn(hidden_t[...], dy_ref[:, cols])


def shared_backward(x_tokens, dy_tokens, shared_gate, shared_up, shared_down):
    tokens, width = x_tokens.shape
    inner = shared_gate.shape[1]
    vmem = pl.BlockSpec(memory_space=pltpu.VMEM)
    step = width // TILES
    return pl.pallas_call(
        shared_kernel,
        grid=(TILES,),
        out_shape=(
            jax.ShapeDtypeStruct((tokens, width), F32),
            jax.ShapeDtypeStruct((1, width, inner), F32),
            jax.ShapeDtypeStruct((1, width, inner), F32),
            jax.ShapeDtypeStruct((1, inner, width), F32),
        ),
        in_specs=[vmem] * 5,
        out_specs=(
            pl.BlockSpec((tokens, step), lambda t: (0, t)),
            pl.BlockSpec((1, step, inner), lambda t: (0, t, 0)),
            pl.BlockSpec((1, step, inner), lambda t: (0, t, 0)),
            pl.BlockSpec((1, inner, step), lambda t: (0, 0, t)),
        ),
        scratch_shapes=[
            pltpu.VMEM((inner, tokens), BF16),
            pltpu.VMEM((tokens, inner), BF16),
            pltpu.VMEM((tokens, inner), BF16),
        ],
        compiler_params=pltpu.CompilerParams(dimension_semantics=('arbitrary',), vmem_limit_bytes=40000000),
        cost_estimate=pl.CostEstimate(flops=6_000_000_000, bytes_accessed=20_000_000, transcendentals=0),
        name='shared_backward',
    )(x_tokens, dy_tokens, shared_gate, shared_up, shared_down)


def partners(kind):
    pairs = []
    for me in range(8):
        core = me % 2
        along_x, along_y = me ^ 2, me ^ 4
        first, second = (along_x, along_y) if core == 0 else (along_y, along_x)
        pairs.append((me, {'first': first, 'second': second, 'chip': me ^ 1}[kind]))
    return pairs


def solution(mesh):
    token_spec = P(('dp', 'ep'), None)
    expert_spec = P('ep', None, None)
    whole_spec = P(None, None)
    grad_spec = P(('dp', 'ep'), None, None)

    def local_backward(x_tokens, dy_tokens, expert_ids, gate_vals, slot_pos, w_gate, w_up, w_down, shared_gate, shared_up, shared_down):
        code = jnp.where(slot_pos >= 0, expert_ids * SLOT + slot_pos, -1)
        code = jnp.pad(code.T, ((0, 6), (0, 0)), constant_values=-1)
        gate = jnp.pad(gate_vals.T, ((0, 6), (0, 0)))
        x_rows, z_rows, act_gate, act_up, codes = gather_rows(x_tokens, dy_tokens, code, gate, w_gate, w_up)
        hidden, d_gate, d_up, give, keep = middle(z_rows, act_gate, act_up, codes, w_gate, w_up, w_down)
        got = lax.ppermute(give, 'ep', partners('first'))
        grad_w_gate, grad_w_up, grad_w_down = weight_grads(x_rows, z_rows, hidden, d_gate, d_up)
        onward = keep[0] + got[0]
        got_second = lax.ppermute(onward, 'ep', partners('second'))
        x_late, dy_late, _ = lax.optimization_barrier((x_tokens, dy_tokens, onward))
        shared_dx, grad_shared_gate, grad_shared_up, grad_shared_down = shared_backward(x_late, dy_late, shared_gate, shared_up, shared_down)
        mine = keep[1] + got[1] + got_second
        core = lax.rem(lax.axis_index('ep'), 2)
        swapped = lax.ppermute(lax.dynamic_index_in_dim(mine, 1 - core, 0, keepdims=False), 'ep', partners('chip'))
        own = lax.dynamic_index_in_dim(mine, core, 0, keepdims=False)
        left = jnp.where(core == 0, own, swapped)
        right = jnp.where(core == 0, swapped, own)
        grad_x = (jnp.concatenate((left, right), axis=1) + shared_dx).astype(BF16)
        return grad_x, grad_w_gate, grad_w_up, grad_w_down, grad_shared_gate, grad_shared_up, grad_shared_down

    return jax.shard_map(local_backward, mesh=mesh, in_specs=(token_spec, token_spec, token_spec, token_spec, token_spec, expert_spec, expert_spec, expert_spec, whole_spec, whole_spec, whole_spec), out_specs=(token_spec, grad_spec, grad_spec, grad_spec, grad_spec, grad_spec, grad_spec), check_vma=False)
```

```python
import jax
import jax.numpy as jnp
from jax import lax
from jax.experimental import pallas as pl
from jax.experimental.pallas import tpu as pltpu
from jax.sharding import PartitionSpec as P

MESH = pl.DeviceIdType.MESH
SLOT = 64
BF16 = jnp.bfloat16
F32 = jnp.float32


def swiglu_parts(act_gate, act_up, grad_hidden):
    gate_f32 = act_gate.astype(F32)
    up_f32 = act_up.astype(F32)
    sigma = jax.nn.sigmoid(gate_f32)
    silu_gate = gate_f32 * sigma
    hidden = (silu_gate * up_f32).astype(BF16)
    grad_gate = (grad_hidden * up_f32 * sigma * (1.0 + gate_f32 * (1.0 - sigma))).astype(BF16)
    grad_up = (grad_hidden * silu_gate).astype(BF16)
    return hidden, grad_gate, grad_up


def dot_nn(a, b):
    return lax.dot_general(a, b, (((1,), (0,)), ((), ())), preferred_element_type=F32)


def dot_nt(a, b):
    return lax.dot_general(a, b, (((1,), (1,)), ((), ())), preferred_element_type=F32)


def dot_tn(a, b):
    return lax.dot_general(a, b, (((0,), (0,)), ((), ())), preferred_element_type=F32)


def places():
    me = lax.axis_index('ep')
    core = lax.rem(me, 2)
    flip_x = 2 - 4 * lax.rem(me // 2, 2)
    flip_y = 4 - 8 * (me // 4)
    first = me + flip_x * (1 - core) + flip_y * core
    second = me + flip_y * (1 - core) + flip_x * core
    diag = me + flip_x + flip_y
    partner = me + 1 - 2 * core
    return me, core, first, second, diag, partner


def remote(src, dst, send_sem, recv_sem, device):
    return pltpu.make_async_remote_copy(src_ref=src, dst_ref=dst, send_sem=send_sem, recv_sem=recv_sem, device_id={'ep': device}, device_id_type=MESH)


def pair_of(role, step):
    me, core, first, second, diag, partner = places()
    other = 1 - core
    if role == 0:
        return me * (1 - step) + partner * step
    if role == 1:
        return first * (1 - step) + ((second // 2) * 2 + other) * step
    if role == 2:
        return second * (1 - step) + ((first // 2) * 2 + other) * step
    return diag * (1 - step) + ((diag // 2) * 2 + other) * step


def one_hot(code, base, rows):
    slot = lax.broadcasted_iota(jnp.int32, (rows, 128), 0) + base
    hits = jnp.zeros((rows, 128), F32)
    for choice in range(10):
        hits = jnp.where(slot == code[choice:choice + 1, :], 1.0, hits)
    return hits


def gather_kernel(x_ref, dy_ref, code_ref, gate_ref, w1_ref, w3_ref, xr_ref, zr_ref, a_ref, b_ref, codeg_ref, xbuf, dybuf, x_rows, z_rows, w1_buf, w3_buf, a_buf, b_buf, gateg, send_sem, recv_sem, meta_send, meta_recv, load_sem, out_sem, act_sem):
    me, core, first, second, diag, partner = places()
    loads = []
    for expert in range(4):
        for which, (src, dst) in enumerate(((w1_ref, w1_buf), (w3_ref, w3_buf))):
            copy = pltpu.make_async_copy(src.at[expert], dst.at[expert], load_sem.at[which, expert])
            copy.start()
            loads.append(copy)
    barrier = pltpu.get_barrier_semaphore()
    for step in range(1, 8):
        pl.semaphore_signal(barrier, inc=1, device_id={'ep': lax.rem(me + step, 8)}, device_id_type=MESH)
    pl.semaphore_wait(barrier, 7)

    half = 64
    srcs = (x_ref, dy_ref)
    bufs = (xbuf, dybuf)
    copies = {}

    def send(array, part, kind, block, device, own=False):
        rows = pl.ds(part * half, half)
        src = srcs[array].at[rows] if own else bufs[array].at[block, rows]
        copy = remote(src, bufs[array].at[block, rows], send_sem.at[array, part, kind], recv_sem.at[array, part, kind], device)
        copy.start()
        copies[array, part, kind] = copy

    def got(array, part, kind):
        copies[array, part, kind].wait_recv()

    for part in range(2):
        send(0, part, 0, me, first, own=True)
    meta = []
    for step in range(1, 8):
        peer = lax.rem(me + step, 8)
        for which, (src, dst) in enumerate(((code_ref, codeg_ref), (gate_ref, gateg))):
            copy = remote(src, dst.at[me], meta_send.at[which, step - 1], meta_recv.at[which, step - 1], peer)
            copy.start()
            meta.append(copy)
    for array in range(2):
        for part in range(2):
            send(array, part, 2, me, partner, own=True)
    codeg_ref[me] = code_ref[...]
    gateg[me] = gate_ref[...]
    xbuf[me] = x_ref[...]
    dybuf[me] = dy_ref[...]

    outs = []

    def pick(array, role):
        def one(step, carry):
            source = pair_of(role, step)
            hits = one_hot(codeg_ref[source], me * 256, 256)
            select = hits.astype(BF16)
            if array == 1:
                slot = lax.broadcasted_iota(jnp.int32, (256, 128), 0) + me * 256
                gates = jnp.zeros((256, 128), F32)
                for choice in range(10):
                    gates = jnp.where(slot == codeg_ref[source, choice:choice + 1, :], gateg[source, choice:choice + 1, :], gates)
                scale = jnp.sum(gates, axis=1, keepdims=True)
            rows = (x_rows, z_rows)[array]
            for tile in range(4):
                cols = slice(tile * 512, tile * 512 + 512)
                value = dot_nn(select, bufs[array][source, :, cols])
                if array == 1:
                    value = value * scale
                rows[source, :, :, cols] = value.astype(BF16).reshape(4, SLOT, 512)
            return carry

        lax.fori_loop(0, 2, one, 0)
        for step in range(2):
            source = pair_of(role, step)
            copy = pltpu.make_async_copy((x_rows, z_rows)[array].at[source], (xr_ref, zr_ref)[array].at[source], out_sem.at[array, role, step])
            copy.start()
            outs.append(copy)

    def relay_first(array):
        for part in range(2):
            got(array, part, 0)
            send(array, part, 1, me, second, own=True)
            send(array, part, 3, first, second)
            send(array, part, 4, first, partner)

    def relay_rest(array, part):
        got(array, part, 1)
        send(array, part, 5, second, partner)
        got(array, part, 3)
        send(array, part, 6, diag, partner)

    def activations(expert):
        rows = x_rows[:, expert].reshape(8 * SLOT, 2048)
        for which, (w_buf, act, out) in enumerate(((w1_buf, a_buf, a_ref), (w3_buf, b_buf, b_ref))):
            loads[expert * 2 + which].wait()
            act[:, expert] = dot_nn(rows, w_buf[expert]).astype(BF16).reshape(8, SLOT, 512)
            copy = pltpu.make_async_copy(act.at[:, expert], out.at[:, expert], act_sem.at[which, expert])
            copy.start()
            outs.append(copy)

    relay_first(0)
    for copy in meta:
        copy.wait_recv()
    got(0, 0, 2)
    got(0, 1, 2)
    pick(0, 0)
    got(0, 0, 4)
    got(0, 1, 4)
    pick(0, 1)
    for part in range(2):
        relay_rest(0, part)
        send(1, part, 0, me, first, own=True)
    got(1, 0, 2)
    got(1, 1, 2)
    pick(1, 0)
    for part in range(2):
        got(0, part, 5)
        got(0, part, 6)
    pick(0, 2)
    pick(0, 3)
    activations(0)
    relay_first(1)
    activations(1)
    got(1, 0, 4)
    got(1, 1, 4)
    pick(1, 1)
    activations(2)
    relay_rest(1, 0)
    activations(3)
    relay_rest(1, 1)
    for part in range(2):
        got(1, part, 5)
    pick(1, 2)
    for part in range(2):
        got(1, part, 6)
    pick(1, 3)
    for copy in copies.values():
        copy.wait_send()
    for copy in meta:
        copy.wait_send()
    for copy in outs:
        copy.wait()


def gather_rows(x_tokens, dy_tokens, code, gate, w_gate, w_up):
    tokens, width = x_tokens.shape
    experts, _, inner = w_gate.shape
    vmem = pl.BlockSpec(memory_space=pltpu.VMEM)
    hbm = pl.BlockSpec(memory_space=pl.ANY)
    rows = jax.ShapeDtypeStruct((8, experts, SLOT, width), BF16)
    acts = jax.ShapeDtypeStruct((8, experts, SLOT, inner), BF16)
    dma = pltpu.SemaphoreType.DMA
    return pl.pallas_call(
        gather_kernel,
        out_shape=(rows, rows, acts, acts, jax.ShapeDtypeStruct((8,) + code.shape, jnp.int32)),
        in_specs=[vmem] * 4 + [hbm] * 2,
        out_specs=(hbm, hbm, hbm, hbm, vmem),
        scratch_shapes=[
            pltpu.VMEM((8, tokens, width), BF16),
            pltpu.VMEM((8, tokens, width), BF16),
            pltpu.VMEM(rows.shape, BF16),
            pltpu.VMEM(rows.shape, BF16),
            pltpu.VMEM(w_gate.shape, BF16),
            pltpu.VMEM(w_up.shape, BF16),
            pltpu.VMEM(acts.shape, BF16),
            pltpu.VMEM(acts.shape, BF16),
            pltpu.VMEM((8,) + gate.shape, F32),
            dma((2, 2, 7)),
            dma((2, 2, 7)),
            dma((2, 7)),
            dma((2, 7)),
            dma((2, 4)),
            dma((2, 4, 2)),
            dma((2, 4)),
        ],
        compiler_params=pltpu.CompilerParams(collective_id=0, has_side_effects=True, vmem_limit_bytes=64000000),
        name='gather_rows',
    )(x_tokens, dy_tokens, code, gate, w_gate, w_up)


def middle_kernel(z_ref, a_ref, b_ref, code_ref, w1_ref, w3_ref, w2_ref, h_ref, da_ref, db_ref, give_ref, keep_ref, r_mine, r_send, r_got, picks, sums, send_sem, recv_sem, out_sem):
    me, core, first, second, diag, partner = places()
    other = 1 - core
    expert = pl.program_id(0)

    def swap(index):
        return remote(r_send.at[index], r_got.at[index], send_sem.at[index], recv_sem.at[index], partner)

    @pl.when(expert == 0)
    def _():
        barrier = pltpu.get_barrier_semaphore()
        pl.semaphore_signal(barrier, inc=1, device_id={'ep': partner}, device_id_type=MESH)

        def one(source, carry):
            picks[source, :, 0:256] = one_hot(code_ref[source], me * 256, 256).T.astype(BF16)
            picks[source, :, 256:512] = one_hot(code_ref[source], partner * 256, 256).T.astype(BF16)
            return carry

        lax.fori_loop(0, 8, one, 0)
        pl.semaphore_wait(barrier, 1)

    grad_hidden = dot_nt(z_ref[:, 0].reshape(512, 2048), w2_ref[0])
    hidden, d_gate, d_up = swiglu_parts(a_ref[:, 0].reshape(512, 512), b_ref[:, 0].reshape(512, 512), grad_hidden)
    h_ref[:, 0] = hidden.reshape(8, SLOT, 512)
    da_ref[:, 0] = d_gate.reshape(8, SLOT, 512)
    db_ref[:, 0] = d_up.reshape(8, SLOT, 512)

    def rows_back(dst, side):
        for tile in range(2):
            at = pl.ds(pl.multiple_of(side * 1024 + tile * 512, 512), 512)
            value = dot_nt(da_ref[:, 0].reshape(512, 512), w1_ref[0, at, :]) + dot_nt(db_ref[:, 0].reshape(512, 512), w3_ref[0, at, :])
            dst[expert, :, :, tile * 512:(tile + 1) * 512] = value.astype(BF16).reshape(8, SLOT, 512)

    rows_back(r_send, other)
    swap(expert).start()
    rows_back(r_mine, core)

    @pl.when(expert == 3)
    def _():
        for index in range(4):
            swap(index).wait_recv()
        outs = []
        for index, chip in enumerate((diag // 2, first // 2, second // 2, me // 2)):
            for which in range(2):
                source = chip * 2 + which
                pick = picks[source]
                sums[index, which] = dot_nn(pick[:, 0:256], r_mine[:, source].reshape(256, 1024)) + dot_nn(pick[:, 256:512], r_got[:, source].reshape(256, 1024))
            copy = pltpu.make_async_copy(sums.at[index], (give_ref, give_ref, keep_ref, keep_ref)[index].at[index % 2], out_sem.at[index])
            copy.start()
            outs.append(copy)
        for index in range(4):
            swap(index).wait_send()
        for copy in outs:
            copy.wait()


def middle(z_rows, act_gate, act_up, codes, w_gate, w_up, w_down):
    experts, width, inner = w_gate.shape
    tokens = codes.shape[2]
    by_expert = lambda e: (0, e, 0, 0)
    acts = pl.BlockSpec((8, 1, SLOT, inner), by_expert)
    act_shape = jax.ShapeDtypeStruct((8, experts, SLOT, inner), BF16)
    part = jax.ShapeDtypeStruct((2, 2, tokens, width // 2), F32)
    half = (experts, 8, SLOT, width // 2)
    dma = pltpu.SemaphoreType.DMA
    return pl.pallas_call(
        middle_kernel,
        grid=(experts,),
        out_shape=(act_shape, act_shape, act_shape, part, part),
        in_specs=[
            pl.BlockSpec((8, 1, SLOT, width), by_expert),
            acts,
            acts,
            pl.BlockSpec(memory_space=pltpu.VMEM),
            pl.BlockSpec((1, width, inner), lambda e: (e, 0, 0)),
            pl.BlockSpec((1, width, inner), lambda e: (e, 0, 0)),
            pl.BlockSpec((1, inner, width), lambda e: (e, 0, 0)),
        ],
        out_specs=(acts, acts, acts, pl.BlockSpec(memory_space=pl.ANY), pl.BlockSpec(memory_space=pl.ANY)),
        scratch_shapes=[
            pltpu.VMEM(half, BF16),
            pltpu.VMEM(half, BF16),
            pltpu.VMEM(half, BF16),
            pltpu.VMEM((8, tokens, 512), BF16),
            pltpu.VMEM((4, 2, tokens, width // 2), F32),
            dma((4,)),
            dma((4,)),
            dma((4,)),
        ],
        compiler_params=pltpu.CompilerParams(collective_id=1, has_side_effects=True, dimension_semantics=('arbitrary',), vmem_limit_bytes=64000000),
        name='middle',
    )(z_rows, act_gate, act_up, codes, w_gate, w_up, w_down)


TILES = 4


def weight_kernel(x_ref, z_ref, h_ref, da_ref, db_ref, dw1_ref, dw3_ref, dw2_ref, hidden_t):
    tile = pl.program_id(1)
    rows = 8 * SLOT

    @pl.when(tile == 0)
    def _():
        hidden_t[...] = h_ref[:, 0].reshape(rows, 512).T

    cols = pl.ds(pl.multiple_of(tile * 512, 512), 512)
    x_cols_t = x_ref[:, 0, :, cols].reshape(rows, 512).T
    dw1_ref[0] = dot_nn(x_cols_t, da_ref[:, 0].reshape(rows, 512))
    dw3_ref[0] = dot_nn(x_cols_t, db_ref[:, 0].reshape(rows, 512))
    dw2_ref[0] = dot_nn(hidden_t[...], z_ref[:, 0, :, cols].reshape(rows, 512))


def weight_grads(x_rows, z_rows, hidden, d_gate, d_up):
    _, experts, _, width = x_rows.shape
    inner = hidden.shape[3]
    by_expert = lambda e, t: (0, e, 0, 0)
    row_spec = pl.BlockSpec((8, 1, SLOT, width), by_expert)
    act_spec = pl.BlockSpec((8, 1, SLOT, inner), by_expert)
    return pl.pallas_call(
        weight_kernel,
        grid=(experts, TILES),
        out_shape=(
            jax.ShapeDtypeStruct((experts, width, inner), F32),
            jax.ShapeDtypeStruct((experts, width, inner), F32),
            jax.ShapeDtypeStruct((experts, inner, width), F32),
        ),
        in_specs=[row_spec, row_spec, act_spec, act_spec, act_spec],
        out_specs=(
            pl.BlockSpec((1, width // TILES, inner), lambda e, t: (e, t, 0)),
            pl.BlockSpec((1, width // TILES, inner), lambda e, t: (e, t, 0)),
            pl.BlockSpec((1, inner, width // TILES), lambda e, t: (e, 0, t)),
        ),
        scratch_shapes=[pltpu.VMEM((inner, 8 * SLOT), BF16)],
        compiler_params=pltpu.CompilerParams(dimension_semantics=('arbitrary', 'arbitrary'), vmem_limit_bytes=50000000),
        cost_estimate=pl.CostEstimate(flops=12_900_000_000, bytes_accessed=70_000_000, transcendentals=0),
        name='weight_grads',
    )(x_rows, z_rows, hidden, d_gate, d_up)


def shared_kernel(x_ref, dy_ref, w1_ref, w3_ref, w2_ref, dx_ref, dw1_ref, dw3_ref, dw2_ref, hidden_t, grad_gate, grad_up):
    tile = pl.program_id(0)

    @pl.when(tile == 0)
    def _():
        act_gate = dot_nn(x_ref[...], w1_ref[...]).astype(BF16)
        act_up = dot_nn(x_ref[...], w3_ref[...]).astype(BF16)
        hidden, d_gate, d_up = swiglu_parts(act_gate, act_up, dot_nt(dy_ref[...], w2_ref[...]))
        hidden_t[...] = hidden.T
        grad_gate[...] = d_gate
        grad_up[...] = d_up

    cols = pl.ds(pl.multiple_of(tile * 512, 512), 512)
    dx_ref[...] = dot_nt(grad_gate[...], w1_ref[cols, :]) + dot_nt(grad_up[...], w3_ref[cols, :])
    x_cols_t = x_ref[:, cols].T
    dw1_ref[0] = dot_nn(x_cols_t, grad_gate[...])
    dw3_ref[0] = dot_nn(x_cols_t, grad_up[...])
    dw2_ref[0] = dot_nn(hidden_t[...], dy_ref[:, cols])


def shared_backward(x_tokens, dy_tokens, shared_gate, shared_up, shared_down):
    tokens, width = x_tokens.shape
    inner = shared_gate.shape[1]
    vmem = pl.BlockSpec(memory_space=pltpu.VMEM)
    step = width // TILES
    return pl.pallas_call(
        shared_kernel,
        grid=(TILES,),
        out_shape=(
            jax.ShapeDtypeStruct((tokens, width), F32),
            jax.ShapeDtypeStruct((1, width, inner), F32),
            jax.ShapeDtypeStruct((1, width, inner), F32),
            jax.ShapeDtypeStruct((1, inner, width), F32),
        ),
        in_specs=[vmem] * 5,
        out_specs=(
            pl.BlockSpec((tokens, step), lambda t: (0, t)),
            pl.BlockSpec((1, step, inner), lambda t: (0, t, 0)),
            pl.BlockSpec((1, step, inner), lambda t: (0, t, 0)),
            pl.BlockSpec((1, inner, step), lambda t: (0, 0, t)),
        ),
        scratch_shapes=[
            pltpu.VMEM((inner, tokens), BF16),
            pltpu.VMEM((tokens, inner), BF16),
            pltpu.VMEM((tokens, inner), BF16),
        ],
        compiler_params=pltpu.CompilerParams(dimension_semantics=('arbitrary',), vmem_limit_bytes=40000000),
        cost_estimate=pl.CostEstimate(flops=6_000_000_000, bytes_accessed=20_000_000, transcendentals=0),
        name='shared_backward',
    )(x_tokens, dy_tokens, shared_gate, shared_up, shared_down)


def partners(kind):
    pairs = []
    for me in range(8):
        core = me % 2
        along_x, along_y = me ^ 2, me ^ 4
        first, second = (along_x, along_y) if core == 0 else (along_y, along_x)
        pairs.append((me, {'first': first, 'second': second, 'chip': me ^ 1}[kind]))
    return pairs


def solution(mesh):
    token_spec = P(('dp', 'ep'), None)
    expert_spec = P('ep', None, None)
    whole_spec = P(None, None)
    grad_spec = P(('dp', 'ep'), None, None)

    def local_backward(x_tokens, dy_tokens, expert_ids, gate_vals, slot_pos, w_gate, w_up, w_down, shared_gate, shared_up, shared_down):
        code = jnp.where(slot_pos >= 0, expert_ids * SLOT + slot_pos, -1)
        code = jnp.pad(code.T, ((0, 6), (0, 0)), constant_values=-1)
        gate = jnp.pad(gate_vals.T, ((0, 6), (0, 0)))
        x_rows, z_rows, act_gate, act_up, codes = gather_rows(x_tokens, dy_tokens, code, gate, w_gate, w_up)
        hidden, d_gate, d_up, give, keep = middle(z_rows, act_gate, act_up, codes, w_gate, w_up, w_down)
        got = lax.ppermute(give, 'ep', partners('first'))
        grads = weight_grads(x_rows, z_rows, hidden, d_gate, d_up)
        got, grad_w_gate, grad_w_up, grad_w_down = lax.optimization_barrier((got,) + tuple(grads))
        onward = keep[0] + got[0]
        got_second = lax.ppermute(onward, 'ep', partners('second'))
        x_late, dy_late, _ = lax.optimization_barrier((x_tokens, dy_tokens, onward))
        shared_dx, grad_shared_gate, grad_shared_up, grad_shared_down = shared_backward(x_late, dy_late, shared_gate, shared_up, shared_down)
        got_second, shared_dx = lax.optimization_barrier((got_second, shared_dx))
        mine = keep[1] + got[1] + got_second
        core = lax.rem(lax.axis_index('ep'), 2)
        swapped = lax.ppermute(lax.dynamic_index_in_dim(mine, 1 - core, 0, keepdims=False), 'ep', partners('chip'))
        own = lax.dynamic_index_in_dim(mine, core, 0, keepdims=False)
        left = jnp.where(core == 0, own, swapped)
        right = jnp.where(core == 0, swapped, own)
        grad_x = (jnp.concatenate((left, right), axis=1) + shared_dx).astype(BF16)
        return grad_x, grad_w_gate, grad_w_up, grad_w_down, grad_shared_gate, grad_shared_up, grad_shared_down

    return jax.shard_map(local_backward, mesh=mesh, in_specs=(token_spec, token_spec, token_spec, token_spec, token_spec, expert_spec, expert_spec, expert_spec, whole_spec, whole_spec, whole_spec), out_specs=(token_spec, grad_spec, grad_spec, grad_spec, grad_spec, grad_spec, grad_spec), check_vma=False)
```

```python
import jax
import jax.numpy as jnp
from jax import lax
from jax.experimental import pallas as pl
from jax.experimental.pallas import tpu as pltpu
from jax.sharding import PartitionSpec as P

MESH = pl.DeviceIdType.MESH
SLOT = 64
BF16 = jnp.bfloat16
F32 = jnp.float32


def swiglu_parts(act_gate, act_up, grad_hidden):
    gate_f32 = act_gate.astype(F32)
    up_f32 = act_up.astype(F32)
    sigma = jax.nn.sigmoid(gate_f32)
    silu_gate = gate_f32 * sigma
    hidden = (silu_gate * up_f32).astype(BF16)
    grad_gate = (grad_hidden * up_f32 * sigma * (1.0 + gate_f32 * (1.0 - sigma))).astype(BF16)
    grad_up = (grad_hidden * silu_gate).astype(BF16)
    return hidden, grad_gate, grad_up


def dot_nn(a, b):
    return lax.dot_general(a, b, (((1,), (0,)), ((), ())), preferred_element_type=F32)


def dot_nt(a, b):
    return lax.dot_general(a, b, (((1,), (1,)), ((), ())), preferred_element_type=F32)


def dot_tn(a, b):
    return lax.dot_general(a, b, (((0,), (0,)), ((), ())), preferred_element_type=F32)


def places():
    me = lax.axis_index('ep')
    core = lax.rem(me, 2)
    flip_x = 2 - 4 * lax.rem(me // 2, 2)
    flip_y = 4 - 8 * (me // 4)
    first = me + flip_x * (1 - core) + flip_y * core
    second = me + flip_y * (1 - core) + flip_x * core
    diag = me + flip_x + flip_y
    partner = me + 1 - 2 * core
    return me, core, first, second, diag, partner


def remote(src, dst, send_sem, recv_sem, device):
    return pltpu.make_async_remote_copy(src_ref=src, dst_ref=dst, send_sem=send_sem, recv_sem=recv_sem, device_id={'ep': device}, device_id_type=MESH)


def one_hot(code, base, rows):
    slot = lax.broadcasted_iota(jnp.int32, (rows, 128), 0) + base
    hits = jnp.zeros((rows, 128), F32)
    for choice in range(10):
        hits = jnp.where(slot == code[choice:choice + 1, :], 1.0, hits)
    return hits


SEEN_AS = {1: 1, 2: 2, 3: 5, 4: 4, 5: 3, 6: 6, 7: 7}
PART = 64


def rows_kernel(x_ref, dy_ref, code_ref, gate_ref, w1_ref, w3_ref, w2_ref, xr_ref, zr_ref, h_ref, da_ref, db_ref, give_ref, keep_ref, xbuf, dybuf, codes, gates, picks, picks_partner, x_rows, z_rows, w1_buf, w3_buf, w2_buf, acts, grads, r_send, r_mine, r_got, sums, own_sem, send_sem, recv_sem, meta_send, meta_recv, load_sem, rows_sem, grads_sem, swap_send, swap_recv, sums_sem):
    me, core, first, second, diag, partner = places()
    other = 1 - core
    bufs = (xbuf, dybuf)

    def own(which):
        src, dst = ((x_ref, xbuf.at[0]), (dy_ref, dybuf.at[0]), (code_ref, codes.at[0]), (gate_ref, gates.at[0]))[which]
        return pltpu.make_async_copy(src, dst, own_sem.at[which])

    def load(which, expert):
        src, dst = ((w1_ref, w1_buf), (w3_ref, w3_buf), (w2_ref, w2_buf))[which]
        return pltpu.make_async_copy(src.at[expert], dst.at[expert], load_sem.at[which, expert])

    def trip(array, part, kind):
        src, dst, device = ((0, 2, first), (0, 4, second), (0, 1, partner), (2, 6, second), (2, 3, partner), (4, 5, partner), (6, 7, partner))[kind]
        rows = pl.ds(part * PART, PART)
        return remote(bufs[array].at[src, rows], bufs[array].at[dst, rows], send_sem.at[array, part, kind], recv_sem.at[array, part, kind], device)

    def meta(which, role):
        device = {1: partner, 2: first, 3: (second // 2) * 2 + other, 4: second, 5: (first // 2) * 2 + other, 6: diag, 7: (diag // 2) * 2 + other}[role]
        table = (codes, gates)[which]
        seen = SEEN_AS[role]
        return remote(table.at[0], table.at[seen], meta_send.at[which, role - 1], meta_recv.at[which, seen - 1], device)

    def relay_first(array, part):
        trip(array, part, 0).wait_recv()
        trip(array, part, 1).start()
        trip(array, part, 3).start()
        trip(array, part, 4).start()

    def relay_rest(array, part):
        trip(array, part, 1).wait_recv()
        trip(array, part, 5).start()
        trip(array, part, 3).wait_recv()
        trip(array, part, 6).start()

    def arrived(array, kind):
        for part in range(2):
            trip(array, part, kind).wait_recv()

    def rows_out(array, half, at):
        return pltpu.make_async_copy((x_rows, z_rows)[array].at[at], (xr_ref, zr_ref)[array].at[half, at], rows_sem.at[array, half, at])

    def pick_x(half, low, high):
        def one(at, carry):
            role = half * 4 + at
            select = one_hot(codes[role], me * 256, 256).astype(BF16)
            picks[role] = select
            picks_partner[role] = one_hot(codes[role], partner * 256, 256).astype(BF16)
            for tile in range(4):
                cols = slice(tile * 512, tile * 512 + 512)
                x_rows[at, :, :, cols] = dot_nn(select, xbuf[role, :, cols]).astype(BF16).reshape(4, SLOT, 512)
            rows_out(0, half, at).start()
            return carry

        lax.fori_loop(low, high, one, 0)

    def pick_z(half, low, high):
        def one(at, carry):
            role = half * 4 + at
            slot = lax.broadcasted_iota(jnp.int32, (256, 128), 0) + me * 256
            spread = jnp.zeros((256, 128), F32)
            for choice in range(10):
                spread = jnp.where(slot == codes[role, choice:choice + 1, :], gates[role, choice:choice + 1, :], spread)
            scale = jnp.sum(spread, axis=1, keepdims=True)
            select = picks[role]
            for tile in range(4):
                cols = slice(tile * 512, tile * 512 + 512)
                value = dot_nn(select, dybuf[role, :, cols]) * scale
                z_rows[at, :, :, cols] = value.astype(BF16).reshape(4, SLOT, 512)
            rows_out(1, half, at).start()
            return carry

        lax.fori_loop(low, high, one, 0)

    def activations(half, after):
        def one(expert, carry):
            if half == 0:
                load(0, expert).wait()
                load(1, expert).wait()
            rows = x_rows[:, expert].reshape(4 * SLOT, 2048)
            acts[0, half, expert] = dot_nn(rows, w1_buf[expert]).astype(BF16)
            acts[1, half, expert] = dot_nn(rows, w3_buf[expert]).astype(BF16)
            for step, action in after.items():
                pl.when(expert == step)(action)
            return carry

        lax.fori_loop(0, 4, one, 0)

    def grads_out(which, half, expert):
        return pltpu.make_async_copy(grads.at[which, expert], (h_ref, da_ref, db_ref)[which].at[half, :, expert], grads_sem.at[which, half, expert])

    def swap(half, expert):
        return remote(r_send.at[expert], r_got.at[half, expert], swap_send.at[half, expert], swap_recv.at[half, expert], partner)

    def back(half, after):
        def one(expert, carry):
            if half == 0:
                load(2, expert).wait()
            grad_hidden = dot_nt(z_rows[:, expert].reshape(4 * SLOT, 2048), w2_buf[expert])
            parts = swiglu_parts(acts[0, half, expert], acts[1, half, expert], grad_hidden)
            for which in range(3):
                if half == 1:
                    grads_out(which, 0, expert).wait()
                grads[which, expert] = parts[which].reshape(4, SLOT, 512)
                grads_out(which, half, expert).start()
            d_gate, d_up = parts[1], parts[2]

            def rows_back(side, tile):
                at = pl.ds(pl.multiple_of(side * 1024 + tile * 512, 512), 512)
                value = dot_nt(d_gate, w1_buf[expert, at, :]) + dot_nt(d_up, w3_buf[expert, at, :])
                return value.astype(BF16).reshape(4, SLOT, 512)

            if half == 1:
                swap(0, expert).wait_send()
            for tile in range(2):
                r_send[expert, :, :, tile * 512:(tile + 1) * 512] = rows_back(other, tile)
            swap(half, expert).start()
            for tile in range(2):
                r_mine[half, expert, :, :, tile * 512:(tile + 1) * 512] = rows_back(core, tile)
            for step, action in after.items():
                pl.when(expert == step)(action)
            return carry

        lax.fori_loop(0, 4, one, 0)

    def sums_out(role):
        ref, index, which = {6: (give_ref, 0, 0), 7: (give_ref, 0, 1), 2: (give_ref, 1, 0), 5: (give_ref, 1, 1), 4: (keep_ref, 0, 0), 3: (keep_ref, 0, 1), 0: (keep_ref, 1, 0), 1: (keep_ref, 1, 1)}[role]
        return pltpu.make_async_copy(sums.at[role % 4], ref.at[index, which], sums_sem.at[role])

    def total(half):
        for expert in range(4):
            swap(half, expert).wait_recv()
        for at in range(4):
            role = half * 4 + at
            if half == 1:
                sums_out(at).wait()
            sums[at] = dot_tn(picks[role], r_mine[half, :, at].reshape(256, 1024)) + dot_tn(picks_partner[role], r_got[half, :, at ^ 1].reshape(256, 1024))
            sums_out(role).start()

    for which in range(4):
        own(which).start()
    for expert in range(4):
        load(0, expert).start()
        load(1, expert).start()
    for expert in range(4):
        load(2, expert).start()
    barrier = pltpu.get_barrier_semaphore()
    for step in range(1, 8):
        pl.semaphore_signal(barrier, inc=1, device_id={'ep': lax.rem(me + step, 8)}, device_id_type=MESH)
    own(0).wait()
    own(1).wait()
    own(2).wait()
    own(3).wait()
    pl.semaphore_wait(barrier, 7)

    for part in range(2):
        trip(0, part, 0).start()
    for array in range(2):
        for part in range(2):
            trip(array, part, 2).start()
    for role in range(1, 8):
        for which in range(2):
            meta(which, role).start()

    relay_first(0, 0)
    for role in range(1, 8):
        for which in range(2):
            meta(which, role).wait_recv()
    arrived(0, 2)
    pick_x(0, 0, 2)
    relay_first(0, 1)
    arrived(0, 4)
    pick_x(0, 2, 4)

    def rest_x(part):
        relay_rest(0, part)
        trip(1, part, 0).start()

    activations(0, {1: lambda: rest_x(0)})
    arrived(1, 2)
    pick_z(0, 0, 2)
    rest_x(1)
    for at in range(4):
        rows_out(0, 0, at).wait()
    arrived(0, 5)
    pick_x(1, 0, 2)
    arrived(0, 6)
    pick_x(1, 2, 4)
    relay_first(1, 0)
    activations(1, {0: lambda: relay_first(1, 1)})
    arrived(1, 4)
    pick_z(0, 2, 4)
    back(0, {0: lambda: relay_rest(1, 0), 2: lambda: relay_rest(1, 1)})
    total(0)
    for at in range(4):
        rows_out(1, 0, at).wait()
    arrived(1, 5)
    pick_z(1, 0, 2)
    arrived(1, 6)
    pick_z(1, 2, 4)
    back(1, {})
    total(1)

    for array in range(2):
        for part in range(2):
            for kind in range(7):
                trip(array, part, kind).wait_send()
    for role in range(1, 8):
        for which in range(2):
            meta(which, role).wait_send()
    for expert in range(4):
        swap(1, expert).wait_send()
        for which in range(3):
            grads_out(which, 1, expert).wait()
    for at in range(4):
        rows_out(0, 1, at).wait()
        rows_out(1, 1, at).wait()
        sums_out(4 + at).wait()


def rows_backward(x_tokens, dy_tokens, code, gate, w_gate, w_up, w_down):
    tokens, width = x_tokens.shape
    experts, _, inner = w_gate.shape
    hbm = pl.BlockSpec(memory_space=pl.ANY)
    rows = (2, 4, experts, SLOT, width)
    grads = (2, 4, experts, SLOT, inner)
    part = (2, 2, tokens, width // 2)
    dma = pltpu.SemaphoreType.DMA
    outs = (rows, rows, grads, grads, grads)
    return pl.pallas_call(
        rows_kernel,
        out_shape=tuple(jax.ShapeDtypeStruct(s, BF16) for s in outs) + (jax.ShapeDtypeStruct(part, F32),) * 2,
        in_specs=[hbm] * 7,
        out_specs=(hbm,) * 7,
        scratch_shapes=[
            pltpu.VMEM((8, tokens, width), BF16),
            pltpu.VMEM((8, tokens, width), BF16),
            pltpu.VMEM((8,) + code.shape, jnp.int32),
            pltpu.VMEM((8,) + gate.shape, F32),
            pltpu.VMEM((8, 256, tokens), BF16),
            pltpu.VMEM((8, 256, tokens), BF16),
            pltpu.VMEM(rows[1:], BF16),
            pltpu.VMEM(rows[1:], BF16),
            pltpu.VMEM(w_gate.shape, BF16),
            pltpu.VMEM(w_up.shape, BF16),
            pltpu.VMEM(w_down.shape, BF16),
            pltpu.VMEM((2, 2, experts, 4 * SLOT, inner), BF16),
            pltpu.VMEM((3, experts, 4, SLOT, inner), BF16),
            pltpu.VMEM((experts, 4, SLOT, width // 2), BF16),
            pltpu.VMEM((2, experts, 4, SLOT, width // 2), BF16),
            pltpu.VMEM((2, experts, 4, SLOT, width // 2), BF16),
            pltpu.VMEM((4, tokens, width // 2), F32),
            dma((4,)),
            dma((2, 2, 7)),
            dma((2, 2, 7)),
            dma((2, 7)),
            dma((2, 7)),
            dma((3, 4)),
            dma((2, 2, 4)),
            dma((3, 2, 4)),
            dma((2, 4)),
            dma((2, 4)),
            dma((8,)),
        ],
        compiler_params=pltpu.CompilerParams(collective_id=0, has_side_effects=True, vmem_limit_bytes=67000000),
        name='rows_backward',
    )(x_tokens, dy_tokens, code, gate, w_gate, w_up, w_down)


TILES = 4


def weight_kernel(x_ref, z_ref, h_ref, da_ref, db_ref, dw1_ref, dw3_ref, dw2_ref, hidden_t):
    tile = pl.program_id(1)
    rows = 8 * SLOT

    @pl.when(tile == 0)
    def _():
        hidden_t[...] = h_ref[:, 0].reshape(rows, 512).T

    cols = pl.ds(pl.multiple_of(tile * 512, 512), 512)
    x_cols_t = x_ref[:, 0, :, cols].reshape(rows, 512).T
    dw1_ref[0] = dot_nn(x_cols_t, da_ref[:, 0].reshape(rows, 512))
    dw3_ref[0] = dot_nn(x_cols_t, db_ref[:, 0].reshape(rows, 512))
    dw2_ref[0] = dot_nn(hidden_t[...], z_ref[:, 0, :, cols].reshape(rows, 512))


def weight_grads(x_rows, z_rows, hidden, d_gate, d_up):
    _, experts, _, width = x_rows.shape
    inner = hidden.shape[3]
    by_expert = lambda e, t: (0, e, 0, 0)
    row_spec = pl.BlockSpec((8, 1, SLOT, width), by_expert)
    act_spec = pl.BlockSpec((8, 1, SLOT, inner), by_expert)
    return pl.pallas_call(
        weight_kernel,
        grid=(experts, TILES),
        out_shape=(
            jax.ShapeDtypeStruct((experts, width, inner), F32),
            jax.ShapeDtypeStruct((experts, width, inner), F32),
            jax.ShapeDtypeStruct((experts, inner, width), F32),
        ),
        in_specs=[row_spec, row_spec, act_spec, act_spec, act_spec],
        out_specs=(
            pl.BlockSpec((1, width // TILES, inner), lambda e, t: (e, t, 0)),
            pl.BlockSpec((1, width // TILES, inner), lambda e, t: (e, t, 0)),
            pl.BlockSpec((1, inner, width // TILES), lambda e, t: (e, 0, t)),
        ),
        scratch_shapes=[pltpu.VMEM((inner, 8 * SLOT), BF16)],
        compiler_params=pltpu.CompilerParams(dimension_semantics=('arbitrary', 'arbitrary'), vmem_limit_bytes=50000000),
        cost_estimate=pl.CostEstimate(flops=12_900_000_000, bytes_accessed=70_000_000, transcendentals=0),
        name='weight_grads',
    )(x_rows, z_rows, hidden, d_gate, d_up)


def shared_kernel(x_ref, dy_ref, w1_ref, w3_ref, w2_ref, dx_ref, dw1_ref, dw3_ref, dw2_ref, hidden_t, grad_gate, grad_up):
    tile = pl.program_id(0)

    @pl.when(tile == 0)
    def _():
        act_gate = dot_nn(x_ref[...], w1_ref[...]).astype(BF16)
        act_up = dot_nn(x_ref[...], w3_ref[...]).astype(BF16)
        hidden, d_gate, d_up = swiglu_parts(act_gate, act_up, dot_nt(dy_ref[...], w2_ref[...]))
        hidden_t[...] = hidden.T
        grad_gate[...] = d_gate
        grad_up[...] = d_up

    cols = pl.ds(pl.multiple_of(tile * 512, 512), 512)
    dx_ref[...] = dot_nt(grad_gate[...], w1_ref[cols, :]) + dot_nt(grad_up[...], w3_ref[cols, :])
    x_cols_t = x_ref[:, cols].T
    dw1_ref[0] = dot_nn(x_cols_t, grad_gate[...])
    dw3_ref[0] = dot_nn(x_cols_t, grad_up[...])
    dw2_ref[0] = dot_nn(hidden_t[...], dy_ref[:, cols])


def shared_backward(x_tokens, dy_tokens, shared_gate, shared_up, shared_down):
    tokens, width = x_tokens.shape
    inner = shared_gate.shape[1]
    vmem = pl.BlockSpec(memory_space=pltpu.VMEM)
    step = width // TILES
    return pl.pallas_call(
        shared_kernel,
        grid=(TILES,),
        out_shape=(
            jax.ShapeDtypeStruct((tokens, width), F32),
            jax.ShapeDtypeStruct((1, width, inner), F32),
            jax.ShapeDtypeStruct((1, width, inner), F32),
            jax.ShapeDtypeStruct((1, inner, width), F32),
        ),
        in_specs=[vmem] * 5,
        out_specs=(
            pl.BlockSpec((tokens, step), lambda t: (0, t)),
            pl.BlockSpec((1, step, inner), lambda t: (0, t, 0)),
            pl.BlockSpec((1, step, inner), lambda t: (0, t, 0)),
            pl.BlockSpec((1, inner, step), lambda t: (0, 0, t)),
        ),
        scratch_shapes=[
            pltpu.VMEM((inner, tokens), BF16),
            pltpu.VMEM((tokens, inner), BF16),
            pltpu.VMEM((tokens, inner), BF16),
        ],
        compiler_params=pltpu.CompilerParams(dimension_semantics=('arbitrary',), vmem_limit_bytes=40000000),
        cost_estimate=pl.CostEstimate(flops=6_000_000_000, bytes_accessed=20_000_000, transcendentals=0),
        name='shared_backward',
    )(x_tokens, dy_tokens, shared_gate, shared_up, shared_down)


def partners(kind):
    pairs = []
    for me in range(8):
        core = me % 2
        along_x, along_y = me ^ 2, me ^ 4
        first, second = (along_x, along_y) if core == 0 else (along_y, along_x)
        pairs.append((me, {'first': first, 'second': second, 'chip': me ^ 1}[kind]))
    return pairs


def solution(mesh):
    token_spec = P(('dp', 'ep'), None)
    expert_spec = P('ep', None, None)
    whole_spec = P(None, None)
    grad_spec = P(('dp', 'ep'), None, None)

    def local_backward(x_tokens, dy_tokens, expert_ids, gate_vals, slot_pos, w_gate, w_up, w_down, shared_gate, shared_up, shared_down):
        code = jnp.where(slot_pos >= 0, expert_ids * SLOT + slot_pos, -1)
        code = jnp.pad(code.T, ((0, 6), (0, 0)), constant_values=-1)
        gate = jnp.pad(gate_vals.T, ((0, 6), (0, 0)))
        *saved, give, keep = rows_backward(x_tokens, dy_tokens, code, gate, w_gate, w_up, w_down)
        saved = [rows.reshape((8,) + rows.shape[2:]) for rows in saved]
        got = lax.ppermute(give, 'ep', partners('first'))
        grads = weight_grads(*saved)
        got, grad_w_gate, grad_w_up, grad_w_down = lax.optimization_barrier((got,) + tuple(grads))
        onward = keep[0] + got[0]
        got_second = lax.ppermute(onward, 'ep', partners('second'))
        x_late, dy_late, _ = lax.optimization_barrier((x_tokens, dy_tokens, onward))
        shared_dx, grad_shared_gate, grad_shared_up, grad_shared_down = shared_backward(x_late, dy_late, shared_gate, shared_up, shared_down)
        got_second, shared_dx = lax.optimization_barrier((got_second, shared_dx))
        mine = keep[1] + got[1] + got_second
        swapped = lax.ppermute(mine[1], 'ep', partners('chip'))
        own = mine[0]
        core = lax.rem(lax.axis_index('ep'), 2)
        left = jnp.where(core == 0, own, swapped)
        right = jnp.where(core == 0, swapped, own)
        grad_x = (jnp.concatenate((left, right), axis=1) + shared_dx).astype(BF16)
        return grad_x, grad_w_gate, grad_w_up, grad_w_down, grad_shared_gate, grad_shared_up, grad_shared_down

    return jax.shard_map(local_backward, mesh=mesh, in_specs=(token_spec, token_spec, token_spec, token_spec, token_spec, expert_spec, expert_spec, expert_spec, whole_spec, whole_spec, whole_spec), out_specs=(token_spec, grad_spec, grad_spec, grad_spec, grad_spec, grad_spec, grad_spec), check_vma=False)
```

```python
import jax
import jax.numpy as jnp
from jax import lax
from jax.experimental import pallas as pl
from jax.experimental.pallas import tpu as pltpu
from jax.sharding import PartitionSpec as P

MESH = pl.DeviceIdType.MESH
SLOT = 64
BF16 = jnp.bfloat16
F32 = jnp.float32


def swiglu_parts(act_gate, act_up, grad_hidden):
    gate_f32 = act_gate.astype(F32)
    up_f32 = act_up.astype(F32)
    sigma = jax.nn.sigmoid(gate_f32)
    silu_gate = gate_f32 * sigma
    hidden = (silu_gate * up_f32).astype(BF16)
    grad_gate = (grad_hidden * up_f32 * sigma * (1.0 + gate_f32 * (1.0 - sigma))).astype(BF16)
    grad_up = (grad_hidden * silu_gate).astype(BF16)
    return hidden, grad_gate, grad_up


def dot_nn(a, b):
    return lax.dot_general(a, b, (((1,), (0,)), ((), ())), preferred_element_type=F32)


def dot_nt(a, b):
    return lax.dot_general(a, b, (((1,), (1,)), ((), ())), preferred_element_type=F32)


def dot_tn(a, b):
    return lax.dot_general(a, b, (((0,), (0,)), ((), ())), preferred_element_type=F32)


def places():
    me = lax.axis_index('ep')
    core = lax.rem(me, 2)
    flip_x = 2 - 4 * lax.rem(me // 2, 2)
    flip_y = 4 - 8 * (me // 4)
    first = me + flip_x * (1 - core) + flip_y * core
    second = me + flip_y * (1 - core) + flip_x * core
    diag = me + flip_x + flip_y
    partner = me + 1 - 2 * core
    return me, core, first, second, diag, partner


def remote(src, dst, send_sem, recv_sem, device):
    return pltpu.make_async_remote_copy(src_ref=src, dst_ref=dst, send_sem=send_sem, recv_sem=recv_sem, device_id={'ep': device}, device_id_type=MESH)


def one_hot(code, base, rows):
    slot = lax.broadcasted_iota(jnp.int32, (rows, 128), 0) + base
    hits = jnp.zeros((rows, 128), F32)
    for choice in range(10):
        hits = jnp.where(slot == code[choice:choice + 1, :], 1.0, hits)
    return hits


SEEN_AS = {1: 1, 2: 2, 3: 5, 4: 4, 5: 3, 6: 6, 7: 7}
PART = 64


def rows_kernel(x_ref, dy_ref, code_ref, gate_ref, w1_ref, w3_ref, w2_ref, xr_ref, zr_ref, h_ref, da_ref, db_ref, give_ref, keep_ref, xbuf, dybuf, codes, gates, picks, picks_partner, x_rows, z_rows, w1_buf, w3_buf, w2_buf, acts, grads, r_send, r_mine, r_got, sums, own_sem, send_sem, recv_sem, meta_send, meta_recv, load_sem, rows_sem, grads_sem, swap_send, swap_recv, sums_sem):
    me, core, first, second, diag, partner = places()
    other = 1 - core
    bufs = (xbuf, dybuf)

    def own(which):
        src, dst = ((x_ref, xbuf.at[0]), (dy_ref, dybuf.at[0]), (code_ref, codes.at[0]), (gate_ref, gates.at[0]))[which]
        return pltpu.make_async_copy(src, dst, own_sem.at[which])

    def load(which, expert):
        src, dst = ((w1_ref, w1_buf), (w3_ref, w3_buf), (w2_ref, w2_buf))[which]
        return pltpu.make_async_copy(src.at[expert], dst.at[expert], load_sem.at[which, expert])

    def trip(array, part, kind):
        src, dst, device = ((0, 2, first), (0, 4, second), (0, 1, partner), (2, 6, second), (2, 3, partner), (4, 5, partner), (6, 7, partner))[kind]
        rows = pl.ds(part * PART, PART)
        return remote(bufs[array].at[src, rows], bufs[array].at[dst, rows], send_sem.at[array, part, kind], recv_sem.at[array, part, kind], device)

    def meta(which, role):
        device = {1: partner, 2: first, 3: (second // 2) * 2 + other, 4: second, 5: (first // 2) * 2 + other, 6: diag, 7: (diag // 2) * 2 + other}[role]
        table = (codes, gates)[which]
        seen = SEEN_AS[role]
        return remote(table.at[0], table.at[seen], meta_send.at[which, role - 1], meta_recv.at[which, seen - 1], device)

    def relay_first(array, part):
        trip(array, part, 0).wait_recv()
        trip(array, part, 1).start()
        trip(array, part, 3).start()
        trip(array, part, 4).start()

    def relay_rest(array, part):
        trip(array, part, 1).wait_recv()
        trip(array, part, 5).start()
        trip(array, part, 3).wait_recv()
        trip(array, part, 6).start()

    def arrived(array, kind):
        for part in range(2):
            trip(array, part, kind).wait_recv()

    def rows_out(array, half, at):
        return pltpu.make_async_copy((x_rows, z_rows)[array].at[at], (xr_ref, zr_ref)[array].at[half, at], rows_sem.at[array, half, at])

    def pick_x(half, low, high):
        def one(at, carry):
            role = half * 4 + at
            select = one_hot(codes[role], me * 256, 256).astype(BF16)
            picks[role] = select
            picks_partner[role] = one_hot(codes[role], partner * 256, 256).astype(BF16)
            for tile in range(4):
                cols = slice(tile * 512, tile * 512 + 512)
                x_rows[at, :, :, cols] = dot_nn(select, xbuf[role, :, cols]).astype(BF16).reshape(4, SLOT, 512)
            rows_out(0, half, at).start()
            return carry

        lax.fori_loop(low, high, one, 0)

    def pick_z(half, low, high):
        def one(at, carry):
            role = half * 4 + at
            slot = lax.broadcasted_iota(jnp.int32, (256, 128), 0) + me * 256
            spread = jnp.zeros((256, 128), F32)
            for choice in range(10):
                spread = jnp.where(slot == codes[role, choice:choice + 1, :], gates[role, choice:choice + 1, :], spread)
            scale = jnp.sum(spread, axis=1, keepdims=True)
            select = picks[role]
            for tile in range(4):
                cols = slice(tile * 512, tile * 512 + 512)
                value = dot_nn(select, dybuf[role, :, cols]) * scale
                z_rows[at, :, :, cols] = value.astype(BF16).reshape(4, SLOT, 512)
            rows_out(1, half, at).start()
            return carry

        lax.fori_loop(low, high, one, 0)

    def activations(half, after):
        def one(expert, carry):
            if half == 0:
                load(0, expert).wait()
                load(1, expert).wait()
            rows = x_rows[:, expert].reshape(4 * SLOT, 2048)
            acts[0, half, expert] = dot_nn(rows, w1_buf[expert]).astype(BF16)
            acts[1, half, expert] = dot_nn(rows, w3_buf[expert]).astype(BF16)
            for step, action in after.items():
                pl.when(expert == step)(action)
            return carry

        lax.fori_loop(0, 4, one, 0)

    def grads_out(which, half, expert):
        return pltpu.make_async_copy(grads.at[which, expert], (h_ref, da_ref, db_ref)[which].at[half, :, expert], grads_sem.at[which, half, expert])

    def swap(half, expert):
        return remote(r_send.at[expert], r_got.at[half, expert], swap_send.at[half, expert], swap_recv.at[half, expert], partner)

    def back(half, after):
        def one(expert, carry):
            if half == 0:
                load(2, expert).wait()
            grad_hidden = dot_nt(z_rows[:, expert].reshape(4 * SLOT, 2048), w2_buf[expert])
            parts = swiglu_parts(acts[0, half, expert], acts[1, half, expert], grad_hidden)
            for which in range(3):
                if half == 1:
                    grads_out(which, 0, expert).wait()
                grads[which, expert] = parts[which].reshape(4, SLOT, 512)
                grads_out(which, half, expert).start()
            d_gate, d_up = parts[1], parts[2]

            def rows_back(side, tile):
                at = pl.ds(pl.multiple_of(side * 1024 + tile * 512, 512), 512)
                value = dot_nt(d_gate, w1_buf[expert, at, :]) + dot_nt(d_up, w3_buf[expert, at, :])
                return value.astype(BF16).reshape(4, SLOT, 512)

            if half == 1:
                swap(0, expert).wait_send()
            for tile in range(2):
                r_send[expert, :, :, tile * 512:(tile + 1) * 512] = rows_back(other, tile)
            swap(half, expert).start()
            for tile in range(2):
                r_mine[half, expert, :, :, tile * 512:(tile + 1) * 512] = rows_back(core, tile)
            for step, action in after.items():
                pl.when(expert == step)(action)
            return carry

        lax.fori_loop(0, 4, one, 0)

    def sums_out(role):
        ref, index, which = {6: (give_ref, 0, 0), 7: (give_ref, 0, 1), 2: (give_ref, 1, 0), 5: (give_ref, 1, 1), 4: (keep_ref, 0, 0), 3: (keep_ref, 0, 1), 0: (keep_ref, 1, 0), 1: (keep_ref, 1, 1)}[role]
        return pltpu.make_async_copy(sums.at[role % 4], ref.at[index, which], sums_sem.at[role])

    def total(half):
        for expert in range(4):
            swap(half, expert).wait_recv()
        for at in range(4):
            role = half * 4 + at
            if half == 1:
                sums_out(at).wait()
            sums[at] = dot_tn(picks[role], r_mine[half, :, at].reshape(256, 1024)) + dot_tn(picks_partner[role], r_got[half, :, at ^ 1].reshape(256, 1024))
            sums_out(role).start()

    for which in range(4):
        own(which).start()
    for expert in range(4):
        load(0, expert).start()
        load(1, expert).start()
    for expert in range(4):
        load(2, expert).start()
    barrier = pltpu.get_barrier_semaphore()
    for step in range(1, 8):
        pl.semaphore_signal(barrier, inc=1, device_id={'ep': lax.rem(me + step, 8)}, device_id_type=MESH)
    own(0).wait()
    own(1).wait()
    own(2).wait()
    own(3).wait()
    pl.semaphore_wait(barrier, 7)

    for role in range(1, 8):
        for which in range(2):
            meta(which, role).start()
    for part in range(2):
        trip(0, part, 0).start()
    for array in range(2):
        for part in range(2):
            trip(array, part, 2).start()

    pick_x(0, 0, 1)
    pick_z(0, 0, 1)
    for role in range(1, 8):
        for which in range(2):
            meta(which, role).wait_recv()
    arrived(0, 2)
    pick_x(0, 1, 2)
    relay_first(0, 0)
    arrived(1, 2)
    pick_z(0, 1, 2)
    relay_first(0, 1)
    trip(1, 0, 0).start()
    arrived(0, 4)
    pick_x(0, 2, 4)

    def rest_x():
        relay_rest(0, 0)
        trip(1, 1, 0).start()

    activations(0, {1: rest_x, 3: lambda: relay_first(1, 0)})
    relay_rest(0, 1)
    for at in range(4):
        rows_out(0, 0, at).wait()
    arrived(0, 5)
    pick_x(1, 0, 2)
    arrived(0, 6)
    pick_x(1, 2, 4)
    relay_first(1, 1)
    activations(1, {2: lambda: relay_rest(1, 0)})
    arrived(1, 4)
    pick_z(0, 2, 4)
    back(0, {2: lambda: relay_rest(1, 1)})
    total(0)
    for at in range(4):
        rows_out(1, 0, at).wait()
    arrived(1, 5)
    pick_z(1, 0, 2)
    arrived(1, 6)
    pick_z(1, 2, 4)
    back(1, {})
    total(1)

    for array in range(2):
        for part in range(2):
            for kind in range(7):
                trip(array, part, kind).wait_send()
    for role in range(1, 8):
        for which in range(2):
            meta(which, role).wait_send()
    for expert in range(4):
        swap(1, expert).wait_send()
        for which in range(3):
            grads_out(which, 1, expert).wait()
    for at in range(4):
        rows_out(0, 1, at).wait()
        rows_out(1, 1, at).wait()
        sums_out(4 + at).wait()


def rows_backward(x_tokens, dy_tokens, code, gate, w_gate, w_up, w_down):
    tokens, width = x_tokens.shape
    experts, _, inner = w_gate.shape
    hbm = pl.BlockSpec(memory_space=pl.ANY)
    rows = (2, 4, experts, SLOT, width)
    grads = (2, 4, experts, SLOT, inner)
    part = (2, 2, tokens, width // 2)
    dma = pltpu.SemaphoreType.DMA
    outs = (rows, rows, grads, grads, grads)
    return pl.pallas_call(
        rows_kernel,
        out_shape=tuple(jax.ShapeDtypeStruct(s, BF16) for s in outs) + (jax.ShapeDtypeStruct(part, F32),) * 2,
        in_specs=[hbm] * 7,
        out_specs=(hbm,) * 7,
        scratch_shapes=[
            pltpu.VMEM((8, tokens, width), BF16),
            pltpu.VMEM((8, tokens, width), BF16),
            pltpu.VMEM((8,) + code.shape, jnp.int32),
            pltpu.VMEM((8,) + gate.shape, F32),
            pltpu.VMEM((8, 256, tokens), BF16),
            pltpu.VMEM((8, 256, tokens), BF16),
            pltpu.VMEM(rows[1:], BF16),
            pltpu.VMEM(rows[1:], BF16),
            pltpu.VMEM(w_gate.shape, BF16),
            pltpu.VMEM(w_up.shape, BF16),
            pltpu.VMEM(w_down.shape, BF16),
            pltpu.VMEM((2, 2, experts, 4 * SLOT, inner), BF16),
            pltpu.VMEM((3, experts, 4, SLOT, inner), BF16),
            pltpu.VMEM((experts, 4, SLOT, width // 2), BF16),
            pltpu.VMEM((2, experts, 4, SLOT, width // 2), BF16),
            pltpu.VMEM((2, experts, 4, SLOT, width // 2), BF16),
            pltpu.VMEM((4, tokens, width // 2), F32),
            dma((4,)),
            dma((2, 2, 7)),
            dma((2, 2, 7)),
            dma((2, 7)),
            dma((2, 7)),
            dma((3, 4)),
            dma((2, 2, 4)),
            dma((3, 2, 4)),
            dma((2, 4)),
            dma((2, 4)),
            dma((8,)),
        ],
        compiler_params=pltpu.CompilerParams(collective_id=0, has_side_effects=True, vmem_limit_bytes=67000000),
        name='rows_backward',
    )(x_tokens, dy_tokens, code, gate, w_gate, w_up, w_down)


WEIGHT_TILES = 1


def weight_kernel(x_ref, z_ref, h_ref, da_ref, db_ref, dw1_ref, dw3_ref, dw2_ref, hidden_t):
    tile = pl.program_id(1)
    rows = 8 * SLOT

    @pl.when(tile == 0)
    def _():
        hidden_t[...] = h_ref[:, 0].reshape(rows, 512).T

    wide = 2048 // WEIGHT_TILES
    for piece in range(wide // 512):
        at = slice(piece * 512, piece * 512 + 512)
        cols = pl.ds(pl.multiple_of(tile * wide + piece * 512, 512), 512)
        x_cols_t = x_ref[:, 0, :, cols].reshape(rows, 512).T
        dw1_ref[0, at, :] = dot_nn(x_cols_t, da_ref[:, 0].reshape(rows, 512))
        dw3_ref[0, at, :] = dot_nn(x_cols_t, db_ref[:, 0].reshape(rows, 512))
        dw2_ref[0, :, at] = dot_nn(hidden_t[...], z_ref[:, 0, :, cols].reshape(rows, 512))


def weight_grads(x_rows, z_rows, hidden, d_gate, d_up):
    _, experts, _, width = x_rows.shape
    inner = hidden.shape[3]
    by_expert = lambda e, t: (0, e, 0, 0)
    row_spec = pl.BlockSpec((8, 1, SLOT, width), by_expert)
    act_spec = pl.BlockSpec((8, 1, SLOT, inner), by_expert)
    return pl.pallas_call(
        weight_kernel,
        grid=(experts, WEIGHT_TILES),
        out_shape=(
            jax.ShapeDtypeStruct((experts, width, inner), F32),
            jax.ShapeDtypeStruct((experts, width, inner), F32),
            jax.ShapeDtypeStruct((experts, inner, width), F32),
        ),
        in_specs=[row_spec, row_spec, act_spec, act_spec, act_spec],
        out_specs=(
            pl.BlockSpec((1, width // WEIGHT_TILES, inner), lambda e, t: (e, t, 0)),
            pl.BlockSpec((1, width // WEIGHT_TILES, inner), lambda e, t: (e, t, 0)),
            pl.BlockSpec((1, inner, width // WEIGHT_TILES), lambda e, t: (e, 0, t)),
        ),
        scratch_shapes=[pltpu.VMEM((inner, 8 * SLOT), BF16)],
        compiler_params=pltpu.CompilerParams(dimension_semantics=('arbitrary', 'arbitrary'), vmem_limit_bytes=67000000),
        cost_estimate=pl.CostEstimate(flops=12_900_000_000, bytes_accessed=70_000_000, transcendentals=0),
        name='weight_grads',
    )(x_rows, z_rows, hidden, d_gate, d_up)


SHARED_TILES = 4


def shared_kernel(x_ref, dy_ref, w1_ref, w3_ref, w2_ref, dx_ref, dw1_ref, dw3_ref, dw2_ref, hidden_t, grad_gate, grad_up):
    tile = pl.program_id(0)

    @pl.when(tile == 0)
    def _():
        act_gate = dot_nn(x_ref[...], w1_ref[...]).astype(BF16)
        act_up = dot_nn(x_ref[...], w3_ref[...]).astype(BF16)
        hidden, d_gate, d_up = swiglu_parts(act_gate, act_up, dot_nt(dy_ref[...], w2_ref[...]))
        hidden_t[...] = hidden.T
        grad_gate[...] = d_gate
        grad_up[...] = d_up

    cols = pl.ds(pl.multiple_of(tile * 512, 512), 512)
    dx_ref[...] = dot_nt(grad_gate[...], w1_ref[cols, :]) + dot_nt(grad_up[...], w3_ref[cols, :])
    x_cols_t = x_ref[:, cols].T
    dw1_ref[0] = dot_nn(x_cols_t, grad_gate[...])
    dw3_ref[0] = dot_nn(x_cols_t, grad_up[...])
    dw2_ref[0] = dot_nn(hidden_t[...], dy_ref[:, cols])


def shared_backward(x_tokens, dy_tokens, shared_gate, shared_up, shared_down):
    tokens, width = x_tokens.shape
    inner = shared_gate.shape[1]
    vmem = pl.BlockSpec(memory_space=pltpu.VMEM)
    step = width // SHARED_TILES
    return pl.pallas_call(
        shared_kernel,
        grid=(SHARED_TILES,),
        out_shape=(
            jax.ShapeDtypeStruct((tokens, width), F32),
            jax.ShapeDtypeStruct((1, width, inner), F32),
            jax.ShapeDtypeStruct((1, width, inner), F32),
            jax.ShapeDtypeStruct((1, inner, width), F32),
        ),
        in_specs=[vmem] * 5,
        out_specs=(
            pl.BlockSpec((tokens, step), lambda t: (0, t)),
            pl.BlockSpec((1, step, inner), lambda t: (0, t, 0)),
            pl.BlockSpec((1, step, inner), lambda t: (0, t, 0)),
            pl.BlockSpec((1, inner, step), lambda t: (0, 0, t)),
        ),
        scratch_shapes=[
            pltpu.VMEM((inner, tokens), BF16),
            pltpu.VMEM((tokens, inner), BF16),
            pltpu.VMEM((tokens, inner), BF16),
        ],
        compiler_params=pltpu.CompilerParams(dimension_semantics=('arbitrary',), vmem_limit_bytes=67000000),
        cost_estimate=pl.CostEstimate(flops=6_000_000_000, bytes_accessed=20_000_000, transcendentals=0),
        name='shared_backward',
    )(x_tokens, dy_tokens, shared_gate, shared_up, shared_down)


def partners(kind):
    pairs = []
    for me in range(8):
        core = me % 2
        along_x, along_y = me ^ 2, me ^ 4
        first, second = (along_x, along_y) if core == 0 else (along_y, along_x)
        pairs.append((me, {'first': first, 'second': second, 'chip': me ^ 1}[kind]))
    return pairs


def solution(mesh):
    token_spec = P(('dp', 'ep'), None)
    expert_spec = P('ep', None, None)
    whole_spec = P(None, None)
    grad_spec = P(('dp', 'ep'), None, None)

    def local_backward(x_tokens, dy_tokens, expert_ids, gate_vals, slot_pos, w_gate, w_up, w_down, shared_gate, shared_up, shared_down):
        code = jnp.where(slot_pos >= 0, expert_ids * SLOT + slot_pos, -1)
        code = jnp.pad(code.T, ((0, 6), (0, 0)), constant_values=-1)
        gate = jnp.pad(gate_vals.T, ((0, 6), (0, 0)))
        *saved, give, keep = rows_backward(x_tokens, dy_tokens, code, gate, w_gate, w_up, w_down)
        saved = [rows.reshape((8,) + rows.shape[2:]) for rows in saved]
        got = lax.ppermute(give, 'ep', partners('first'))
        grads = weight_grads(*saved)
        got, grad_w_gate, grad_w_up, grad_w_down = lax.optimization_barrier((got,) + tuple(grads))
        onward = keep[0] + got[0]
        got_second = lax.ppermute(onward, 'ep', partners('second'))
        x_late, dy_late, _ = lax.optimization_barrier((x_tokens, dy_tokens, onward))
        shared_dx, grad_shared_gate, grad_shared_up, grad_shared_down = shared_backward(x_late, dy_late, shared_gate, shared_up, shared_down)
        got_second, shared_dx = lax.optimization_barrier((got_second, shared_dx))
        mine = keep[1] + got[1] + got_second
        swapped = lax.ppermute(mine[1], 'ep', partners('chip'))
        own = mine[0]
        core = lax.rem(lax.axis_index('ep'), 2)
        left = jnp.where(core == 0, own, swapped)
        right = jnp.where(core == 0, swapped, own)
        grad_x = (jnp.concatenate((left, right), axis=1) + shared_dx).astype(BF16)
        return grad_x, grad_w_gate, grad_w_up, grad_w_down, grad_shared_gate, grad_shared_up, grad_shared_down

    return jax.shard_map(local_backward, mesh=mesh, in_specs=(token_spec, token_spec, token_spec, token_spec, token_spec, expert_spec, expert_spec, expert_spec, whole_spec, whole_spec, whole_spec), out_specs=(token_spec, grad_spec, grad_spec, grad_spec, grad_spec, grad_spec, grad_spec), check_vma=False)
```

```python
import jax
import jax.numpy as jnp
from jax import lax
from jax.experimental import pallas as pl
from jax.experimental.pallas import tpu as pltpu
from jax.sharding import PartitionSpec as P

MESH = pl.DeviceIdType.MESH
SLOT = 64
BF16 = jnp.bfloat16
F32 = jnp.float32


def swiglu_parts(act_gate, act_up, grad_hidden):
    gate_f32 = act_gate.astype(F32)
    up_f32 = act_up.astype(F32)
    sigma = jax.nn.sigmoid(gate_f32)
    silu_gate = gate_f32 * sigma
    hidden = (silu_gate * up_f32).astype(BF16)
    grad_gate = (grad_hidden * up_f32 * sigma * (1.0 + gate_f32 * (1.0 - sigma))).astype(BF16)
    grad_up = (grad_hidden * silu_gate).astype(BF16)
    return hidden, grad_gate, grad_up


def dot_nn(a, b):
    return lax.dot_general(a, b, (((1,), (0,)), ((), ())), preferred_element_type=F32)


def dot_nt(a, b):
    return lax.dot_general(a, b, (((1,), (1,)), ((), ())), preferred_element_type=F32)


def dot_tn(a, b):
    return lax.dot_general(a, b, (((0,), (0,)), ((), ())), preferred_element_type=F32)


def places():
    me = lax.axis_index('ep')
    core = lax.rem(me, 2)
    flip_x = 2 - 4 * lax.rem(me // 2, 2)
    flip_y = 4 - 8 * (me // 4)
    first = me + flip_x * (1 - core) + flip_y * core
    second = me + flip_y * (1 - core) + flip_x * core
    diag = me + flip_x + flip_y
    partner = me + 1 - 2 * core
    return me, core, first, second, diag, partner


def remote(src, dst, send_sem, recv_sem, device):
    return pltpu.make_async_remote_copy(src_ref=src, dst_ref=dst, send_sem=send_sem, recv_sem=recv_sem, device_id={'ep': device}, device_id_type=MESH)


def one_hot(code, base, rows):
    slot = lax.broadcasted_iota(jnp.int32, (rows, 128), 0) + base
    hits = jnp.zeros((rows, 128), F32)
    for choice in range(10):
        hits = jnp.where(slot == code[choice:choice + 1, :], 1.0, hits)
    return hits


SEEN_AS = {1: 1, 2: 2, 3: 5, 4: 4, 5: 3, 6: 6, 7: 7}
PART = 64


def rows_kernel(x_ref, dy_ref, ids_ref, pos_ref, gate_ref, w1_ref, w3_ref, w2_ref, xr_ref, zr_ref, h_ref, da_ref, db_ref, give_ref, keep_ref, xbuf, dybuf, codes, gates, picks, picks_partner, x_rows, z_rows, w1_buf, w3_buf, w2_buf, acts, grads, r_send, r_mine, r_got, sums, own_sem, send_sem, recv_sem, meta_send, meta_recv, load_sem, rows_sem, grads_sem, swap_send, swap_recv, sums_sem):
    me, core, first, second, diag, partner = places()
    other = 1 - core
    bufs = (xbuf, dybuf)

    def own(which):
        src, dst = ((x_ref, xbuf.at[0]), (dy_ref, dybuf.at[0]))[which]
        return pltpu.make_async_copy(src, dst, own_sem.at[which])

    def load(which, expert):
        src, dst = ((w1_ref, w1_buf), (w3_ref, w3_buf), (w2_ref, w2_buf))[which]
        return pltpu.make_async_copy(src.at[expert], dst.at[expert], load_sem.at[which, expert])

    def trip(array, part, kind):
        src, dst, device = ((0, 2, first), (0, 4, second), (0, 1, partner), (2, 6, second), (2, 3, partner), (4, 5, partner), (6, 7, partner))[kind]
        rows = pl.ds(part * PART, PART)
        return remote(bufs[array].at[src, rows], bufs[array].at[dst, rows], send_sem.at[array, part, kind], recv_sem.at[array, part, kind], device)

    def meta(which, role):
        device = {1: partner, 2: first, 3: (second // 2) * 2 + other, 4: second, 5: (first // 2) * 2 + other, 6: diag, 7: (diag // 2) * 2 + other}[role]
        table = (codes, gates)[which]
        seen = SEEN_AS[role]
        return remote(table.at[0], table.at[seen], meta_send.at[which, role - 1], meta_recv.at[which, seen - 1], device)

    def relay_first(array, part):
        trip(array, part, 0).wait_recv()
        trip(array, part, 1).start()
        trip(array, part, 3).start()
        trip(array, part, 4).start()

    def relay_rest(array, part):
        trip(array, part, 1).wait_recv()
        trip(array, part, 5).start()
        trip(array, part, 3).wait_recv()
        trip(array, part, 6).start()

    def arrived(array, kind):
        for part in range(2):
            trip(array, part, kind).wait_recv()

    def rows_out(array, half, at):
        return pltpu.make_async_copy((x_rows, z_rows)[array].at[at], (xr_ref, zr_ref)[array].at[half, at], rows_sem.at[array, half, at])

    def pick_x(half, low, high):
        def one(at, carry):
            role = half * 4 + at
            select = one_hot(codes[role], me * 256, 256).astype(BF16)
            picks[role] = select
            picks_partner[role] = one_hot(codes[role], partner * 256, 256).astype(BF16)
            for tile in range(4):
                cols = slice(tile * 512, tile * 512 + 512)
                x_rows[at, :, :, cols] = dot_nn(select, xbuf[role, :, cols]).astype(BF16).reshape(4, SLOT, 512)
            rows_out(0, half, at).start()
            return carry

        lax.fori_loop(low, high, one, 0)

    def pick_z(half, low, high):
        def one(at, carry):
            role = half * 4 + at
            slot = lax.broadcasted_iota(jnp.int32, (256, 128), 0) + me * 256
            spread = jnp.zeros((256, 128), F32)
            for choice in range(10):
                spread = jnp.where(slot == codes[role, choice:choice + 1, :], gates[role, choice:choice + 1, :], spread)
            scale = jnp.sum(spread, axis=1, keepdims=True)
            select = picks[role]
            for tile in range(4):
                cols = slice(tile * 512, tile * 512 + 512)
                value = dot_nn(select, dybuf[role, :, cols]) * scale
                z_rows[at, :, :, cols] = value.astype(BF16).reshape(4, SLOT, 512)
            rows_out(1, half, at).start()
            return carry

        lax.fori_loop(low, high, one, 0)

    def activations(half, after):
        def one(expert, carry):
            if half == 0:
                load(0, expert).wait()
                load(1, expert).wait()
            rows = x_rows[:, expert].reshape(4 * SLOT, 2048)
            acts[0, half, expert] = dot_nn(rows, w1_buf[expert]).astype(BF16)
            acts[1, half, expert] = dot_nn(rows, w3_buf[expert]).astype(BF16)
            for step, action in after.items():
                pl.when(expert == step)(action)
            return carry

        lax.fori_loop(0, 4, one, 0)

    def grads_out(which, half, expert):
        return pltpu.make_async_copy(grads.at[which, expert], (h_ref, da_ref, db_ref)[which].at[half, :, expert], grads_sem.at[which, half, expert])

    def swap(half, expert):
        return remote(r_send.at[expert], r_got.at[half, expert], swap_send.at[half, expert], swap_recv.at[half, expert], partner)

    def back(half, after):
        def one(expert, carry):
            if half == 0:
                load(2, expert).wait()
            grad_hidden = dot_nt(z_rows[:, expert].reshape(4 * SLOT, 2048), w2_buf[expert])
            parts = swiglu_parts(acts[0, half, expert], acts[1, half, expert], grad_hidden)
            for which in range(3):
                if half == 1:
                    grads_out(which, 0, expert).wait()
                grads[which, expert] = parts[which].reshape(4, SLOT, 512)
                grads_out(which, half, expert).start()
            d_gate, d_up = parts[1], parts[2]

            def rows_back(side, tile):
                at = pl.ds(pl.multiple_of(side * 1024 + tile * 512, 512), 512)
                value = dot_nt(d_gate, w1_buf[expert, at, :]) + dot_nt(d_up, w3_buf[expert, at, :])
                return value.astype(BF16).reshape(4, SLOT, 512)

            if half == 1:
                swap(0, expert).wait_send()
            for tile in range(2):
                r_send[expert, :, :, tile * 512:(tile + 1) * 512] = rows_back(other, tile)
            swap(half, expert).start()
            for tile in range(2):
                r_mine[half, expert, :, :, tile * 512:(tile + 1) * 512] = rows_back(core, tile)
            for step, action in after.items():
                pl.when(expert == step)(action)
            return carry

        lax.fori_loop(0, 4, one, 0)

    def sums_out(role):
        ref, index, which = {6: (give_ref, 0, 0), 7: (give_ref, 0, 1), 2: (give_ref, 1, 0), 5: (give_ref, 1, 1), 4: (keep_ref, 0, 0), 3: (keep_ref, 0, 1), 0: (keep_ref, 1, 0), 1: (keep_ref, 1, 1)}[role]
        return pltpu.make_async_copy(sums.at[role % 4], ref.at[index, which], sums_sem.at[role])

    def total(half):
        for expert in range(4):
            swap(half, expert).wait_recv()
        for at in range(4):
            role = half * 4 + at
            if half == 1:
                sums_out(at).wait()
            sums[at] = dot_tn(picks[role], r_mine[half, :, at].reshape(256, 1024)) + dot_tn(picks_partner[role], r_got[half, :, at ^ 1].reshape(256, 1024))
            sums_out(role).start()

    for which in range(2):
        own(which).start()
    barrier = pltpu.get_barrier_semaphore()
    for step in range(1, 8):
        pl.semaphore_signal(barrier, inc=1, device_id={'ep': lax.rem(me + step, 8)}, device_id_type=MESH)
    code = jnp.where(pos_ref[...] >= 0, ids_ref[...] * SLOT + pos_ref[...], -1)
    codes[0] = jnp.zeros((16, 128), jnp.int32)
    gates[0] = jnp.zeros((16, 128), F32)
    codes[0, 0:10, :] = code.T
    gates[0, 0:10, :] = gate_ref[...].T
    own(0).wait()
    own(1).wait()
    pl.semaphore_wait(barrier, 7)

    for role in range(1, 8):
        for which in range(2):
            meta(which, role).start()
    for array in range(2):
        for part in range(2):
            trip(array, part, 0).start()
    for array in range(2):
        for part in range(2):
            trip(array, part, 2).start()

    pick_x(0, 0, 1)
    pick_z(0, 0, 1)
    for expert in range(4):
        load(0, expert).start()
        load(1, expert).start()
    for role in range(1, 8):
        for which in range(2):
            meta(which, role).wait_recv()
    arrived(0, 2)
    pick_x(0, 1, 2)
    relay_first(0, 0)
    arrived(1, 2)
    pick_z(0, 1, 2)
    relay_first(0, 1)
    for expert in range(4):
        load(2, expert).start()
    arrived(0, 4)
    pick_x(0, 2, 4)
    activations(0, {1: lambda: relay_first(1, 0)})
    relay_first(1, 1)
    arrived(1, 4)
    pick_z(0, 2, 4)
    back(0, {1: lambda: relay_rest(0, 0), 3: lambda: relay_rest(0, 1)})
    total(0)
    for at in range(4):
        rows_out(0, 0, at).wait()
    arrived(0, 5)
    pick_x(1, 0, 2)
    arrived(0, 6)
    pick_x(1, 2, 4)
    activations(1, {1: lambda: relay_rest(1, 0)})
    relay_rest(1, 1)
    for at in range(4):
        rows_out(1, 0, at).wait()
    arrived(1, 5)
    pick_z(1, 0, 2)
    arrived(1, 6)
    pick_z(1, 2, 4)
    back(1, {})
    total(1)

    for array in range(2):
        for part in range(2):
            for kind in range(7):
                trip(array, part, kind).wait_send()
    for role in range(1, 8):
        for which in range(2):
            meta(which, role).wait_send()
    for expert in range(4):
        swap(1, expert).wait_send()
        for which in range(3):
            grads_out(which, 1, expert).wait()
    for at in range(4):
        rows_out(0, 1, at).wait()
        rows_out(1, 1, at).wait()
        sums_out(4 + at).wait()


def rows_backward(x_tokens, dy_tokens, expert_ids, slot_pos, gate_vals, w_gate, w_up, w_down):
    tokens, width = x_tokens.shape
    experts, _, inner = w_gate.shape
    hbm = pl.BlockSpec(memory_space=pl.ANY)
    rows = (2, 4, experts, SLOT, width)
    grads = (2, 4, experts, SLOT, inner)
    part = (2, 2, tokens, width // 2)
    dma = pltpu.SemaphoreType.DMA
    outs = (rows, rows, grads, grads, grads)
    return pl.pallas_call(
        rows_kernel,
        out_shape=tuple(jax.ShapeDtypeStruct(s, BF16) for s in outs) + (jax.ShapeDtypeStruct(part, F32),) * 2,
        in_specs=[hbm] * 2 + [pl.BlockSpec(memory_space=pltpu.VMEM)] * 3 + [hbm] * 3,
        out_specs=(hbm,) * 7,
        scratch_shapes=[
            pltpu.VMEM((8, tokens, width), BF16),
            pltpu.VMEM((8, tokens, width), BF16),
            pltpu.VMEM((8, 16, tokens), jnp.int32),
            pltpu.VMEM((8, 16, tokens), F32),
            pltpu.VMEM((8, 256, tokens), BF16),
            pltpu.VMEM((8, 256, tokens), BF16),
            pltpu.VMEM(rows[1:], BF16),
            pltpu.VMEM(rows[1:], BF16),
            pltpu.VMEM(w_gate.shape, BF16),
            pltpu.VMEM(w_up.shape, BF16),
            pltpu.VMEM(w_down.shape, BF16),
            pltpu.VMEM((2, 2, experts, 4 * SLOT, inner), BF16),
            pltpu.VMEM((3, experts, 4, SLOT, inner), BF16),
            pltpu.VMEM((experts, 4, SLOT, width // 2), BF16),
            pltpu.VMEM((2, experts, 4, SLOT, width // 2), BF16),
            pltpu.VMEM((2, experts, 4, SLOT, width // 2), BF16),
            pltpu.VMEM((4, tokens, width // 2), F32),
            dma((2,)),
            dma((2, 2, 7)),
            dma((2, 2, 7)),
            dma((2, 7)),
            dma((2, 7)),
            dma((3, 4)),
            dma((2, 2, 4)),
            dma((3, 2, 4)),
            dma((2, 4)),
            dma((2, 4)),
            dma((8,)),
        ],
        compiler_params=pltpu.CompilerParams(collective_id=0, has_side_effects=True, vmem_limit_bytes=67000000),
        name='rows_backward',
    )(x_tokens, dy_tokens, expert_ids, slot_pos, gate_vals, w_gate, w_up, w_down)


WEIGHT_TILES = 1


def weight_kernel(x_ref, z_ref, h_ref, da_ref, db_ref, dw1_ref, dw3_ref, dw2_ref, hidden_t):
    tile = pl.program_id(1)
    rows = 8 * SLOT

    @pl.when(tile == 0)
    def _():
        hidden_t[...] = h_ref[:, 0].reshape(rows, 512).T

    wide = 2048 // WEIGHT_TILES
    for piece in range(wide // 512):
        at = slice(piece * 512, piece * 512 + 512)
        cols = pl.ds(pl.multiple_of(tile * wide + piece * 512, 512), 512)
        x_cols_t = x_ref[:, 0, :, cols].reshape(rows, 512).T
        dw1_ref[0, at, :] = dot_nn(x_cols_t, da_ref[:, 0].reshape(rows, 512))
        dw3_ref[0, at, :] = dot_nn(x_cols_t, db_ref[:, 0].reshape(rows, 512))
        dw2_ref[0, :, at] = dot_nn(hidden_t[...], z_ref[:, 0, :, cols].reshape(rows, 512))


def weight_grads(x_rows, z_rows, hidden, d_gate, d_up):
    _, experts, _, width = x_rows.shape
    inner = hidden.shape[3]
    by_expert = lambda e, t: (0, e, 0, 0)
    row_spec = pl.BlockSpec((8, 1, SLOT, width), by_expert)
    act_spec = pl.BlockSpec((8, 1, SLOT, inner), by_expert)
    return pl.pallas_call(
        weight_kernel,
        grid=(experts, WEIGHT_TILES),
        out_shape=(
            jax.ShapeDtypeStruct((experts, width, inner), F32),
            jax.ShapeDtypeStruct((experts, width, inner), F32),
            jax.ShapeDtypeStruct((experts, inner, width), F32),
        ),
        in_specs=[row_spec, row_spec, act_spec, act_spec, act_spec],
        out_specs=(
            pl.BlockSpec((1, width // WEIGHT_TILES, inner), lambda e, t: (e, t, 0)),
            pl.BlockSpec((1, width // WEIGHT_TILES, inner), lambda e, t: (e, t, 0)),
            pl.BlockSpec((1, inner, width // WEIGHT_TILES), lambda e, t: (e, 0, t)),
        ),
        scratch_shapes=[pltpu.VMEM((inner, 8 * SLOT), BF16)],
        compiler_params=pltpu.CompilerParams(dimension_semantics=('arbitrary', 'arbitrary'), vmem_limit_bytes=67000000),
        cost_estimate=pl.CostEstimate(flops=12_900_000_000, bytes_accessed=70_000_000, transcendentals=0),
        name='weight_grads',
    )(x_rows, z_rows, hidden, d_gate, d_up)


SHARED_TILES = 4


def shared_kernel(x_ref, dy_ref, w1_ref, w3_ref, w2_ref, dx_ref, dw1_ref, dw3_ref, dw2_ref, hidden_t, grad_gate, grad_up):
    tile = pl.program_id(0)

    @pl.when(tile == 0)
    def _():
        act_gate = dot_nn(x_ref[...], w1_ref[...]).astype(BF16)
        act_up = dot_nn(x_ref[...], w3_ref[...]).astype(BF16)
        hidden, d_gate, d_up = swiglu_parts(act_gate, act_up, dot_nt(dy_ref[...], w2_ref[...]))
        hidden_t[...] = hidden.T
        grad_gate[...] = d_gate
        grad_up[...] = d_up

    cols = pl.ds(pl.multiple_of(tile * 512, 512), 512)
    dx_ref[...] = dot_nt(grad_gate[...], w1_ref[cols, :]) + dot_nt(grad_up[...], w3_ref[cols, :])
    x_cols_t = x_ref[:, cols].T
    dw1_ref[0] = dot_nn(x_cols_t, grad_gate[...])
    dw3_ref[0] = dot_nn(x_cols_t, grad_up[...])
    dw2_ref[0] = dot_nn(hidden_t[...], dy_ref[:, cols])


def shared_backward(x_tokens, dy_tokens, shared_gate, shared_up, shared_down):
    tokens, width = x_tokens.shape
    inner = shared_gate.shape[1]
    vmem = pl.BlockSpec(memory_space=pltpu.VMEM)
    step = width // SHARED_TILES
    return pl.pallas_call(
        shared_kernel,
        grid=(SHARED_TILES,),
        out_shape=(
            jax.ShapeDtypeStruct((tokens, width), F32),
            jax.ShapeDtypeStruct((1, width, inner), F32),
            jax.ShapeDtypeStruct((1, width, inner), F32),
            jax.ShapeDtypeStruct((1, inner, width), F32),
        ),
        in_specs=[vmem] * 5,
        out_specs=(
            pl.BlockSpec((tokens, step), lambda t: (0, t)),
            pl.BlockSpec((1, step, inner), lambda t: (0, t, 0)),
            pl.BlockSpec((1, step, inner), lambda t: (0, t, 0)),
            pl.BlockSpec((1, inner, step), lambda t: (0, 0, t)),
        ),
        scratch_shapes=[
            pltpu.VMEM((inner, tokens), BF16),
            pltpu.VMEM((tokens, inner), BF16),
            pltpu.VMEM((tokens, inner), BF16),
        ],
        compiler_params=pltpu.CompilerParams(dimension_semantics=('arbitrary',), vmem_limit_bytes=67000000),
        cost_estimate=pl.CostEstimate(flops=6_000_000_000, bytes_accessed=20_000_000, transcendentals=0),
        name='shared_backward',
    )(x_tokens, dy_tokens, shared_gate, shared_up, shared_down)


def partners(kind):
    pairs = []
    for me in range(8):
        core = me % 2
        along_x, along_y = me ^ 2, me ^ 4
        first, second = (along_x, along_y) if core == 0 else (along_y, along_x)
        pairs.append((me, {'first': first, 'second': second, 'chip': me ^ 1}[kind]))
    return pairs


def solution(mesh):
    token_spec = P(('dp', 'ep'), None)
    expert_spec = P('ep', None, None)
    whole_spec = P(None, None)
    grad_spec = P(('dp', 'ep'), None, None)

    def local_backward(x_tokens, dy_tokens, expert_ids, gate_vals, slot_pos, w_gate, w_up, w_down, shared_gate, shared_up, shared_down):
        *saved, give, keep = rows_backward(x_tokens, dy_tokens, expert_ids, slot_pos, gate_vals, w_gate, w_up, w_down)
        saved = [rows.reshape((8,) + rows.shape[2:]) for rows in saved]
        got = lax.ppermute(give, 'ep', partners('first'))
        grads = weight_grads(*saved)
        got, grad_w_gate, grad_w_up, grad_w_down = lax.optimization_barrier((got,) + tuple(grads))
        onward = keep[0] + got[0]
        got_second = lax.ppermute(onward, 'ep', partners('second'))
        x_late, dy_late, _ = lax.optimization_barrier((x_tokens, dy_tokens, onward))
        shared_dx, grad_shared_gate, grad_shared_up, grad_shared_down = shared_backward(x_late, dy_late, shared_gate, shared_up, shared_down)
        got_second, shared_dx = lax.optimization_barrier((got_second, shared_dx))
        mine = keep[1] + got[1] + got_second
        swapped = lax.ppermute(mine[1], 'ep', partners('chip'))
        own = mine[0]
        core = lax.rem(lax.axis_index('ep'), 2)
        left = jnp.where(core == 0, own, swapped)
        right = jnp.where(core == 0, swapped, own)
        grad_x = (jnp.concatenate((left, right), axis=1) + shared_dx).astype(BF16)
        return grad_x, grad_w_gate, grad_w_up, grad_w_down, grad_shared_gate, grad_shared_up, grad_shared_down

    return jax.shard_map(local_backward, mesh=mesh, in_specs=(token_spec, token_spec, token_spec, token_spec, token_spec, expert_spec, expert_spec, expert_spec, whole_spec, whole_spec, whole_spec), out_specs=(token_spec, grad_spec, grad_spec, grad_spec, grad_spec, grad_spec, grad_spec), check_vma=False)
```

```python
import jax
import jax.numpy as jnp
from jax import lax
from jax.experimental import pallas as pl
from jax.experimental.pallas import tpu as pltpu
from jax.sharding import PartitionSpec as P

MESH = pl.DeviceIdType.MESH
BF16 = jnp.bfloat16
F32 = jnp.float32
TOKENS, TOP_K, EXPERTS, ROLES, PARTS = 128, 10, 4, 8, 2
WIDTH, HALF, INNER, SLOT, PART = 2048, 1024, 512, 64, 64
ROWS = 256
X, DY = range(2)
EARLY, LATE = range(2)
TO_FIRST, TO_SECOND, TO_PARTNER, FIRST_ON, FIRST_OVER, SECOND_OVER, DIAG_OVER = range(7)
TRIPS = 7
SEEN_AS = {1: 1, 2: 2, 3: 5, 4: 4, 5: 3, 6: 6, 7: 7}


def swiglu_parts(act_gate, act_up, grad_hidden):
    gate_f32 = act_gate.astype(F32)
    up_f32 = act_up.astype(F32)
    sigma = jax.nn.sigmoid(gate_f32)
    silu_gate = gate_f32 * sigma
    hidden = (silu_gate * up_f32).astype(BF16)
    grad_gate = (grad_hidden * up_f32 * sigma * (1.0 + gate_f32 * (1.0 - sigma))).astype(BF16)
    grad_up = (grad_hidden * silu_gate).astype(BF16)
    return hidden, grad_gate, grad_up


def dot_nn(a, b):
    return lax.dot_general(a, b, (((1,), (0,)), ((), ())), preferred_element_type=F32)


def dot_nt(a, b):
    return lax.dot_general(a, b, (((1,), (1,)), ((), ())), preferred_element_type=F32)


def dot_tn(a, b):
    return lax.dot_general(a, b, (((0,), (0,)), ((), ())), preferred_element_type=F32)


def places():
    me = lax.axis_index('ep')
    core = lax.rem(me, 2)
    flip_x = 2 - 4 * lax.rem(me // 2, 2)
    flip_y = 4 - 8 * (me // 4)
    first = me + flip_x * (1 - core) + flip_y * core
    second = me + flip_y * (1 - core) + flip_x * core
    diag = me + flip_x + flip_y
    partner = me + 1 - 2 * core
    return me, core, first, second, diag, partner


def remote(src, dst, send_sem, recv_sem, device):
    return pltpu.make_async_remote_copy(src_ref=src, dst_ref=dst, send_sem=send_sem, recv_sem=recv_sem, device_id={'ep': device}, device_id_type=MESH)


def one_hot(code, base):
    slot = lax.broadcasted_iota(jnp.int32, (ROWS, TOKENS), 0) + base
    hits = jnp.zeros((ROWS, TOKENS), F32)
    for choice in range(TOP_K):
        hits = jnp.where(slot == code[choice:choice + 1, :], 1.0, hits)
    return hits.astype(BF16)


def rows_kernel(x_ref, dy_ref, ids_ref, pos_ref, gate_ref, w1_ref, w3_ref, w2_ref, s1_ref, s3_ref, s2_ref, xr_ref, zr_ref, h_ref, da_ref, db_ref, far_ref, cross_ref, near_ref, base_ref, leaf_ref, dx_ref, parts_ref, xbuf, dybuf, codes, gates, picks, picks_partner, x_rows, z_rows, w1_buf, w3_buf, w2_buf, acts, grads, r_send, r_mine, r_got, sums, own_sem, send_sem, recv_sem, meta_send, meta_recv, load_sem, rows_sem, grads_sem, swap_send, swap_recv, sums_sem, leaf_send, leaf_recv, shared_sem, shared_out):
    me, core, first, second, diag, partner = places()
    other = 1 - core
    bufs = (xbuf, dybuf)

    def own(which):
        return pltpu.make_async_copy((x_ref, dy_ref)[which], bufs[which].at[0], own_sem.at[which])

    def load(which, expert):
        src, dst = ((w1_ref, w1_buf), (w3_ref, w3_buf), (w2_ref, w2_buf))[which]
        return pltpu.make_async_copy(src.at[expert], dst.at[expert], load_sem.at[which, expert])

    def trip(array, part, kind):
        src, dst, device = ((0, 2, first), (0, 4, second), (0, 1, partner), (2, 6, second), (2, 3, partner), (4, 5, partner), (6, 7, partner))[kind]
        rows = pl.ds(part * PART, PART)
        return remote(bufs[array].at[src, rows], bufs[array].at[dst, rows], send_sem.at[array, part, kind], recv_sem.at[array, part, kind], device)

    def meta(which, role):
        device = (me, partner, first, partner + second - me, second, partner + first - me, diag, partner + diag - me)[role]
        table = (codes, gates)[which]
        seen = SEEN_AS[role]
        return remote(table.at[0], table.at[seen], meta_send.at[which, role], meta_recv.at[which, seen], device)

    def start(array, part, kind):
        trip(array, part, kind).start()

    def pass_over(array, part, kind, over):
        trip(array, part, kind).wait_recv()
        trip(array, part, over).start()

    def first_in(array, part):
        pass_over(array, part, TO_FIRST, FIRST_OVER)

    def second_in(array, part):
        pass_over(array, part, TO_SECOND, SECOND_OVER)

    def diag_in(array, part):
        pass_over(array, part, FIRST_ON, DIAG_OVER)

    def arrived(array, kind):
        for part in range(PARTS):
            trip(array, part, kind).wait_recv()

    def rows_out(array, half, at):
        return pltpu.make_async_copy((x_rows, z_rows)[array].at[at], (xr_ref, zr_ref)[array].at[half, at], rows_sem.at[array, half, at])

    def pick_x(half, low, high):
        def one(at, carry):
            role = half * 4 + at
            select = one_hot(codes[role], me * ROWS)
            picks[role] = select
            picks_partner[role] = one_hot(codes[role], partner * ROWS)
            for tile in range(4):
                cols = slice(tile * INNER, tile * INNER + INNER)
                x_rows[at, :, :, cols] = dot_nn(select, xbuf[role, :, cols]).astype(BF16).reshape(EXPERTS, SLOT, INNER)
            rows_out(X, half, at).start()
            return carry

        lax.fori_loop(low, high, one, 0)

    def pick_z(half, low, high):
        def one(at, carry):
            role = half * 4 + at
            slot = lax.broadcasted_iota(jnp.int32, (ROWS, TOKENS), 0) + me * ROWS
            spread = jnp.zeros((ROWS, TOKENS), F32)
            for choice in range(TOP_K):
                spread = jnp.where(slot == codes[role, choice:choice + 1, :], gates[role, choice:choice + 1, :], spread)
            scale = jnp.sum(spread, axis=1, keepdims=True)
            select = picks[role]
            for tile in range(4):
                cols = slice(tile * INNER, tile * INNER + INNER)
                value = dot_nn(select, dybuf[role, :, cols]) * scale
                z_rows[at, :, :, cols] = value.astype(BF16).reshape(EXPERTS, SLOT, INNER)
            rows_out(DY, half, at).start()
            return carry

        lax.fori_loop(low, high, one, 0)

    def activations(half, after):
        def one(expert, carry):
            if half == EARLY:
                load(0, expert).wait()
                load(1, expert).wait()
            rows = x_rows[:, expert].reshape(ROWS, WIDTH)
            acts[0, half, expert] = dot_nn(rows, w1_buf[expert]).astype(BF16)
            acts[1, half, expert] = dot_nn(rows, w3_buf[expert]).astype(BF16)
            for step, action in after.items():
                pl.when(expert == step)(action)
            return carry

        lax.fori_loop(0, EXPERTS, one, 0)

    def grads_out(which, half, expert):
        return pltpu.make_async_copy(grads.at[which, expert], (h_ref, da_ref, db_ref)[which].at[half, :, expert], grads_sem.at[which, half, expert])

    def sent_rows(expert):
        return r_send.at[pl.ds(expert * 4, 4)]

    def swap(half, expert):
        return remote(sent_rows(expert), r_got.at[half, expert], swap_send.at[half, expert], swap_recv.at[half, expert], partner)

    def rows_back(d_gate, d_up, expert, side, tile):
        at = pl.ds(pl.multiple_of(side * HALF + tile * INNER, INNER), INNER)
        value = dot_nt(d_gate, w1_buf[expert, at, :]) + dot_nt(d_up, w3_buf[expert, at, :])
        return value.astype(BF16).reshape(4, SLOT, INNER)

    def back(half, after):
        def send_side(expert, carry):
            if half == EARLY:
                load(2, expert).wait()
            grad_hidden = dot_nt(z_rows[:, expert].reshape(ROWS, WIDTH), w2_buf[expert])
            parts = swiglu_parts(acts[0, half, expert], acts[1, half, expert], grad_hidden)
            for which in range(3):
                if half == LATE:
                    grads_out(which, EARLY, expert).wait()
                grads[which, expert] = parts[which].reshape(4, SLOT, INNER)
                grads_out(which, half, expert).start()
            if half == LATE:
                swap(EARLY, expert).wait_send()
            for tile in range(2):
                r_send[pl.ds(expert * 4, 4), :, tile * INNER:(tile + 1) * INNER] = rows_back(parts[1], parts[2], expert, other, tile)
            swap(half, expert).start()
            for step, action in after.items():
                pl.when(expert == step)(action)
            return carry

        def own_side(expert, carry):
            d_gate = grads[1, expert].reshape(ROWS, INNER)
            d_up = grads[2, expert].reshape(ROWS, INNER)
            for tile in range(2):
                value = rows_back(d_gate, d_up, expert, core, tile)
                for at in range(4):
                    r_mine[(half * 4 + at) * EXPERTS + expert, :, tile * INNER:(tile + 1) * INNER] = value[at]
            return carry

        lax.fori_loop(0, EXPERTS, send_side, 0)
        lax.fori_loop(0, EXPERTS, own_side, 0)

    def sums_out(role):
        ref = {6: far_ref, 7: cross_ref, 4: near_ref.at[0], 5: near_ref.at[1], 0: base_ref.at[0], 1: base_ref.at[1]}[role]
        return pltpu.make_async_copy(sums.at[role % 4], ref, sums_sem.at[role])

    def leaf(which):
        return remote(sums.at[2 + which], leaf_ref.at[which], leaf_send.at[which], leaf_recv.at[which], (first, second)[which])

    def total(half):
        for expert in range(EXPERTS):
            swap(half, expert).wait_recv()
        for at in range(4):
            role = half * 4 + at
            if half == LATE:
                if at < 2:
                    sums_out(at).wait()
                else:
                    leaf(at - 2).wait_send()
            else:
                if at < 2:
                    shared_rows_out(at).wait()
            mine = r_mine[role * EXPERTS:(role + 1) * EXPERTS].reshape(ROWS, HALF)
            sums[at] = dot_tn(picks[role], mine) + dot_tn(picks_partner[role], r_got[half, :, at ^ 1].reshape(ROWS, HALF))
            if half == LATE or at < 2:
                sums_out(role).start()

    def shared_load(which):
        src, dst = ((s1_ref, r_mine.at[:, :, :INNER]), (s3_ref, r_mine.at[:, :, INNER:]), (s2_ref.at[:, :, :HALF], r_send.at[:8]), (s2_ref.at[:, :, HALF:], r_send.at[8:]))[which]
        return pltpu.make_async_copy(src, dst, shared_sem.at[which])

    def shared_rows_out(which):
        return pltpu.make_async_copy(sums.at[which], dx_ref.at[which], shared_out.at[which])

    def shared_parts_out(which):
        return pltpu.make_async_copy(acts.at[1, LATE, which, :TOKENS], parts_ref.at[which], shared_out.at[2 + which])

    def shared_chain():
        for which in range(4):
            shared_load(which).wait()
        x, dy = xbuf[0], dybuf[0]
        act_gate = dot_nn(x, r_mine[:, :, :INNER].reshape(WIDTH, INNER)).astype(BF16)
        act_up = dot_nn(x, r_mine[:, :, INNER:].reshape(WIDTH, INNER)).astype(BF16)
        grad_hidden = dot_nt(dy[:, :HALF], r_send[:8].reshape(INNER, HALF)) + dot_nt(dy[:, HALF:], r_send[8:].reshape(INNER, HALF))
        parts = swiglu_parts(act_gate, act_up, grad_hidden)
        for which in range(3):
            acts[1, LATE, which, :TOKENS] = parts[which]
            shared_parts_out(which).start()
        for which in range(2):
            for tile in range(2):
                at = slice((which * 2 + tile) * 8, (which * 2 + tile) * 8 + 8)
                gate_w = r_mine[at, :, :INNER].reshape(INNER, INNER)
                up_w = r_mine[at, :, INNER:].reshape(INNER, INNER)
                sums[which, :, tile * INNER:(tile + 1) * INNER] = dot_nt(parts[1], gate_w) + dot_nt(parts[2], up_w)
            shared_rows_out(which).start()

    for which in range(2):
        own(which).start()
    barrier = pltpu.get_barrier_semaphore()
    for step in range(1, ROLES):
        pl.semaphore_signal(barrier, inc=1, device_id={'ep': lax.rem(me + step, ROLES)}, device_id_type=MESH)
    codes[0] = jnp.zeros((16, TOKENS), jnp.int32)
    gates[0] = jnp.zeros((16, TOKENS), F32)
    codes[0, :TOP_K, :] = jnp.where(pos_ref[...] >= 0, ids_ref[...] * SLOT + pos_ref[...], -1)
    gates[0, :TOP_K, :] = gate_ref[...]
    for which in range(2):
        own(which).wait()
    pl.semaphore_wait(barrier, ROLES - 1)

    for role in SEEN_AS:
        for which in range(2):
            meta(which, role).start()
    for kind in (TO_FIRST, TO_PARTNER):
        for array in (X, DY):
            for part in range(PARTS):
                start(array, part, kind)
    for which in range(4):
        shared_load(which).start()
    for expert in range(EXPERTS):
        load(0, expert).start()
        load(1, expert).start()
    pick_x(EARLY, 0, 1)
    pick_z(EARLY, 0, 1)
    for role in SEEN_AS:
        for which in range(2):
            meta(which, role).wait_recv()
    arrived(X, TO_PARTNER)
    pick_x(EARLY, 1, 2)
    shared_chain()
    arrived(DY, TO_PARTNER)
    pick_z(EARLY, 1, 2)
    for part in range(PARTS):
        first_in(X, part)
    for expert in range(EXPERTS):
        load(2, expert).start()
    start(X, 0, TO_SECOND)
    arrived(X, FIRST_OVER)
    pick_x(EARLY, 2, 4)

    def queue_x():
        start(X, 1, TO_SECOND)
        start(X, 0, FIRST_ON)

    def queue_both():
        start(X, 1, FIRST_ON)
        first_in(DY, 0)
        start(DY, 0, TO_SECOND)

    def queue_dy():
        first_in(DY, 1)
        start(DY, 1, TO_SECOND)
        start(DY, 0, FIRST_ON)
        start(DY, 1, FIRST_ON)

    activations(EARLY, {0: queue_x, 1: queue_both, 3: queue_dy})
    arrived(DY, FIRST_OVER)
    pick_z(EARLY, 2, 4)

    def rest_x():
        second_in(X, 1)
        diag_in(X, 0)

    back(EARLY, {1: lambda: second_in(X, 0), 3: rest_x})
    total(EARLY)
    diag_in(X, 1)
    for array in (X, DY):
        for at in range(4):
            rows_out(array, EARLY, at).wait()
    arrived(X, SECOND_OVER)
    pick_x(LATE, 0, 2)
    arrived(X, DIAG_OVER)
    pick_x(LATE, 2, 4)
    for which in range(3):
        shared_parts_out(which).wait()
    activations(LATE, {1: lambda: second_in(DY, 0), 3: lambda: second_in(DY, 1)})
    diag_in(DY, 0)
    arrived(DY, SECOND_OVER)
    pick_z(LATE, 0, 2)
    diag_in(DY, 1)
    for which in range(2):
        leaf(which).start()
    arrived(DY, DIAG_OVER)
    pick_z(LATE, 2, 4)
    back(LATE, {})
    total(LATE)

    for array in (X, DY):
        for part in range(PARTS):
            for kind in range(TRIPS):
                trip(array, part, kind).wait_send()
    for role in SEEN_AS:
        for which in range(2):
            meta(which, role).wait_send()
    for expert in range(EXPERTS):
        swap(LATE, expert).wait_send()
        for which in range(3):
            grads_out(which, LATE, expert).wait()
    for which in range(2):
        leaf(which).wait_recv()
    for at in range(4):
        for array in (X, DY):
            rows_out(array, LATE, at).wait()
        sums_out(4 + at).wait()


def rows_backward(x_tokens, dy_tokens, expert_ids, slot_pos, gate_vals, w_gate, w_up, w_down, shared_gate, shared_up, shared_down):
    hbm = pl.BlockSpec(memory_space=pl.ANY)
    vmem = pl.BlockSpec(memory_space=pltpu.VMEM)
    rows = (2, 4, EXPERTS, SLOT, WIDTH)
    grads = (2, 4, EXPERTS, SLOT, INNER)
    pair = (2, TOKENS, HALF)
    parts = (3, TOKENS, INNER)
    blocks = (ROLES, TOKENS, WIDTH)
    tables = (ROLES, 16, TOKENS)
    select = (ROLES, ROWS, TOKENS)
    dma = pltpu.SemaphoreType.DMA
    outs = [(s, BF16) for s in (rows, rows, grads, grads, grads)] + [(pair[1:], F32)] * 2 + [(pair, F32)] * 4 + [(parts, BF16)]
    scratch = [(blocks, BF16), (blocks, BF16), (tables, jnp.int32), (tables, F32), (select, BF16), (select, BF16), (rows[1:], BF16), (rows[1:], BF16)]
    scratch += [(w.shape, BF16) for w in (w_gate, w_up, w_down)]
    scratch += [((2, 2, EXPERTS, ROWS, INNER), BF16), ((3, EXPERTS, 4, SLOT, INNER), BF16), ((16, SLOT, HALF), BF16), ((32, SLOT, HALF), BF16)]
    scratch += [((2, EXPERTS, 4, SLOT, HALF), BF16), ((4, TOKENS, HALF), F32)]
    trips = (2, PARTS, TRIPS)
    sems = [(2,), trips, trips, (2, ROLES), (2, ROLES), (3, EXPERTS), (2, 2, 4), (3, 2, EXPERTS), (2, EXPERTS), (2, EXPERTS), (ROLES,), (2,), (2,), (4,), (5,)]
    return pl.pallas_call(
        rows_kernel,
        out_shape=tuple(jax.ShapeDtypeStruct(s, d) for s, d in outs),
        in_specs=[hbm] * 2 + [vmem] * 3 + [hbm] * 6,
        out_specs=(hbm,) * len(outs),
        scratch_shapes=[pltpu.VMEM(s, d) for s, d in scratch] + [dma(s) for s in sems],
        compiler_params=pltpu.CompilerParams(collective_id=0, has_side_effects=True, vmem_limit_bytes=67000000),
        name='rows_backward',
    )(x_tokens, dy_tokens, expert_ids.T, slot_pos.T, gate_vals.T, w_gate, w_up, w_down, shared_gate.reshape(32, SLOT, INNER), shared_up.reshape(32, SLOT, INNER), shared_down.reshape(8, SLOT, WIDTH))


def down_kernel(z_ref, h_ref, x_ref, dy_ref, parts_ref, dw2_ref, s1_ref, s3_ref, s2_ref, s1_buf, s3_buf, s2_buf, sem):
    expert = pl.program_id(0)

    def shared_out(which):
        src, dst = ((s1_buf, s1_ref), (s3_buf, s3_ref), (s2_buf, s2_ref))[which]
        return pltpu.make_async_copy(src, dst.at[0], sem.at[which])

    @pl.when(expert == 0)
    def _():
        x_t = x_ref[...].T
        s1_buf[...] = dot_nn(x_t, parts_ref[1])
        shared_out(0).start()
        s3_buf[...] = dot_nn(x_t, parts_ref[2])
        shared_out(1).start()
        s2_buf[...] = dot_nn(parts_ref[0].T, dy_ref[...])
        shared_out(2).start()

    hidden_t = h_ref[:, 0].reshape(INNER, INNER).T
    for tile in range(4):
        cols = slice(tile * INNER, tile * INNER + INNER)
        dw2_ref[0, :, cols] = dot_nn(hidden_t, z_ref[:, 0, :, cols].reshape(INNER, INNER))

    @pl.when(expert == EXPERTS - 1)
    def _():
        for which in range(3):
            shared_out(which).wait()


def by_expert(inner):
    return pl.BlockSpec((ROLES, 1, SLOT, inner), lambda e: (0, e, 0, 0))


def down_grads(z_rows, hidden, x_tokens, dy_tokens, parts):
    vmem = pl.BlockSpec(memory_space=pltpu.VMEM)
    hbm = pl.BlockSpec(memory_space=pl.ANY)
    wide, tall = (1, INNER, WIDTH), (1, WIDTH, INNER)
    return pl.pallas_call(
        down_kernel,
        grid=(EXPERTS,),
        out_shape=(jax.ShapeDtypeStruct((EXPERTS, INNER, WIDTH), F32),) + tuple(jax.ShapeDtypeStruct(s, F32) for s in (tall, tall, wide)),
        in_specs=[by_expert(WIDTH), by_expert(INNER), vmem, vmem, vmem],
        out_specs=(pl.BlockSpec(wide, lambda e: (e, 0, 0)), hbm, hbm, hbm),
        scratch_shapes=[pltpu.VMEM(s[1:], F32) for s in (tall, tall, wide)] + [pltpu.SemaphoreType.DMA((3,))],
        compiler_params=pltpu.CompilerParams(dimension_semantics=('arbitrary',), vmem_limit_bytes=67000000),
        cost_estimate=pl.CostEstimate(flops=5_000_000_000, bytes_accessed=40_000_000, transcendentals=0),
        name='down_grads',
    )(z_rows, hidden, x_tokens, dy_tokens, parts)


def up_kernel(x_ref, da_ref, db_ref, dw1_ref, dw3_ref):
    for tile in range(4):
        cols = slice(tile * INNER, tile * INNER + INNER)
        x_t = x_ref[:, 0, :, cols].reshape(INNER, INNER).T
        dw1_ref[0, cols, :] = dot_nn(x_t, da_ref[:, 0].reshape(INNER, INNER))
        dw3_ref[0, cols, :] = dot_nn(x_t, db_ref[:, 0].reshape(INNER, INNER))


def up_grads(x_rows, d_gate, d_up):
    tall = pl.BlockSpec((1, WIDTH, INNER), lambda e: (e, 0, 0))
    return pl.pallas_call(
        up_kernel,
        grid=(EXPERTS,),
        out_shape=(jax.ShapeDtypeStruct((EXPERTS, WIDTH, INNER), F32),) * 2,
        in_specs=[by_expert(WIDTH), by_expert(INNER), by_expert(INNER)],
        out_specs=(tall, tall),
        compiler_params=pltpu.CompilerParams(dimension_semantics=('arbitrary',), vmem_limit_bytes=67000000),
        cost_estimate=pl.CostEstimate(flops=9_000_000_000, bytes_accessed=44_000_000, transcendentals=0),
        name='up_grads',
    )(x_rows, d_gate, d_up)


def partners(kind):
    pairs = []
    for me in range(8):
        core = me % 2
        along_x, along_y = me ^ 2, me ^ 4
        first, second = (along_x, along_y) if core == 0 else (along_y, along_x)
        pairs.append((me, {'first': first, 'second': second, 'chip': me ^ 1}[kind]))
    return pairs


def solution(mesh):
    token_spec = P(('dp', 'ep'), None)
    expert_spec = P('ep', None, None)
    whole_spec = P(None, None)
    grad_spec = P(('dp', 'ep'), None, None)

    def local_backward(x_tokens, dy_tokens, expert_ids, gate_vals, slot_pos, w_gate, w_up, w_down, shared_gate, shared_up, shared_down):
        *saved, far, cross, near, base, leaf, shared_dx, parts = rows_backward(x_tokens, dy_tokens, expert_ids, slot_pos, gate_vals, w_gate, w_up, w_down, shared_gate, shared_up, shared_down)
        x_rows, z_rows, hidden, d_gate, d_up = [rows.reshape((ROLES,) + rows.shape[2:]) for rows in saved]
        far = (lax.ppermute(far, 'ep', partners('first')), lax.ppermute(cross, 'ep', partners('second')))
        down = down_grads(z_rows, hidden, x_tokens, dy_tokens, parts)
        far, down = lax.optimization_barrier((far, down))
        last = (lax.ppermute(near[0] + far[0], 'ep', partners('second')), lax.ppermute(near[1] + far[1], 'ep', partners('first')))
        d_gate, *_ = lax.optimization_barrier((d_gate,) + tuple(far))
        up = up_grads(x_rows, d_gate, d_up)
        last, up = lax.optimization_barrier((last, up))
        own = base[0] + leaf[0] + last[0]
        swapped = lax.ppermute(base[1] + leaf[1] + last[1], 'ep', partners('chip'))
        core = lax.rem(lax.axis_index('ep'), 2)
        left = jnp.where(core == 0, own, swapped)
        right = jnp.where(core == 0, swapped, own)
        grad_x = jnp.concatenate((left + shared_dx[0], right + shared_dx[1]), axis=1).astype(BF16)
        return grad_x, up[0], up[1], down[0], down[1], down[2], down[3]

    return jax.shard_map(local_backward, mesh=mesh, in_specs=(token_spec, token_spec, token_spec, token_spec, token_spec, expert_spec, expert_spec, expert_spec, whole_spec, whole_spec, whole_spec), out_specs=(token_spec, grad_spec, grad_spec, grad_spec, grad_spec, grad_spec, grad_spec), check_vma=False)
```

```python
import jax
import jax.numpy as jnp
from jax import lax
from jax.experimental import pallas as pl
from jax.experimental.pallas import tpu as pltpu
from jax.sharding import PartitionSpec as P

MESH = pl.DeviceIdType.MESH
BF16 = jnp.bfloat16
F32 = jnp.float32
TOKENS, TOP_K, EXPERTS, ROLES, PARTS = 128, 10, 4, 8, 2
WIDTH, HALF, INNER, SLOT, PART = 2048, 1024, 512, 64, 64
ROWS = 256
X, DY = range(2)
EARLY, LATE = range(2)
TO_FIRST, TO_SECOND, TO_PARTNER, FIRST_ON, FIRST_OVER, SECOND_OVER, DIAG_OVER = range(7)
TRIPS = 7
SEEN_AS = {1: 1, 2: 2, 3: 5, 4: 4, 5: 3, 6: 6, 7: 7}


def swiglu_parts(act_gate, act_up, grad_hidden):
    gate_f32 = act_gate.astype(F32)
    up_f32 = act_up.astype(F32)
    sigma = jax.nn.sigmoid(gate_f32)
    silu_gate = gate_f32 * sigma
    hidden = (silu_gate * up_f32).astype(BF16)
    grad_gate = (grad_hidden * up_f32 * sigma * (1.0 + gate_f32 * (1.0 - sigma))).astype(BF16)
    grad_up = (grad_hidden * silu_gate).astype(BF16)
    return hidden, grad_gate, grad_up


def dot_nn(a, b):
    return lax.dot_general(a, b, (((1,), (0,)), ((), ())), preferred_element_type=F32)


def dot_nt(a, b):
    return lax.dot_general(a, b, (((1,), (1,)), ((), ())), preferred_element_type=F32)


def dot_tn(a, b):
    return lax.dot_general(a, b, (((0,), (0,)), ((), ())), preferred_element_type=F32)


def places():
    me = lax.axis_index('ep')
    core = lax.rem(me, 2)
    flip_x = 2 - 4 * lax.rem(me // 2, 2)
    flip_y = 4 - 8 * (me // 4)
    first = me + flip_x * (1 - core) + flip_y * core
    second = me + flip_y * (1 - core) + flip_x * core
    diag = me + flip_x + flip_y
    partner = me + 1 - 2 * core
    return me, core, first, second, diag, partner


def remote(src, dst, send_sem, recv_sem, device):
    return pltpu.make_async_remote_copy(src_ref=src, dst_ref=dst, send_sem=send_sem, recv_sem=recv_sem, device_id={'ep': device}, device_id_type=MESH)


def one_hot(code, base):
    slot = lax.broadcasted_iota(jnp.int32, (ROWS, TOKENS), 0) + base
    hits = jnp.zeros((ROWS, TOKENS), F32)
    for choice in range(TOP_K):
        hits = jnp.where(slot == code[choice:choice + 1, :], 1.0, hits)
    return hits.astype(BF16)


def rows_kernel(x_ref, dy_ref, ids_ref, pos_ref, gate_ref, w1_ref, w3_ref, w2_ref, s1_ref, s3_ref, s2_ref, xr_ref, zr_ref, h_ref, da_ref, db_ref, far_ref, cross_ref, near_ref, base_ref, leaf_ref, dx_ref, parts_ref, xbuf, dybuf, codes, gates, picks, picks_partner, x_rows, z_rows, w1_buf, w3_buf, w2_buf, acts, grads, r_send, r_mine, r_got, sums, own_sem, send_sem, recv_sem, meta_send, meta_recv, load_sem, rows_sem, grads_sem, swap_send, swap_recv, sums_sem, leaf_send, leaf_recv, shared_sem, shared_out):
    me, core, first, second, diag, partner = places()
    other = 1 - core
    bufs = (xbuf, dybuf)

    def own(which):
        return pltpu.make_async_copy((x_ref, dy_ref)[which], bufs[which].at[0], own_sem.at[which])

    def load(which, expert):
        src, dst = ((w1_ref, w1_buf), (w3_ref, w3_buf), (w2_ref, w2_buf))[which]
        return pltpu.make_async_copy(src.at[expert], dst.at[expert], load_sem.at[which, expert])

    def trip(array, part, kind):
        src, dst, device = ((0, 2, first), (0, 4, second), (0, 1, partner), (2, 6, second), (2, 3, partner), (4, 5, partner), (6, 7, partner))[kind]
        rows = pl.ds(part * PART, PART)
        return remote(bufs[array].at[src, rows], bufs[array].at[dst, rows], send_sem.at[array, part, kind], recv_sem.at[array, part, kind], device)

    def meta(which, role):
        device = (me, partner, first, partner + second - me, second, partner + first - me, diag, partner + diag - me)[role]
        table = (codes, gates)[which]
        seen = SEEN_AS[role]
        return remote(table.at[0], table.at[seen], meta_send.at[which, role], meta_recv.at[which, seen], device)

    def start(array, part, kind):
        trip(array, part, kind).start()

    def pass_over(array, part, kind, over):
        trip(array, part, kind).wait_recv()
        trip(array, part, over).start()

    def first_in(array, part):
        pass_over(array, part, TO_FIRST, FIRST_OVER)

    def second_in(array, part):
        pass_over(array, part, TO_SECOND, SECOND_OVER)

    def diag_in(array, part):
        pass_over(array, part, FIRST_ON, DIAG_OVER)

    def arrived(array, kind):
        for part in range(PARTS):
            trip(array, part, kind).wait_recv()

    def rows_out(array, half, at):
        return pltpu.make_async_copy((x_rows, z_rows)[array].at[at], (xr_ref, zr_ref)[array].at[half, at], rows_sem.at[array, half, at])

    def pick_x(half, low, high):
        def one(at, carry):
            role = half * 4 + at
            select = one_hot(codes[role], me * ROWS)
            picks[role] = select
            picks_partner[role] = one_hot(codes[role], partner * ROWS)
            for tile in range(4):
                cols = slice(tile * INNER, tile * INNER + INNER)
                x_rows[at, :, :, cols] = dot_nn(select, xbuf[role, :, cols]).astype(BF16).reshape(EXPERTS, SLOT, INNER)
            rows_out(X, half, at).start()
            return carry

        lax.fori_loop(low, high, one, 0)

    def pick_z(half, low, high):
        def one(at, carry):
            role = half * 4 + at
            slot = lax.broadcasted_iota(jnp.int32, (ROWS, TOKENS), 0) + me * ROWS
            spread = jnp.zeros((ROWS, TOKENS), F32)
            for choice in range(TOP_K):
                spread = jnp.where(slot == codes[role, choice:choice + 1, :], gates[role, choice:choice + 1, :], spread)
            scale = jnp.sum(spread, axis=1, keepdims=True)
            select = picks[role]
            for tile in range(4):
                cols = slice(tile * INNER, tile * INNER + INNER)
                value = dot_nn(select, dybuf[role, :, cols]) * scale
                z_rows[at, :, :, cols] = value.astype(BF16).reshape(EXPERTS, SLOT, INNER)
            rows_out(DY, half, at).start()
            return carry

        lax.fori_loop(low, high, one, 0)

    def activations(half, after):
        def one(expert, carry):
            if half == EARLY:
                load(0, expert).wait()
                load(1, expert).wait()
            rows = x_rows[:, expert].reshape(ROWS, WIDTH)
            acts[0, half, expert] = dot_nn(rows, w1_buf[expert]).astype(BF16)
            acts[1, half, expert] = dot_nn(rows, w3_buf[expert]).astype(BF16)
            for step, action in after.items():
                pl.when(expert == step)(action)
            return carry

        lax.fori_loop(0, EXPERTS, one, 0)

    def grads_out(which, half, expert):
        return pltpu.make_async_copy(grads.at[which, expert], (h_ref, da_ref, db_ref)[which].at[half, :, expert], grads_sem.at[which, half, expert])

    def sent_rows(expert):
        return r_send.at[pl.ds(expert * 4, 4)]

    def swap(half, expert):
        return remote(sent_rows(expert), r_got.at[half, expert], swap_send.at[half, expert], swap_recv.at[half, expert], partner)

    def rows_back(d_gate, d_up, expert, side, tile):
        at = pl.ds(pl.multiple_of(side * HALF + tile * INNER, INNER), INNER)
        value = dot_nt(d_gate, w1_buf[expert, at, :]) + dot_nt(d_up, w3_buf[expert, at, :])
        return value.astype(BF16).reshape(4, SLOT, INNER)

    def back(half, after):
        def send_side(expert, carry):
            if half == EARLY:
                load(2, expert).wait()
            grad_hidden = dot_nt(z_rows[:, expert].reshape(ROWS, WIDTH), w2_buf[expert])
            parts = swiglu_parts(acts[0, half, expert], acts[1, half, expert], grad_hidden)
            for which in range(3):
                if half == LATE:
                    grads_out(which, EARLY, expert).wait()
                grads[which, expert] = parts[which].reshape(4, SLOT, INNER)
                grads_out(which, half, expert).start()
            if half == LATE:
                swap(EARLY, expert).wait_send()
            for tile in range(2):
                r_send[pl.ds(expert * 4, 4), :, tile * INNER:(tile + 1) * INNER] = rows_back(parts[1], parts[2], expert, other, tile)
            swap(half, expert).start()
            for step, action in after.items():
                pl.when(expert == step)(action)
            return carry

        def own_side(expert, carry):
            d_gate = grads[1, expert].reshape(ROWS, INNER)
            d_up = grads[2, expert].reshape(ROWS, INNER)
            for tile in range(2):
                value = rows_back(d_gate, d_up, expert, core, tile)
                for at in range(4):
                    r_mine[(half * 4 + at) * EXPERTS + expert, :, tile * INNER:(tile + 1) * INNER] = value[at]
            return carry

        lax.fori_loop(0, EXPERTS, send_side, 0)
        lax.fori_loop(0, EXPERTS, own_side, 0)

    def sums_out(role):
        ref = {6: far_ref, 7: cross_ref, 4: near_ref.at[0], 5: near_ref.at[1], 0: base_ref.at[0], 1: base_ref.at[1]}[role]
        return pltpu.make_async_copy(sums.at[role % 4], ref, sums_sem.at[role])

    def leaf(which):
        return remote(sums.at[2 + which], leaf_ref.at[which], leaf_send.at[which], leaf_recv.at[which], (first, second)[which])

    def total(half):
        for expert in range(EXPERTS):
            swap(half, expert).wait_recv()
        for at in range(4):
            role = half * 4 + at
            if half == LATE:
                if at < 2:
                    sums_out(at).wait()
                else:
                    leaf(at - 2).wait_send()
            else:
                if at < 2:
                    shared_rows_out(at).wait()
            mine = r_mine[role * EXPERTS:(role + 1) * EXPERTS].reshape(ROWS, HALF)
            sums[at] = dot_tn(picks[role], mine) + dot_tn(picks_partner[role], r_got[half, :, at ^ 1].reshape(ROWS, HALF))
            if half == LATE or at < 2:
                sums_out(role).start()

    def shared_load(which):
        src, dst = ((s1_ref, r_mine.at[:, :, :INNER]), (s3_ref, r_mine.at[:, :, INNER:]), (s2_ref.at[:, :, :HALF], r_send.at[:8]), (s2_ref.at[:, :, HALF:], r_send.at[8:]))[which]
        return pltpu.make_async_copy(src, dst, shared_sem.at[which])

    def shared_rows_out(which):
        return pltpu.make_async_copy(sums.at[which], dx_ref.at[:, which * HALF:(which + 1) * HALF], shared_out.at[which])

    def shared_parts_out(which):
        return pltpu.make_async_copy(acts.at[1, LATE, which, :TOKENS], parts_ref.at[which], shared_out.at[2 + which])

    def shared_chain():
        x, dy = xbuf[0], dybuf[0]
        act_gate = dot_nn(x, r_mine[:, :, :INNER].reshape(WIDTH, INNER)).astype(BF16)
        act_up = dot_nn(x, r_mine[:, :, INNER:].reshape(WIDTH, INNER)).astype(BF16)
        grad_hidden = dot_nt(dy[:, :HALF], r_send[:8].reshape(INNER, HALF)) + dot_nt(dy[:, HALF:], r_send[8:].reshape(INNER, HALF))
        parts = swiglu_parts(act_gate, act_up, grad_hidden)
        for which in range(3):
            acts[1, LATE, which, :TOKENS] = parts[which]
            shared_parts_out(which).start()
        for which in range(2):
            for tile in range(2):
                at = slice((which * 2 + tile) * 8, (which * 2 + tile) * 8 + 8)
                gate_w = r_mine[at, :, :INNER].reshape(INNER, INNER)
                up_w = r_mine[at, :, INNER:].reshape(INNER, INNER)
                sums[which, :, tile * INNER:(tile + 1) * INNER] = dot_nt(parts[1], gate_w) + dot_nt(parts[2], up_w)
            shared_rows_out(which).start()

    for which in range(2):
        own(which).start()
    barrier = pltpu.get_barrier_semaphore()
    for step in range(1, ROLES):
        pl.semaphore_signal(barrier, inc=1, device_id={'ep': lax.rem(me + step, ROLES)}, device_id_type=MESH)
    codes[0] = jnp.zeros((16, TOKENS), jnp.int32)
    gates[0] = jnp.zeros((16, TOKENS), F32)
    codes[0, :TOP_K, :] = jnp.where(pos_ref[...] >= 0, ids_ref[...] * SLOT + pos_ref[...], -1)
    gates[0, :TOP_K, :] = gate_ref[...]
    for which in range(2):
        own(which).wait()
    pl.semaphore_wait(barrier, ROLES - 1)

    for role in SEEN_AS:
        for which in range(2):
            meta(which, role).start()
    for kind in (TO_FIRST, TO_PARTNER):
        for array in (X, DY):
            for part in range(PARTS):
                start(array, part, kind)
    for which in range(4):
        shared_load(which).start()
    pick_x(EARLY, 0, 1)
    pick_z(EARLY, 0, 1)
    for which in range(4):
        shared_load(which).wait()
    for expert in range(EXPERTS):
        load(0, expert).start()
        load(1, expert).start()
    shared_chain()
    first_in(X, 0)
    start(X, 0, TO_SECOND)
    for role in SEEN_AS:
        for which in range(2):
            meta(which, role).wait_recv()
    arrived(X, TO_PARTNER)
    pick_x(EARLY, 1, 2)
    first_in(X, 1)
    for expert in range(EXPERTS):
        load(2, expert).start()
    arrived(DY, TO_PARTNER)
    pick_z(EARLY, 1, 2)
    arrived(X, FIRST_OVER)
    pick_x(EARLY, 2, 4)

    def queue_x():
        start(X, 1, TO_SECOND)
        start(X, 0, FIRST_ON)

    def queue_both():
        start(X, 1, FIRST_ON)
        first_in(DY, 0)
        start(DY, 0, TO_SECOND)

    def queue_dy():
        first_in(DY, 1)
        start(DY, 1, TO_SECOND)
        start(DY, 0, FIRST_ON)
        start(DY, 1, FIRST_ON)

    activations(EARLY, {0: queue_x, 1: queue_both, 3: queue_dy})
    arrived(DY, FIRST_OVER)
    pick_z(EARLY, 2, 4)

    def rest_x():
        second_in(X, 1)
        diag_in(X, 0)

    back(EARLY, {1: lambda: second_in(X, 0), 3: rest_x})
    total(EARLY)
    diag_in(X, 1)
    for array in (X, DY):
        for at in range(4):
            rows_out(array, EARLY, at).wait()
    arrived(X, SECOND_OVER)
    pick_x(LATE, 0, 2)
    arrived(X, DIAG_OVER)
    pick_x(LATE, 2, 4)
    for which in range(3):
        shared_parts_out(which).wait()
    activations(LATE, {1: lambda: second_in(DY, 0), 3: lambda: second_in(DY, 1)})
    diag_in(DY, 0)
    arrived(DY, SECOND_OVER)
    pick_z(LATE, 0, 2)
    diag_in(DY, 1)
    for which in range(2):
        leaf(which).start()
    arrived(DY, DIAG_OVER)
    pick_z(LATE, 2, 4)
    back(LATE, {})
    total(LATE)

    for array in (X, DY):
        for part in range(PARTS):
            for kind in range(TRIPS):
                trip(array, part, kind).wait_send()
    for role in SEEN_AS:
        for which in range(2):
            meta(which, role).wait_send()
    for expert in range(EXPERTS):
        swap(LATE, expert).wait_send()
        for which in range(3):
            grads_out(which, LATE, expert).wait()
    for which in range(2):
        leaf(which).wait_recv()
    for at in range(4):
        for array in (X, DY):
            rows_out(array, LATE, at).wait()
        sums_out(4 + at).wait()


def rows_backward(x_tokens, dy_tokens, expert_ids, slot_pos, gate_vals, w_gate, w_up, w_down, shared_gate, shared_up, shared_down):
    hbm = pl.BlockSpec(memory_space=pl.ANY)
    vmem = pl.BlockSpec(memory_space=pltpu.VMEM)
    rows = (2, 4, EXPERTS, SLOT, WIDTH)
    grads = (2, 4, EXPERTS, SLOT, INNER)
    pair = (2, TOKENS, HALF)
    parts = (3, TOKENS, INNER)
    blocks = (ROLES, TOKENS, WIDTH)
    tables = (ROLES, 16, TOKENS)
    select = (ROLES, ROWS, TOKENS)
    dma = pltpu.SemaphoreType.DMA
    outs = [(s, BF16) for s in (rows, rows, grads, grads, grads)] + [(pair[1:], F32)] * 2 + [(pair, F32)] * 3 + [((TOKENS, WIDTH), F32), (parts, BF16)]
    scratch = [(blocks, BF16), (blocks, BF16), (tables, jnp.int32), (tables, F32), (select, BF16), (select, BF16), (rows[1:], BF16), (rows[1:], BF16)]
    scratch += [(w.shape, BF16) for w in (w_gate, w_up, w_down)]
    scratch += [((2, 2, EXPERTS, ROWS, INNER), BF16), ((3, EXPERTS, 4, SLOT, INNER), BF16), ((16, SLOT, HALF), BF16), ((32, SLOT, HALF), BF16)]
    scratch += [((2, EXPERTS, 4, SLOT, HALF), BF16), ((4, TOKENS, HALF), F32)]
    trips = (2, PARTS, TRIPS)
    sems = [(2,), trips, trips, (2, ROLES), (2, ROLES), (3, EXPERTS), (2, 2, 4), (3, 2, EXPERTS), (2, EXPERTS), (2, EXPERTS), (ROLES,), (2,), (2,), (4,), (5,)]
    return pl.pallas_call(
        rows_kernel,
        out_shape=tuple(jax.ShapeDtypeStruct(s, d) for s, d in outs),
        in_specs=[hbm] * 2 + [vmem] * 3 + [hbm] * 6,
        out_specs=(hbm,) * len(outs),
        scratch_shapes=[pltpu.VMEM(s, d) for s, d in scratch] + [dma(s) for s in sems],
        compiler_params=pltpu.CompilerParams(collective_id=0, has_side_effects=True, vmem_limit_bytes=67000000),
        name='rows_backward',
    )(x_tokens, dy_tokens, expert_ids.T, slot_pos.T, gate_vals.T, w_gate, w_up, w_down, shared_gate.reshape(32, SLOT, INNER), shared_up.reshape(32, SLOT, INNER), shared_down.reshape(8, SLOT, WIDTH))


def down_kernel(z_ref, h_ref, x_ref, dy_ref, parts_ref, dw2_ref, s1_ref, s3_ref, s2_ref, s1_buf, s3_buf, s2_buf, sem):
    expert = pl.program_id(0)

    def shared_out(which):
        src, dst = ((s1_buf, s1_ref), (s3_buf, s3_ref), (s2_buf, s2_ref))[which]
        return pltpu.make_async_copy(src, dst.at[0], sem.at[which])

    @pl.when(expert == 0)
    def _():
        x_t = x_ref[...].T
        s1_buf[...] = dot_nn(x_t, parts_ref[1])
        shared_out(0).start()
        s3_buf[...] = dot_nn(x_t, parts_ref[2])
        shared_out(1).start()
        s2_buf[...] = dot_nn(parts_ref[0].T, dy_ref[...])
        shared_out(2).start()

    hidden_t = h_ref[:, 0].reshape(INNER, INNER).T
    for tile in range(4):
        cols = slice(tile * INNER, tile * INNER + INNER)
        dw2_ref[0, :, cols] = dot_nn(hidden_t, z_ref[:, 0, :, cols].reshape(INNER, INNER))

    @pl.when(expert == EXPERTS - 1)
    def _():
        for which in range(3):
            shared_out(which).wait()


def by_expert(inner):
    return pl.BlockSpec((ROLES, 1, SLOT, inner), lambda e: (0, e, 0, 0))


def down_grads(z_rows, hidden, x_tokens, dy_tokens, parts):
    vmem = pl.BlockSpec(memory_space=pltpu.VMEM)
    hbm = pl.BlockSpec(memory_space=pl.ANY)
    wide, tall = (1, INNER, WIDTH), (1, WIDTH, INNER)
    return pl.pallas_call(
        down_kernel,
        grid=(EXPERTS,),
        out_shape=(jax.ShapeDtypeStruct((EXPERTS, INNER, WIDTH), F32),) + tuple(jax.ShapeDtypeStruct(s, F32) for s in (tall, tall, wide)),
        in_specs=[by_expert(WIDTH), by_expert(INNER), vmem, vmem, vmem],
        out_specs=(pl.BlockSpec(wide, lambda e: (e, 0, 0)), hbm, hbm, hbm),
        scratch_shapes=[pltpu.VMEM(s[1:], F32) for s in (tall, tall, wide)] + [pltpu.SemaphoreType.DMA((3,))],
        compiler_params=pltpu.CompilerParams(dimension_semantics=('arbitrary',), vmem_limit_bytes=67000000),
        cost_estimate=pl.CostEstimate(flops=5_000_000_000, bytes_accessed=40_000_000, transcendentals=0),
        name='down_grads',
    )(z_rows, hidden, x_tokens, dy_tokens, parts)


def up_kernel(x_ref, da_ref, db_ref, dw1_ref, dw3_ref):
    for tile in range(4):
        cols = slice(tile * INNER, tile * INNER + INNER)
        x_t = x_ref[:, 0, :, cols].reshape(INNER, INNER).T
        dw1_ref[0, cols, :] = dot_nn(x_t, da_ref[:, 0].reshape(INNER, INNER))
        dw3_ref[0, cols, :] = dot_nn(x_t, db_ref[:, 0].reshape(INNER, INNER))


def up_grads(x_rows, d_gate, d_up):
    tall = pl.BlockSpec((1, WIDTH, INNER), lambda e: (e, 0, 0))
    return pl.pallas_call(
        up_kernel,
        grid=(EXPERTS,),
        out_shape=(jax.ShapeDtypeStruct((EXPERTS, WIDTH, INNER), F32),) * 2,
        in_specs=[by_expert(WIDTH), by_expert(INNER), by_expert(INNER)],
        out_specs=(tall, tall),
        compiler_params=pltpu.CompilerParams(dimension_semantics=('arbitrary',), vmem_limit_bytes=67000000),
        cost_estimate=pl.CostEstimate(flops=9_000_000_000, bytes_accessed=44_000_000, transcendentals=0),
        name='up_grads',
    )(x_rows, d_gate, d_up)


def partners(kind):
    pairs = []
    for me in range(8):
        core = me % 2
        along_x, along_y = me ^ 2, me ^ 4
        first, second = (along_x, along_y) if core == 0 else (along_y, along_x)
        pairs.append((me, {'first': first, 'second': second, 'chip': me ^ 1}[kind]))
    return pairs


def solution(mesh):
    token_spec = P(('dp', 'ep'), None)
    expert_spec = P('ep', None, None)
    whole_spec = P(None, None)
    grad_spec = P(('dp', 'ep'), None, None)

    def local_backward(x_tokens, dy_tokens, expert_ids, gate_vals, slot_pos, w_gate, w_up, w_down, shared_gate, shared_up, shared_down):
        *saved, far, cross, near, base, leaf, shared_dx, parts = rows_backward(x_tokens, dy_tokens, expert_ids, slot_pos, gate_vals, w_gate, w_up, w_down, shared_gate, shared_up, shared_down)
        x_rows, z_rows, hidden, d_gate, d_up = [rows.reshape((ROLES,) + rows.shape[2:]) for rows in saved]
        far = (lax.ppermute(far, 'ep', partners('first')), lax.ppermute(cross, 'ep', partners('second')))
        down = down_grads(z_rows, hidden, x_tokens, dy_tokens, parts)
        far, down = lax.optimization_barrier((far, down))
        last = (lax.ppermute(near[0] + far[0], 'ep', partners('second')), lax.ppermute(near[1] + far[1], 'ep', partners('first')))
        d_gate, *_ = lax.optimization_barrier((d_gate,) + tuple(far))
        up = up_grads(x_rows, d_gate, d_up)
        last, up = lax.optimization_barrier((last, up))
        own = base[0] + leaf[0] + last[0]
        swapped = lax.ppermute(base[1] + leaf[1] + last[1], 'ep', partners('chip'))
        core = lax.rem(lax.axis_index('ep'), 2)
        left = jnp.where(core == 0, own, swapped)
        right = jnp.where(core == 0, swapped, own)
        grad_x = (jnp.concatenate((left, right), axis=1) + shared_dx).astype(BF16)
        return grad_x, up[0], up[1], down[0], down[1], down[2], down[3]

    return jax.shard_map(local_backward, mesh=mesh, in_specs=(token_spec, token_spec, token_spec, token_spec, token_spec, expert_spec, expert_spec, expert_spec, whole_spec, whole_spec, whole_spec), out_specs=(token_spec, grad_spec, grad_spec, grad_spec, grad_spec, grad_spec, grad_spec), check_vma=False)
```

```python
import jax
import jax.numpy as jnp
from jax import lax
from jax.experimental import pallas as pl
from jax.experimental.pallas import tpu as pltpu
from jax.sharding import PartitionSpec as P

MESH = pl.DeviceIdType.MESH
BF16 = jnp.bfloat16
F32 = jnp.float32
TOKENS, TOP_K, EXPERTS, ROLES, PARTS = 128, 10, 4, 8, 2
WIDTH, HALF, INNER, SLOT, PART = 2048, 1024, 512, 64, 64
ROWS = 256
X, DY = range(2)
EARLY, LATE = range(2)
TO_FIRST, TO_SECOND, TO_PARTNER, FIRST_ON, FIRST_OVER, SECOND_OVER, DIAG_OVER = range(7)
TRIPS = 7
SEEN_AS = {1: 1, 2: 2, 3: 5, 4: 4, 5: 3, 6: 6, 7: 7}


def swiglu_parts(act_gate, act_up, grad_hidden):
    gate_f32 = act_gate.astype(F32)
    up_f32 = act_up.astype(F32)
    sigma = jax.nn.sigmoid(gate_f32)
    silu_gate = gate_f32 * sigma
    hidden = (silu_gate * up_f32).astype(BF16)
    grad_gate = (grad_hidden * up_f32 * sigma * (1.0 + gate_f32 * (1.0 - sigma))).astype(BF16)
    grad_up = (grad_hidden * silu_gate).astype(BF16)
    return hidden, grad_gate, grad_up


def dot_nn(a, b):
    return lax.dot_general(a, b, (((1,), (0,)), ((), ())), preferred_element_type=F32)


def dot_nt(a, b):
    return lax.dot_general(a, b, (((1,), (1,)), ((), ())), preferred_element_type=F32)


def dot_tn(a, b):
    return lax.dot_general(a, b, (((0,), (0,)), ((), ())), preferred_element_type=F32)


def places():
    me = lax.axis_index('ep')
    core = lax.rem(me, 2)
    flip_x = 2 - 4 * lax.rem(me // 2, 2)
    flip_y = 4 - 8 * (me // 4)
    first = me + flip_x * (1 - core) + flip_y * core
    second = me + flip_y * (1 - core) + flip_x * core
    diag = me + flip_x + flip_y
    partner = me + 1 - 2 * core
    return me, core, first, second, diag, partner


def remote(src, dst, send_sem, recv_sem, device):
    return pltpu.make_async_remote_copy(src_ref=src, dst_ref=dst, send_sem=send_sem, recv_sem=recv_sem, device_id={'ep': device}, device_id_type=MESH)


def one_hot(code, base):
    slot = lax.broadcasted_iota(jnp.int32, (ROWS, TOKENS), 0) + base
    hits = jnp.zeros((ROWS, TOKENS), F32)
    for choice in range(TOP_K):
        hits = jnp.where(slot == code[choice:choice + 1, :], 1.0, hits)
    return hits.astype(BF16)


def unrolled(low, high, step):
    for index in range(low, high):
        step(index, 0)


def rows_kernel(x_ref, dy_ref, ids_ref, pos_ref, gate_ref, w1_ref, w3_ref, w2_ref, s1_ref, s3_ref, s2_ref, xr_ref, zr_ref, h_ref, da_ref, db_ref, far_ref, cross_ref, near_ref, base_ref, leaf_ref, dx_ref, parts_ref, xbuf, dybuf, codes, gates, picks, picks_partner, x_rows, z_rows, w1_buf, w3_buf, w2_buf, acts, grads, r_send, r_mine, r_got, sums, own_sem, send_sem, recv_sem, meta_send, meta_recv, load_sem, rows_sem, grads_sem, swap_send, swap_recv, sums_sem, leaf_send, leaf_recv, shared_sem, shared_out):
    me, core, first, second, diag, partner = places()
    other = 1 - core
    bufs = (xbuf, dybuf)

    def own(which):
        return pltpu.make_async_copy((x_ref, dy_ref)[which], bufs[which].at[0], own_sem.at[which])

    def load(which, expert):
        src, dst = ((w1_ref, w1_buf), (w3_ref, w3_buf), (w2_ref, w2_buf))[which]
        return pltpu.make_async_copy(src.at[expert], dst.at[expert], load_sem.at[which, expert])

    def trip(array, part, kind):
        src, dst, device = ((0, 2, first), (0, 4, second), (0, 1, partner), (2, 6, second), (2, 3, partner), (4, 5, partner), (6, 7, partner))[kind]
        rows = pl.ds(part * PART, PART)
        return remote(bufs[array].at[src, rows], bufs[array].at[dst, rows], send_sem.at[array, part, kind], recv_sem.at[array, part, kind], device)

    def meta(which, role):
        device = (me, partner, first, partner + second - me, second, partner + first - me, diag, partner + diag - me)[role]
        table = (codes, gates)[which]
        seen = SEEN_AS[role]
        return remote(table.at[0], table.at[seen], meta_send.at[which, role], meta_recv.at[which, seen], device)

    def start(array, part, kind):
        trip(array, part, kind).start()

    def pass_over(array, part, kind, over):
        trip(array, part, kind).wait_recv()
        trip(array, part, over).start()

    def first_in(array, part):
        pass_over(array, part, TO_FIRST, FIRST_OVER)

    def second_in(array, part):
        pass_over(array, part, TO_SECOND, SECOND_OVER)

    def diag_in(array, part):
        pass_over(array, part, FIRST_ON, DIAG_OVER)

    def arrived(array, kind):
        for part in range(PARTS):
            trip(array, part, kind).wait_recv()

    def rows_out(array, half, at):
        return pltpu.make_async_copy((x_rows, z_rows)[array].at[at], (xr_ref, zr_ref)[array].at[half, at], rows_sem.at[array, half, at])

    def pick_x(half, low, high):
        def one(at, carry):
            role = half * 4 + at
            select = one_hot(codes[role], me * ROWS)
            picks[role] = select
            picks_partner[role] = one_hot(codes[role], partner * ROWS)
            for tile in range(4):
                cols = slice(tile * INNER, tile * INNER + INNER)
                x_rows[at, :, :, cols] = dot_nn(select, xbuf[role, :, cols]).astype(BF16).reshape(EXPERTS, SLOT, INNER)
            rows_out(X, half, at).start()
            return carry

        unrolled(low, high, one)

    def pick_z(half, low, high):
        def one(at, carry):
            role = half * 4 + at
            slot = lax.broadcasted_iota(jnp.int32, (ROWS, TOKENS), 0) + me * ROWS
            spread = jnp.zeros((ROWS, TOKENS), F32)
            for choice in range(TOP_K):
                spread = jnp.where(slot == codes[role, choice:choice + 1, :], gates[role, choice:choice + 1, :], spread)
            scale = jnp.sum(spread, axis=1, keepdims=True)
            select = picks[role]
            for tile in range(4):
                cols = slice(tile * INNER, tile * INNER + INNER)
                value = dot_nn(select, dybuf[role, :, cols]) * scale
                z_rows[at, :, :, cols] = value.astype(BF16).reshape(EXPERTS, SLOT, INNER)
            rows_out(DY, half, at).start()
            return carry

        unrolled(low, high, one)

    def activations(half, after):
        def one(expert, carry):
            if half == EARLY:
                load(0, expert).wait()
                load(1, expert).wait()
            rows = x_rows[:, expert].reshape(ROWS, WIDTH)
            acts[0, half, expert] = dot_nn(rows, w1_buf[expert]).astype(BF16)
            acts[1, half, expert] = dot_nn(rows, w3_buf[expert]).astype(BF16)
            if expert in after:
                after[expert]()

        unrolled(0, EXPERTS, one)

    def grads_out(which, half, expert):
        return pltpu.make_async_copy(grads.at[which, expert], (h_ref, da_ref, db_ref)[which].at[half, :, expert], grads_sem.at[which, half, expert])

    def sent_rows(expert):
        return r_send.at[pl.ds(expert * 4, 4)]

    def swap(half, expert):
        return remote(sent_rows(expert), r_got.at[half, expert], swap_send.at[half, expert], swap_recv.at[half, expert], partner)

    def rows_back(d_gate, d_up, expert, side, tile):
        at = pl.ds(pl.multiple_of(side * HALF + tile * INNER, INNER), INNER)
        value = dot_nt(d_gate, w1_buf[expert, at, :]) + dot_nt(d_up, w3_buf[expert, at, :])
        return value.astype(BF16).reshape(4, SLOT, INNER)

    def back(half, after):
        def send_side(expert, carry):
            if half == EARLY:
                load(2, expert).wait()
            grad_hidden = dot_nt(z_rows[:, expert].reshape(ROWS, WIDTH), w2_buf[expert])
            parts = swiglu_parts(acts[0, half, expert], acts[1, half, expert], grad_hidden)
            for which in range(3):
                if half == LATE:
                    grads_out(which, EARLY, expert).wait()
                grads[which, expert] = parts[which].reshape(4, SLOT, INNER)
                grads_out(which, half, expert).start()
            if half == LATE:
                swap(EARLY, expert).wait_send()
            for tile in range(2):
                r_send[pl.ds(expert * 4, 4), :, tile * INNER:(tile + 1) * INNER] = rows_back(parts[1], parts[2], expert, other, tile)
            swap(half, expert).start()
            for step, action in after.items():
                pl.when(expert == step)(action)
            return carry

        def own_side(expert, carry):
            d_gate = grads[1, expert].reshape(ROWS, INNER)
            d_up = grads[2, expert].reshape(ROWS, INNER)
            for tile in range(2):
                value = rows_back(d_gate, d_up, expert, core, tile)
                for at in range(4):
                    r_mine[(half * 4 + at) * EXPERTS + expert, :, tile * INNER:(tile + 1) * INNER] = value[at]
            return carry

        lax.fori_loop(0, EXPERTS, send_side, 0)
        lax.fori_loop(0, EXPERTS, own_side, 0)

    def sums_out(role):
        ref = {6: far_ref, 7: cross_ref, 4: near_ref.at[0], 5: near_ref.at[1], 0: base_ref.at[0], 1: base_ref.at[1]}[role]
        return pltpu.make_async_copy(sums.at[role % 4], ref, sums_sem.at[role])

    def leaf(which):
        return remote(sums.at[2 + which], leaf_ref.at[which], leaf_send.at[which], leaf_recv.at[which], (first, second)[which])

    def total(half):
        for expert in range(EXPERTS):
            swap(half, expert).wait_recv()
        for at in range(4):
            role = half * 4 + at
            if half == LATE:
                if at < 2:
                    sums_out(at).wait()
                else:
                    leaf(at - 2).wait_send()
            else:
                if at < 2:
                    shared_rows_out(at).wait()
            mine = r_mine[role * EXPERTS:(role + 1) * EXPERTS].reshape(ROWS, HALF)
            sums[at] = dot_tn(picks[role], mine) + dot_tn(picks_partner[role], r_got[half, :, at ^ 1].reshape(ROWS, HALF))
            if half == LATE or at < 2:
                sums_out(role).start()

    def shared_load(which):
        src, dst = ((s1_ref, r_mine.at[:, :, :INNER]), (s3_ref, r_mine.at[:, :, INNER:]), (s2_ref.at[:, :, :HALF], r_send.at[:8]), (s2_ref.at[:, :, HALF:], r_send.at[8:]))[which]
        return pltpu.make_async_copy(src, dst, shared_sem.at[which])

    def shared_rows_out(which):
        return pltpu.make_async_copy(sums.at[which], dx_ref.at[:, which * HALF:(which + 1) * HALF], shared_out.at[which])

    def shared_parts_out(which):
        return pltpu.make_async_copy(acts.at[1, LATE, which, :TOKENS], parts_ref.at[which], shared_out.at[2 + which])

    def shared_chain():
        x, dy = xbuf[0], dybuf[0]
        act_gate = dot_nn(x, r_mine[:, :, :INNER].reshape(WIDTH, INNER)).astype(BF16)
        act_up = dot_nn(x, r_mine[:, :, INNER:].reshape(WIDTH, INNER)).astype(BF16)
        grad_hidden = dot_nt(dy[:, :HALF], r_send[:8].reshape(INNER, HALF)) + dot_nt(dy[:, HALF:], r_send[8:].reshape(INNER, HALF))
        parts = swiglu_parts(act_gate, act_up, grad_hidden)
        for which in range(3):
            acts[1, LATE, which, :TOKENS] = parts[which]
            shared_parts_out(which).start()
        for which in range(2):
            for tile in range(2):
                at = slice((which * 2 + tile) * 8, (which * 2 + tile) * 8 + 8)
                gate_w = r_mine[at, :, :INNER].reshape(INNER, INNER)
                up_w = r_mine[at, :, INNER:].reshape(INNER, INNER)
                sums[which, :, tile * INNER:(tile + 1) * INNER] = dot_nt(parts[1], gate_w) + dot_nt(parts[2], up_w)
            shared_rows_out(which).start()

    for which in range(2):
        own(which).start()
    barrier = pltpu.get_barrier_semaphore()
    for step in range(1, ROLES):
        pl.semaphore_signal(barrier, inc=1, device_id={'ep': lax.rem(me + step, ROLES)}, device_id_type=MESH)
    codes[0] = jnp.zeros((16, TOKENS), jnp.int32)
    gates[0] = jnp.zeros((16, TOKENS), F32)
    codes[0, :TOP_K, :] = jnp.where(pos_ref[...] >= 0, ids_ref[...] * SLOT + pos_ref[...], -1)
    gates[0, :TOP_K, :] = gate_ref[...]
    for which in range(2):
        own(which).wait()
    pl.semaphore_wait(barrier, ROLES - 1)

    for role in SEEN_AS:
        for which in range(2):
            meta(which, role).start()
    for kind in (TO_FIRST, TO_PARTNER):
        for array in (X, DY):
            for part in range(PARTS):
                start(array, part, kind)
    for which in range(4):
        shared_load(which).start()
    pick_x(EARLY, 0, 1)
    pick_z(EARLY, 0, 1)
    for which in range(4):
        shared_load(which).wait()
    for expert in range(EXPERTS):
        load(0, expert).start()
        load(1, expert).start()
    shared_chain()
    first_in(X, 0)
    start(X, 0, TO_SECOND)
    for role in SEEN_AS:
        for which in range(2):
            meta(which, role).wait_recv()
    arrived(X, TO_PARTNER)
    pick_x(EARLY, 1, 2)
    first_in(X, 1)
    for expert in range(EXPERTS):
        load(2, expert).start()
    arrived(DY, TO_PARTNER)
    pick_z(EARLY, 1, 2)
    arrived(X, FIRST_OVER)
    pick_x(EARLY, 2, 4)

    def queue_x():
        start(X, 1, TO_SECOND)
        start(X, 0, FIRST_ON)

    def queue_both():
        start(X, 1, FIRST_ON)
        first_in(DY, 0)
        start(DY, 0, TO_SECOND)

    def queue_dy():
        first_in(DY, 1)
        start(DY, 1, TO_SECOND)
        start(DY, 0, FIRST_ON)
        start(DY, 1, FIRST_ON)

    activations(EARLY, {0: queue_x, 1: queue_both, 3: queue_dy})
    arrived(DY, FIRST_OVER)
    pick_z(EARLY, 2, 4)

    def rest_x():
        second_in(X, 1)
        diag_in(X, 0)

    back(EARLY, {1: lambda: second_in(X, 0), 3: rest_x})
    total(EARLY)
    diag_in(X, 1)
    for array in (X, DY):
        for at in range(4):
            rows_out(array, EARLY, at).wait()
    arrived(X, SECOND_OVER)
    pick_x(LATE, 0, 2)
    arrived(X, DIAG_OVER)
    pick_x(LATE, 2, 4)
    for which in range(3):
        shared_parts_out(which).wait()
    activations(LATE, {1: lambda: second_in(DY, 0), 3: lambda: second_in(DY, 1)})
    diag_in(DY, 0)
    diag_in(DY, 1)
    for which in range(2):
        leaf(which).start()
    arrived(DY, SECOND_OVER)
    pick_z(LATE, 0, 2)
    arrived(DY, DIAG_OVER)
    pick_z(LATE, 2, 4)
    back(LATE, {})
    total(LATE)

    for array in (X, DY):
        for part in range(PARTS):
            for kind in range(TRIPS):
                trip(array, part, kind).wait_send()
    for role in SEEN_AS:
        for which in range(2):
            meta(which, role).wait_send()
    for expert in range(EXPERTS):
        swap(LATE, expert).wait_send()
        for which in range(3):
            grads_out(which, LATE, expert).wait()
    for which in range(2):
        leaf(which).wait_recv()
    for at in range(4):
        for array in (X, DY):
            rows_out(array, LATE, at).wait()
        sums_out(4 + at).wait()


def rows_backward(x_tokens, dy_tokens, expert_ids, slot_pos, gate_vals, w_gate, w_up, w_down, shared_gate, shared_up, shared_down):
    hbm = pl.BlockSpec(memory_space=pl.ANY)
    vmem = pl.BlockSpec(memory_space=pltpu.VMEM)
    rows = (2, 4, EXPERTS, SLOT, WIDTH)
    grads = (2, 4, EXPERTS, SLOT, INNER)
    pair = (2, TOKENS, HALF)
    parts = (3, TOKENS, INNER)
    blocks = (ROLES, TOKENS, WIDTH)
    tables = (ROLES, 16, TOKENS)
    select = (ROLES, ROWS, TOKENS)
    dma = pltpu.SemaphoreType.DMA
    outs = [(s, BF16) for s in (rows, rows, grads, grads, grads)] + [(pair[1:], F32)] * 2 + [(pair, F32)] * 3 + [((TOKENS, WIDTH), F32), (parts, BF16)]
    scratch = [(blocks, BF16), (blocks, BF16), (tables, jnp.int32), (tables, F32), (select, BF16), (select, BF16), (rows[1:], BF16), (rows[1:], BF16)]
    scratch += [(w.shape, BF16) for w in (w_gate, w_up, w_down)]
    scratch += [((2, 2, EXPERTS, ROWS, INNER), BF16), ((3, EXPERTS, 4, SLOT, INNER), BF16), ((16, SLOT, HALF), BF16), ((32, SLOT, HALF), BF16)]
    scratch += [((2, EXPERTS, 4, SLOT, HALF), BF16), ((4, TOKENS, HALF), F32)]
    trips = (2, PARTS, TRIPS)
    sems = [(2,), trips, trips, (2, ROLES), (2, ROLES), (3, EXPERTS), (2, 2, 4), (3, 2, EXPERTS), (2, EXPERTS), (2, EXPERTS), (ROLES,), (2,), (2,), (4,), (5,)]
    return pl.pallas_call(
        rows_kernel,
        out_shape=tuple(jax.ShapeDtypeStruct(s, d) for s, d in outs),
        in_specs=[hbm] * 2 + [vmem] * 3 + [hbm] * 6,
        out_specs=(hbm,) * len(outs),
        scratch_shapes=[pltpu.VMEM(s, d) for s, d in scratch] + [dma(s) for s in sems],
        compiler_params=pltpu.CompilerParams(collective_id=0, has_side_effects=True, vmem_limit_bytes=67000000),
        name='rows_backward',
    )(x_tokens, dy_tokens, expert_ids.T, slot_pos.T, gate_vals.T, w_gate, w_up, w_down, shared_gate.reshape(32, SLOT, INNER), shared_up.reshape(32, SLOT, INNER), shared_down.reshape(8, SLOT, WIDTH))


def down_kernel(z_ref, h_ref, x_ref, dy_ref, parts_ref, dw2_ref, s1_ref, s3_ref, s2_ref, s1_buf, s3_buf, s2_buf, sem):
    expert = pl.program_id(0)

    def shared_out(which):
        src, dst = ((s1_buf, s1_ref), (s3_buf, s3_ref), (s2_buf, s2_ref))[which]
        return pltpu.make_async_copy(src, dst.at[0], sem.at[which])

    @pl.when(expert == 0)
    def _():
        x_t = x_ref[...].T
        s1_buf[...] = dot_nn(x_t, parts_ref[1])
        shared_out(0).start()
        s3_buf[...] = dot_nn(x_t, parts_ref[2])
        shared_out(1).start()
        s2_buf[...] = dot_nn(parts_ref[0].T, dy_ref[...])
        shared_out(2).start()

    hidden_t = h_ref[:, 0].reshape(INNER, INNER).T
    for tile in range(4):
        cols = slice(tile * INNER, tile * INNER + INNER)
        dw2_ref[0, :, cols] = dot_nn(hidden_t, z_ref[:, 0, :, cols].reshape(INNER, INNER))

    @pl.when(expert == EXPERTS - 1)
    def _():
        for which in range(3):
            shared_out(which).wait()


def by_expert(inner):
    return pl.BlockSpec((ROLES, 1, SLOT, inner), lambda e: (0, e, 0, 0))


def down_grads(z_rows, hidden, x_tokens, dy_tokens, parts):
    vmem = pl.BlockSpec(memory_space=pltpu.VMEM)
    hbm = pl.BlockSpec(memory_space=pl.ANY)
    wide, tall = (1, INNER, WIDTH), (1, WIDTH, INNER)
    return pl.pallas_call(
        down_kernel,
        grid=(EXPERTS,),
        out_shape=(jax.ShapeDtypeStruct((EXPERTS, INNER, WIDTH), F32),) + tuple(jax.ShapeDtypeStruct(s, F32) for s in (tall, tall, wide)),
        in_specs=[by_expert(WIDTH), by_expert(INNER), vmem, vmem, vmem],
        out_specs=(pl.BlockSpec(wide, lambda e: (e, 0, 0)), hbm, hbm, hbm),
        scratch_shapes=[pltpu.VMEM(s[1:], F32) for s in (tall, tall, wide)] + [pltpu.SemaphoreType.DMA((3,))],
        compiler_params=pltpu.CompilerParams(dimension_semantics=('arbitrary',), vmem_limit_bytes=67000000),
        cost_estimate=pl.CostEstimate(flops=5_000_000_000, bytes_accessed=40_000_000, transcendentals=0),
        name='down_grads',
    )(z_rows, hidden, x_tokens, dy_tokens, parts)


def up_kernel(x_ref, da_ref, db_ref, dw1_ref, dw3_ref):
    for tile in range(4):
        cols = slice(tile * INNER, tile * INNER + INNER)
        x_t = x_ref[:, 0, :, cols].reshape(INNER, INNER).T
        dw1_ref[0, cols, :] = dot_nn(x_t, da_ref[:, 0].reshape(INNER, INNER))
        dw3_ref[0, cols, :] = dot_nn(x_t, db_ref[:, 0].reshape(INNER, INNER))


def up_grads(x_rows, d_gate, d_up):
    tall = pl.BlockSpec((1, WIDTH, INNER), lambda e: (e, 0, 0))
    return pl.pallas_call(
        up_kernel,
        grid=(EXPERTS,),
        out_shape=(jax.ShapeDtypeStruct((EXPERTS, WIDTH, INNER), F32),) * 2,
        in_specs=[by_expert(WIDTH), by_expert(INNER), by_expert(INNER)],
        out_specs=(tall, tall),
        compiler_params=pltpu.CompilerParams(dimension_semantics=('arbitrary',), vmem_limit_bytes=67000000),
        cost_estimate=pl.CostEstimate(flops=9_000_000_000, bytes_accessed=44_000_000, transcendentals=0),
        name='up_grads',
    )(x_rows, d_gate, d_up)


def partners(kind):
    pairs = []
    for me in range(8):
        core = me % 2
        along_x, along_y = me ^ 2, me ^ 4
        first, second = (along_x, along_y) if core == 0 else (along_y, along_x)
        pairs.append((me, {'first': first, 'second': second, 'chip': me ^ 1}[kind]))
    return pairs


def solution(mesh):
    token_spec = P(('dp', 'ep'), None)
    expert_spec = P('ep', None, None)
    whole_spec = P(None, None)
    grad_spec = P(('dp', 'ep'), None, None)

    def local_backward(x_tokens, dy_tokens, expert_ids, gate_vals, slot_pos, w_gate, w_up, w_down, shared_gate, shared_up, shared_down):
        *saved, far, cross, near, base, leaf, shared_dx, parts = rows_backward(x_tokens, dy_tokens, expert_ids, slot_pos, gate_vals, w_gate, w_up, w_down, shared_gate, shared_up, shared_down)
        x_rows, z_rows, hidden, d_gate, d_up = [rows.reshape((ROLES,) + rows.shape[2:]) for rows in saved]
        far = (lax.ppermute(far, 'ep', partners('first')), lax.ppermute(cross, 'ep', partners('second')))
        down = down_grads(z_rows, hidden, x_tokens, dy_tokens, parts)
        far, down = lax.optimization_barrier((far, down))
        last = (lax.ppermute(near[0] + far[0], 'ep', partners('second')), lax.ppermute(near[1] + far[1], 'ep', partners('first')))
        d_gate, *_ = lax.optimization_barrier((d_gate,) + tuple(far))
        up = up_grads(x_rows, d_gate, d_up)
        last, up = lax.optimization_barrier((last, up))
        own, given = lax.optimization_barrier((base[0] + leaf[0] + last[0], base[1] + leaf[1] + last[1]))
        swapped = lax.ppermute(given, 'ep', partners('chip'))
        core = lax.rem(lax.axis_index('ep'), 2)
        left = jnp.where(core == 0, own, swapped)
        right = jnp.where(core == 0, swapped, own)
        grad_x = (jnp.concatenate((left, right), axis=1) + shared_dx).astype(BF16)
        return grad_x, up[0], up[1], down[0], down[1], down[2], down[3]

    return jax.shard_map(local_backward, mesh=mesh, in_specs=(token_spec, token_spec, token_spec, token_spec, token_spec, expert_spec, expert_spec, expert_spec, whole_spec, whole_spec, whole_spec), out_specs=(token_spec, grad_spec, grad_spec, grad_spec, grad_spec, grad_spec, grad_spec), check_vma=False)
```

```python
import jax
import jax.numpy as jnp
from jax import lax
from jax.experimental import pallas as pl
from jax.experimental.pallas import tpu as pltpu
from jax.sharding import PartitionSpec as P

MESH = pl.DeviceIdType.MESH
BF16 = jnp.bfloat16
F32 = jnp.float32
TOKENS, TOP_K, EXPERTS, ROLES, PARTS = 128, 10, 4, 8, 2
WIDTH, HALF, INNER, SLOT, PART = 2048, 1024, 512, 64, 64
ROWS = 256
X, DY = range(2)
EARLY, LATE = range(2)
TO_FIRST, TO_SECOND, TO_PARTNER, FIRST_ON, FIRST_OVER, SECOND_OVER, DIAG_OVER = range(7)
TRIPS = 7
SEEN_AS = {1: 1, 2: 2, 3: 5, 4: 4, 5: 3, 6: 6, 7: 7}


def swiglu_parts(act_gate, act_up, grad_hidden):
    gate_f32 = act_gate.astype(F32)
    up_f32 = act_up.astype(F32)
    sigma = jax.nn.sigmoid(gate_f32)
    silu_gate = gate_f32 * sigma
    hidden = (silu_gate * up_f32).astype(BF16)
    grad_gate = (grad_hidden * up_f32 * sigma * (1.0 + gate_f32 * (1.0 - sigma))).astype(BF16)
    grad_up = (grad_hidden * silu_gate).astype(BF16)
    return hidden, grad_gate, grad_up


def dot_nn(a, b):
    return lax.dot_general(a, b, (((1,), (0,)), ((), ())), preferred_element_type=F32)


def dot_nt(a, b):
    return lax.dot_general(a, b, (((1,), (1,)), ((), ())), preferred_element_type=F32)


def dot_tn(a, b):
    return lax.dot_general(a, b, (((0,), (0,)), ((), ())), preferred_element_type=F32)


def places():
    me = lax.axis_index('ep')
    core = lax.rem(me, 2)
    flip_x = 2 - 4 * lax.rem(me // 2, 2)
    flip_y = 4 - 8 * (me // 4)
    first = me + flip_x * (1 - core) + flip_y * core
    second = me + flip_y * (1 - core) + flip_x * core
    diag = me + flip_x + flip_y
    partner = me + 1 - 2 * core
    return me, core, first, second, diag, partner


def remote(src, dst, send_sem, recv_sem, device):
    return pltpu.make_async_remote_copy(src_ref=src, dst_ref=dst, send_sem=send_sem, recv_sem=recv_sem, device_id={'ep': device}, device_id_type=MESH)


def one_hot(code, base):
    slot = lax.broadcasted_iota(jnp.int32, (ROWS, TOKENS), 0) + base
    hits = jnp.zeros((ROWS, TOKENS), F32)
    for choice in range(TOP_K):
        hits = jnp.where(slot == code[choice:choice + 1, :], 1.0, hits)
    return hits.astype(BF16)


def unrolled(low, high, step):
    for index in range(low, high):
        step(index, 0)


def rows_kernel(x_ref, dy_ref, ids_ref, pos_ref, gate_ref, w1_ref, w3_ref, w2_ref, s1_ref, s3_ref, s2_ref, xr_ref, zr_ref, h_ref, da_ref, db_ref, far_ref, cross_ref, near_ref, base_ref, leaf_ref, dx_ref, parts_ref, xbuf, dybuf, codes, gates, picks, picks_partner, x_rows, z_rows, w1_buf, w3_buf, w2_buf, acts, grads, r_send, r_mine, r_got, sums, own_sem, send_sem, recv_sem, meta_send, meta_recv, load_sem, rows_sem, grads_sem, swap_send, swap_recv, sums_sem, leaf_send, leaf_recv, shared_sem, shared_out):
    me, core, first, second, diag, partner = places()
    other = 1 - core
    bufs = (xbuf, dybuf)

    def own(which):
        return pltpu.make_async_copy((x_ref, dy_ref)[which], bufs[which].at[0], own_sem.at[which])

    def load(which, expert):
        src, dst = ((w1_ref, w1_buf), (w3_ref, w3_buf), (w2_ref, w2_buf))[which]
        return pltpu.make_async_copy(src.at[expert], dst.at[expert], load_sem.at[which, expert])

    def trip(array, part, kind):
        src, dst, device = ((0, 2, first), (0, 4, second), (0, 1, partner), (2, 6, second), (2, 3, partner), (4, 5, partner), (6, 7, partner))[kind]
        rows = pl.ds(part * PART, PART)
        return remote(bufs[array].at[src, rows], bufs[array].at[dst, rows], send_sem.at[array, part, kind], recv_sem.at[array, part, kind], device)

    def meta(which, role):
        device = (me, partner, first, partner + second - me, second, partner + first - me, diag, partner + diag - me)[role]
        table = (codes, gates)[which]
        seen = SEEN_AS[role]
        return remote(table.at[0], table.at[seen], meta_send.at[which, role], meta_recv.at[which, seen], device)

    def start(array, part, kind):
        trip(array, part, kind).start()

    def pass_over(array, part, kind, over):
        trip(array, part, kind).wait_recv()
        trip(array, part, over).start()

    def first_in(array, part):
        pass_over(array, part, TO_FIRST, FIRST_OVER)

    def second_in(array, part):
        pass_over(array, part, TO_SECOND, SECOND_OVER)

    def diag_in(array, part):
        pass_over(array, part, FIRST_ON, DIAG_OVER)

    def arrived(array, kind):
        for part in range(PARTS):
            trip(array, part, kind).wait_recv()

    def rows_out(array, half, at):
        return pltpu.make_async_copy((x_rows, z_rows)[array].at[at], (xr_ref, zr_ref)[array].at[half, at], rows_sem.at[array, half, at])

    def pick_x(half, low, high):
        def one(at, carry):
            role = half * 4 + at
            select = one_hot(codes[role], me * ROWS)
            picks[role] = select
            picks_partner[role] = one_hot(codes[role], partner * ROWS)
            for tile in range(4):
                cols = slice(tile * INNER, tile * INNER + INNER)
                x_rows[at, :, :, cols] = dot_nn(select, xbuf[role, :, cols]).astype(BF16).reshape(EXPERTS, SLOT, INNER)
            rows_out(X, half, at).start()
            return carry

        unrolled(low, high, one)

    def pick_z(half, low, high):
        def one(at, carry):
            role = half * 4 + at
            slot = lax.broadcasted_iota(jnp.int32, (ROWS, TOKENS), 0) + me * ROWS
            spread = jnp.zeros((ROWS, TOKENS), F32)
            for choice in range(TOP_K):
                spread = jnp.where(slot == codes[role, choice:choice + 1, :], gates[role, choice:choice + 1, :], spread)
            scale = jnp.sum(spread, axis=1, keepdims=True)
            select = picks[role]
            for tile in range(4):
                cols = slice(tile * INNER, tile * INNER + INNER)
                value = dot_nn(select, dybuf[role, :, cols]) * scale
                z_rows[at, :, :, cols] = value.astype(BF16).reshape(EXPERTS, SLOT, INNER)
            rows_out(DY, half, at).start()
            return carry

        unrolled(low, high, one)

    def activations(half, after):
        def one(expert, carry):
            if half == EARLY:
                load(0, expert).wait()
                load(1, expert).wait()
            rows = x_rows[:, expert].reshape(ROWS, WIDTH)
            acts[0, half, expert] = dot_nn(rows, w1_buf[expert]).astype(BF16)
            acts[1, half, expert] = dot_nn(rows, w3_buf[expert]).astype(BF16)
            if expert in after:
                after[expert]()

        unrolled(0, EXPERTS, one)

    def grads_out(which, half, expert):
        return pltpu.make_async_copy(grads.at[which, expert], (h_ref, da_ref, db_ref)[which].at[half, :, expert], grads_sem.at[which, half, expert])

    def sent_rows(expert):
        return r_send.at[pl.ds(expert * 4, 4)]

    def swap(half, expert):
        return remote(sent_rows(expert), r_got.at[half, expert], swap_send.at[half, expert], swap_recv.at[half, expert], partner)

    def rows_back(d_gate, d_up, expert, side, tile):
        at = pl.ds(pl.multiple_of(side * HALF + tile * INNER, INNER), INNER)
        value = dot_nt(d_gate, w1_buf[expert, at, :]) + dot_nt(d_up, w3_buf[expert, at, :])
        return value.astype(BF16).reshape(4, SLOT, INNER)

    def back(half, after):
        def send_side(expert, carry):
            if half == EARLY:
                load(2, expert).wait()
            grad_hidden = dot_nt(z_rows[:, expert].reshape(ROWS, WIDTH), w2_buf[expert])
            parts = swiglu_parts(acts[0, half, expert], acts[1, half, expert], grad_hidden)
            for which in range(3):
                if half == LATE:
                    grads_out(which, EARLY, expert).wait()
                grads[which, expert] = parts[which].reshape(4, SLOT, INNER)
                grads_out(which, half, expert).start()
            if half == LATE:
                swap(EARLY, expert).wait_send()
            for tile in range(2):
                r_send[pl.ds(expert * 4, 4), :, tile * INNER:(tile + 1) * INNER] = rows_back(parts[1], parts[2], expert, other, tile)
            swap(half, expert).start()
            for step, action in after.items():
                pl.when(expert == step)(action)
            return carry

        def own_side(expert, carry):
            d_gate = grads[1, expert].reshape(ROWS, INNER)
            d_up = grads[2, expert].reshape(ROWS, INNER)
            for tile in range(2):
                value = rows_back(d_gate, d_up, expert, core, tile)
                for at in range(4):
                    r_mine[(half * 4 + at) * EXPERTS + expert, :, tile * INNER:(tile + 1) * INNER] = value[at]
            return carry

        lax.fori_loop(0, EXPERTS, send_side, 0)
        lax.fori_loop(0, EXPERTS, own_side, 0)

    def sums_out(role):
        ref = {6: far_ref, 7: cross_ref, 4: near_ref.at[0], 5: near_ref.at[1], 0: base_ref.at[0], 1: base_ref.at[1]}[role]
        return pltpu.make_async_copy(sums.at[role % 4], ref, sums_sem.at[role])

    def leaf(which):
        return remote(sums.at[2 + which], leaf_ref.at[which], leaf_send.at[which], leaf_recv.at[which], (first, second)[which])

    def total(half):
        for expert in range(EXPERTS):
            swap(half, expert).wait_recv()
        for at in range(4):
            role = half * 4 + at
            if half == LATE:
                if at < 2:
                    sums_out(at).wait()
                else:
                    leaf(at - 2).wait_send()
            else:
                if at < 2:
                    shared_rows_out(at).wait()
            mine = r_mine[role * EXPERTS:(role + 1) * EXPERTS].reshape(ROWS, HALF)
            sums[at] = dot_tn(picks[role], mine) + dot_tn(picks_partner[role], r_got[half, :, at ^ 1].reshape(ROWS, HALF))
            if half == LATE or at < 2:
                sums_out(role).start()

    def shared_load(which):
        src, dst = ((s1_ref, r_mine.at[:, :, :INNER]), (s3_ref, r_mine.at[:, :, INNER:]), (s2_ref.at[:, :, :HALF], r_send.at[:8]), (s2_ref.at[:, :, HALF:], r_send.at[8:]))[which]
        return pltpu.make_async_copy(src, dst, shared_sem.at[which])

    def shared_rows_out(which):
        return pltpu.make_async_copy(sums.at[which], dx_ref.at[:, which * HALF:(which + 1) * HALF], shared_out.at[which])

    def shared_parts_out(which):
        return pltpu.make_async_copy(acts.at[1, LATE, which, :TOKENS], parts_ref.at[which], shared_out.at[2 + which])

    def shared_chain():
        x, dy = xbuf[0], dybuf[0]
        act_gate = dot_nn(x, r_mine[:, :, :INNER].reshape(WIDTH, INNER)).astype(BF16)
        act_up = dot_nn(x, r_mine[:, :, INNER:].reshape(WIDTH, INNER)).astype(BF16)
        grad_hidden = dot_nt(dy[:, :HALF], r_send[:8].reshape(INNER, HALF)) + dot_nt(dy[:, HALF:], r_send[8:].reshape(INNER, HALF))
        parts = swiglu_parts(act_gate, act_up, grad_hidden)
        for which in range(3):
            acts[1, LATE, which, :TOKENS] = parts[which]
            shared_parts_out(which).start()
        for which in range(2):
            for tile in range(2):
                at = slice((which * 2 + tile) * 8, (which * 2 + tile) * 8 + 8)
                gate_w = r_mine[at, :, :INNER].reshape(INNER, INNER)
                up_w = r_mine[at, :, INNER:].reshape(INNER, INNER)
                sums[which, :, tile * INNER:(tile + 1) * INNER] = dot_nt(parts[1], gate_w) + dot_nt(parts[2], up_w)
            shared_rows_out(which).start()

    for which in range(2):
        own(which).start()
    barrier = pltpu.get_barrier_semaphore()
    for step in range(1, ROLES):
        pl.semaphore_signal(barrier, inc=1, device_id={'ep': lax.rem(me + step, ROLES)}, device_id_type=MESH)
    codes[0] = jnp.zeros((16, TOKENS), jnp.int32)
    gates[0] = jnp.zeros((16, TOKENS), F32)
    codes[0, :TOP_K, :] = jnp.where(pos_ref[...] >= 0, ids_ref[...] * SLOT + pos_ref[...], -1)
    gates[0, :TOP_K, :] = gate_ref[...]
    for which in range(2):
        own(which).wait()
    pl.semaphore_wait(barrier, ROLES - 1)

    for role in SEEN_AS:
        for which in range(2):
            meta(which, role).start()
    for kind in (TO_FIRST, TO_PARTNER):
        for array in (X, DY):
            for part in range(PARTS):
                start(array, part, kind)
    for which in range(4):
        shared_load(which).start()
    pick_x(EARLY, 0, 1)
    pick_z(EARLY, 0, 1)
    for which in range(4):
        shared_load(which).wait()
    for expert in range(EXPERTS):
        load(0, expert).start()
        load(1, expert).start()
    shared_chain()
    first_in(X, 0)
    start(X, 0, TO_SECOND)
    for role in SEEN_AS:
        for which in range(2):
            meta(which, role).wait_recv()
    arrived(X, TO_PARTNER)
    pick_x(EARLY, 1, 2)
    first_in(X, 1)
    for expert in range(EXPERTS):
        load(2, expert).start()
    arrived(DY, TO_PARTNER)
    pick_z(EARLY, 1, 2)
    arrived(X, FIRST_OVER)
    pick_x(EARLY, 2, 4)

    def queue_x():
        start(X, 1, TO_SECOND)
        start(X, 0, FIRST_ON)

    def queue_both():
        start(X, 1, FIRST_ON)
        first_in(DY, 0)
        start(DY, 0, TO_SECOND)

    def queue_dy():
        first_in(DY, 1)
        start(DY, 1, TO_SECOND)
        start(DY, 0, FIRST_ON)
        start(DY, 1, FIRST_ON)

    activations(EARLY, {0: queue_x, 1: queue_both, 3: queue_dy})
    arrived(DY, FIRST_OVER)
    pick_z(EARLY, 2, 4)

    def rest_x():
        second_in(X, 1)
        diag_in(X, 0)

    back(EARLY, {1: lambda: second_in(X, 0), 3: rest_x})
    total(EARLY)
    diag_in(X, 1)
    for array in (X, DY):
        for at in range(4):
            rows_out(array, EARLY, at).wait()
    arrived(X, SECOND_OVER)
    pick_x(LATE, 0, 2)
    arrived(X, DIAG_OVER)
    pick_x(LATE, 2, 4)
    for which in range(3):
        shared_parts_out(which).wait()
    activations(LATE, {1: lambda: second_in(DY, 0), 3: lambda: second_in(DY, 1)})
    diag_in(DY, 0)
    diag_in(DY, 1)
    for which in range(2):
        leaf(which).start()
    arrived(DY, SECOND_OVER)
    pick_z(LATE, 0, 2)
    arrived(DY, DIAG_OVER)
    pick_z(LATE, 2, 4)
    back(LATE, {})
    total(LATE)

    for array in (X, DY):
        for part in range(PARTS):
            for kind in range(TRIPS):
                trip(array, part, kind).wait_send()
    for role in SEEN_AS:
        for which in range(2):
            meta(which, role).wait_send()
    for expert in range(EXPERTS):
        swap(LATE, expert).wait_send()
        for which in range(3):
            grads_out(which, LATE, expert).wait()
    for which in range(2):
        leaf(which).wait_recv()
    for at in range(4):
        for array in (X, DY):
            rows_out(array, LATE, at).wait()
        sums_out(4 + at).wait()


def rows_backward(x_tokens, dy_tokens, expert_ids, slot_pos, gate_vals, w_gate, w_up, w_down, shared_gate, shared_up, shared_down):
    hbm = pl.BlockSpec(memory_space=pl.ANY)
    vmem = pl.BlockSpec(memory_space=pltpu.VMEM)
    rows = (2, 4, EXPERTS, SLOT, WIDTH)
    grads = (2, 4, EXPERTS, SLOT, INNER)
    pair = (2, TOKENS, HALF)
    parts = (3, TOKENS, INNER)
    blocks = (ROLES, TOKENS, WIDTH)
    tables = (ROLES, 16, TOKENS)
    select = (ROLES, ROWS, TOKENS)
    dma = pltpu.SemaphoreType.DMA
    outs = [(s, BF16) for s in (rows, rows, grads, grads, grads)] + [(pair[1:], F32)] * 2 + [(pair, F32)] * 3 + [((TOKENS, WIDTH), F32), (parts, BF16)]
    scratch = [(blocks, BF16), (blocks, BF16), (tables, jnp.int32), (tables, F32), (select, BF16), (select, BF16), (rows[1:], BF16), (rows[1:], BF16)]
    scratch += [(w.shape, BF16) for w in (w_gate, w_up, w_down)]
    scratch += [((2, 2, EXPERTS, ROWS, INNER), BF16), ((3, EXPERTS, 4, SLOT, INNER), BF16), ((16, SLOT, HALF), BF16), ((32, SLOT, HALF), BF16)]
    scratch += [((2, EXPERTS, 4, SLOT, HALF), BF16), ((4, TOKENS, HALF), F32)]
    trips = (2, PARTS, TRIPS)
    sems = [(2,), trips, trips, (2, ROLES), (2, ROLES), (3, EXPERTS), (2, 2, 4), (3, 2, EXPERTS), (2, EXPERTS), (2, EXPERTS), (ROLES,), (2,), (2,), (4,), (5,)]
    return pl.pallas_call(
        rows_kernel,
        out_shape=tuple(jax.ShapeDtypeStruct(s, d) for s, d in outs),
        in_specs=[hbm] * 2 + [vmem] * 3 + [hbm] * 6,
        out_specs=(hbm,) * len(outs),
        scratch_shapes=[pltpu.VMEM(s, d) for s, d in scratch] + [dma(s) for s in sems],
        compiler_params=pltpu.CompilerParams(collective_id=0, has_side_effects=True, vmem_limit_bytes=67000000),
        name='rows_backward',
    )(x_tokens, dy_tokens, expert_ids.T, slot_pos.T, gate_vals.T, w_gate, w_up, w_down, shared_gate.reshape(32, SLOT, INNER), shared_up.reshape(32, SLOT, INNER), shared_down.reshape(8, SLOT, WIDTH))


def down_kernel(z_ref, h_ref, x_ref, dy_ref, parts_ref, dw2_ref, s1_ref, s3_ref, s2_ref, s1_buf, s3_buf, s2_buf, sem):
    expert = pl.program_id(0)

    def shared_out(which):
        src, dst = ((s1_buf, s1_ref), (s3_buf, s3_ref), (s2_buf, s2_ref))[which]
        return pltpu.make_async_copy(src, dst.at[0], sem.at[which])

    @pl.when(expert == 0)
    def _():
        s1_buf[...] = dot_nn(x_ref[...].T, parts_ref[1])
        shared_out(0).start()

    @pl.when(expert == 1)
    def _():
        s3_buf[...] = dot_nn(x_ref[...].T, parts_ref[2])
        shared_out(1).start()

    @pl.when(expert == 2)
    def _():
        s2_buf[...] = dot_nn(parts_ref[0].T, dy_ref[...])
        shared_out(2).start()

    hidden_t = h_ref[:, 0].reshape(INNER, INNER).T
    for tile in range(4):
        cols = slice(tile * INNER, tile * INNER + INNER)
        dw2_ref[0, :, cols] = dot_nn(hidden_t, z_ref[:, 0, :, cols].reshape(INNER, INNER))

    @pl.when(expert == EXPERTS - 1)
    def _():
        for which in range(3):
            shared_out(which).wait()


def by_expert(inner):
    return pl.BlockSpec((ROLES, 1, SLOT, inner), lambda e: (0, e, 0, 0))


def down_grads(z_rows, hidden, x_tokens, dy_tokens, parts):
    vmem = pl.BlockSpec(memory_space=pltpu.VMEM)
    hbm = pl.BlockSpec(memory_space=pl.ANY)
    wide, tall = (1, INNER, WIDTH), (1, WIDTH, INNER)
    return pl.pallas_call(
        down_kernel,
        grid=(EXPERTS,),
        out_shape=(jax.ShapeDtypeStruct((EXPERTS, INNER, WIDTH), F32),) + tuple(jax.ShapeDtypeStruct(s, F32) for s in (tall, tall, wide)),
        in_specs=[by_expert(WIDTH), by_expert(INNER), vmem, vmem, vmem],
        out_specs=(pl.BlockSpec(wide, lambda e: (e, 0, 0)), hbm, hbm, hbm),
        scratch_shapes=[pltpu.VMEM(s[1:], F32) for s in (tall, tall, wide)] + [pltpu.SemaphoreType.DMA((3,))],
        compiler_params=pltpu.CompilerParams(dimension_semantics=('arbitrary',), vmem_limit_bytes=67000000),
        cost_estimate=pl.CostEstimate(flops=5_000_000_000, bytes_accessed=40_000_000, transcendentals=0),
        name='down_grads',
    )(z_rows, hidden, x_tokens, dy_tokens, parts)


def up_kernel(x_ref, da_ref, db_ref, dw1_ref, dw3_ref):
    for tile in range(4):
        cols = slice(tile * INNER, tile * INNER + INNER)
        x_t = x_ref[:, 0, :, cols].reshape(INNER, INNER).T
        dw1_ref[0, cols, :] = dot_nn(x_t, da_ref[:, 0].reshape(INNER, INNER))
        dw3_ref[0, cols, :] = dot_nn(x_t, db_ref[:, 0].reshape(INNER, INNER))


def up_grads(x_rows, d_gate, d_up):
    tall = pl.BlockSpec((1, WIDTH, INNER), lambda e: (e, 0, 0))
    return pl.pallas_call(
        up_kernel,
        grid=(EXPERTS,),
        out_shape=(jax.ShapeDtypeStruct((EXPERTS, WIDTH, INNER), F32),) * 2,
        in_specs=[by_expert(WIDTH), by_expert(INNER), by_expert(INNER)],
        out_specs=(tall, tall),
        compiler_params=pltpu.CompilerParams(dimension_semantics=('arbitrary',), vmem_limit_bytes=67000000),
        cost_estimate=pl.CostEstimate(flops=9_000_000_000, bytes_accessed=44_000_000, transcendentals=0),
        name='up_grads',
    )(x_rows, d_gate, d_up)


def partners(kind):
    pairs = []
    for me in range(8):
        core = me % 2
        along_x, along_y = me ^ 2, me ^ 4
        first, second = (along_x, along_y) if core == 0 else (along_y, along_x)
        pairs.append((me, {'first': first, 'second': second, 'chip': me ^ 1}[kind]))
    return pairs


def solution(mesh):
    token_spec = P(('dp', 'ep'), None)
    expert_spec = P('ep', None, None)
    whole_spec = P(None, None)
    grad_spec = P(('dp', 'ep'), None, None)

    def local_backward(x_tokens, dy_tokens, expert_ids, gate_vals, slot_pos, w_gate, w_up, w_down, shared_gate, shared_up, shared_down):
        *saved, far, cross, near, base, leaf, shared_dx, parts = rows_backward(x_tokens, dy_tokens, expert_ids, slot_pos, gate_vals, w_gate, w_up, w_down, shared_gate, shared_up, shared_down)
        x_rows, z_rows, hidden, d_gate, d_up = [rows.reshape((ROLES,) + rows.shape[2:]) for rows in saved]
        far = (lax.ppermute(far, 'ep', partners('first')), lax.ppermute(cross, 'ep', partners('second')))
        down = down_grads(z_rows, hidden, x_tokens, dy_tokens, parts)
        far, down = lax.optimization_barrier((far, down))
        last = (lax.ppermute(near[0] + far[0], 'ep', partners('second')), lax.ppermute(near[1] + far[1], 'ep', partners('first')))
        d_gate, *_ = lax.optimization_barrier((d_gate,) + tuple(far))
        up = up_grads(x_rows, d_gate, d_up)
        last, up = lax.optimization_barrier((last, up))
        own, given = lax.optimization_barrier((base[0] + leaf[0] + last[0], base[1] + leaf[1] + last[1]))
        swapped = lax.ppermute(given, 'ep', partners('chip'))
        core = lax.rem(lax.axis_index('ep'), 2)
        left = jnp.where(core == 0, own, swapped)
        right = jnp.where(core == 0, swapped, own)
        grad_x = (jnp.concatenate((left, right), axis=1) + shared_dx).astype(BF16)
        return grad_x, up[0], up[1], down[0], down[1], down[2], down[3]

    return jax.shard_map(local_backward, mesh=mesh, in_specs=(token_spec, token_spec, token_spec, token_spec, token_spec, expert_spec, expert_spec, expert_spec, whole_spec, whole_spec, whole_spec), out_specs=(token_spec, grad_spec, grad_spec, grad_spec, grad_spec, grad_spec, grad_spec), check_vma=False)
```
